32 devices in a mesh: tile: 8 (over z, x), sub: 4 (over y, core).
Axes of the slice: x: 2, y: 2, z: 4, core: 2. Of those that a mesh axis runs over, the one named last changes fastest.
Arguments:
- grid_feats: bfloat16 [4096, 512], P(('tile', 'sub')), may hold values from -6 to 6
- mesh_feats: bfloat16 [4096, 512], P(('tile', 'sub')), may hold values from -6 to 6
- encode_edges: bfloat16 [32768, 512], P(('tile', 'sub')), may hold values from -6 to 6
- decode_edges: bfloat16 [16384, 512], P(('tile', 'sub')), may hold values from -6 to 6
- encode_source: int32 [32768], P(('tile', 'sub')), may hold values from 0 to 4095, as said below
- encode_target: int32 [32768], P(('tile', 'sub')), may hold values from -1 to 4095, as said below
- decode_source: int32 [16384], P(('tile', 'sub')), may hold values from 0 to 4095, as said below
- decode_target: int32 [16384], P(('tile', 'sub')), may hold values from -1 to 4095, as said below
- owner_fine: int32 [4096], P(('tile', 'sub')), may hold values from 0 to 1023, as said below
- owner_coarse: int32 [1024], P('tile'), may hold values from 0 to 511
- encode_weight: bfloat16 [512, 512], replicated, may hold values from -0.25 to 0.25
- decode_weight: bfloat16 [512, 512], replicated, may hold values from -0.25 to 0.25
- middle_weight: bfloat16 [512, 512], replicated, may hold values from -0.25 to 0.25
- summit_weight: bfloat16 [512, 512], replicated, may hold values from -0.25 to 0.25
- cotangent: bfloat16 [4096, 512], P(('tile', 'sub')), may hold values from -6 to 6
Outputs:
- grid_update: bfloat16 [4096, 512], P(('tile', 'sub'))
- encode_grad: float32 [512, 512], replicated
- decode_grad: float32 [512, 512], replicated
- middle_grad: float32 [512, 512], replicated
- summit_grad: float32 [512, 512], replicated
The draws below stay inside these ranges and needn't reach their ends.
Inputs may be any that keep to these rules, and one draw needn't show every extreme that they name: `encode_source`: edge slot e is listed on device d = e // 1024; its source grid node lies on device d - 1, d or d + 1. `encode_target`: -1 marks padding; every other value is a mesh node of the device that lists the slot. On each device padding fills whole blocks of 128 slots after all live ones; every device has a live block, and some device has no padding. `decode_source`: edge slot e is listed on device d = e // 512; its source mesh node lies on device d - 1, d or d + 1. `decode_target`: -1 marks padding; every other value is a grid node of the device that lists the slot. On each device padding fills whole blocks of 128 slots after all live ones; every device has a live block, and some device has no padding. `owner_fine`: the middle node of fine mesh node m lies on the tile of the device that holds m.
All inputs are finite; a program needn't handle non-finite values.
Results may differ from the reference program's by a relative error of at most 0.012.
Values may be sent and summed in bfloat16 or wider, within the bound.
No kernel may reach another device: no remote copies, remote signals or barrier semaphores. Data moves between devices by JAX's collectives and lax.ppermute only.
A program may use at most 64 MiB of HBM per device.

```python
import jax
import jax.numpy as jnp

D = 512
GRID_DEV = 128
MESH_DEV = 128
MID_TILE = 128
TOP_NODES = 512
ENCODE_DEV = 1024
DECODE_DEV = 512
BLOCK = 128
GRID = 4096
MESH = 4096
MIDDLE = 1024
ENCODE = 32768
DECODE = 16384
N_TILE = 8
N_SUB = 4
DEVICES = 32


def near_senders(key, per_device, node_rows):
    device_of = jnp.arange(per_device * DEVICES, dtype=jnp.int32) // per_device
    lowest = jnp.maximum(device_of - 1, 0) * node_rows
    highest = jnp.minimum(device_of + 2, DEVICES) * node_rows
    return jax.random.randint(key, (per_device * DEVICES,), lowest, highest, dtype=jnp.int32)


def own_receivers(key, per_device, node_rows):
    blocks_each = per_device // BLOCK
    live_key = jax.random.fold_in(key, 11)
    full_key = jax.random.fold_in(key, 12)
    node_key = jax.random.fold_in(key, 13)
    live_blocks = jax.random.randint(live_key, (DEVICES,), 1, blocks_each + 1, dtype=jnp.int32)
    full_device = jax.random.randint(full_key, (), 0, DEVICES, dtype=jnp.int32)
    live_blocks = jnp.where(jnp.arange(DEVICES, dtype=jnp.int32) == full_device, blocks_each, live_blocks)
    edge_ids = jnp.arange(per_device * DEVICES, dtype=jnp.int32)
    device_of = edge_ids // per_device
    block_of = edge_ids % per_device // BLOCK
    chosen = jax.random.randint(node_key, (per_device * DEVICES,), device_of * node_rows, (device_of + 1) * node_rows, dtype=jnp.int32)
    return jnp.where(block_of < live_blocks[device_of], chosen, -1).astype(jnp.int32)


def draw_encode_source(key, part):
    return near_senders(jax.random.fold_in(key, 1), ENCODE_DEV, GRID_DEV)


def draw_encode_target(key, part):
    return own_receivers(jax.random.fold_in(key, 2), ENCODE_DEV, MESH_DEV)


def draw_decode_source(key, part):
    return near_senders(jax.random.fold_in(key, 3), DECODE_DEV, MESH_DEV)


def draw_decode_target(key, part):
    return own_receivers(jax.random.fold_in(key, 4), DECODE_DEV, GRID_DEV)


def draw_owner_fine(key, part):
    node_ids = jnp.arange(MESH_DEV * DEVICES, dtype=jnp.int32)
    tile_of = node_ids // MESH_DEV // N_SUB
    return jax.random.randint(jax.random.fold_in(key, 5), (MESH_DEV * DEVICES,), tile_of * MID_TILE, (tile_of + 1) * MID_TILE, dtype=jnp.int32)


def with_ends(drawn, rng, smallest, top_value):
    dims = drawn.shape
    spot = [jax.random.randint(jax.random.fold_in(rng, axis), (), 0, dims[axis]) for axis in range(len(dims))]
    drawn = drawn.at[tuple(spot)].set(smallest)
    longest = dims.index(max(dims))
    spot[longest] = (spot[longest] + 1) % dims[longest]
    return drawn.at[tuple(spot)].set(top_value)


def steps_of(key, extent, pieces, least, top_value):
    factor_of, own = 1.0, jax.random.fold_in(key, 6)
    for axis_at, blocks in pieces:
        draws = jnp.exp(jax.random.uniform(jax.random.fold_in(own, axis_at), (blocks,), jnp.float32, least / len(pieces), top_value / len(pieces)))
        factor_of = factor_of * jnp.repeat(draws, extent[axis_at] // blocks).reshape([-1 if axis == axis_at else 1 for axis in range(len(extent))])
    return factor_of


def noise(stream_key, extent, deviation, reach, pieces=(), kind=jnp.bfloat16):
    level = steps_of(stream_key, extent, pieces, -0.22, 0.18) if pieces else 1.0
    values = jax.random.normal(stream_key, extent, jnp.float32) * deviation * level
    return jnp.minimum(jnp.maximum(values, -reach), reach).astype(kind)


def setup_inputs(seed: int = 0) -> dict:
    key_of = jax.random.split(jax.random.key(seed), 16)
    grid_feats = noise(key_of[0], (GRID, D), 1.0, 6.0, ((0, 32),))
    mesh_feats = noise(key_of[1], (MESH, D), 1.0, 6.0, ((0, 32),))
    encode_edges = noise(key_of[2], (ENCODE, D), 1.0, 6.0, ((0, 32),))
    decode_edges = noise(key_of[3], (DECODE, D), 1.0, 6.0, ((0, 32),))
    encode_source = draw_encode_source(jax.random.fold_in(key_of[15], 71), 0)
    encode_target = draw_encode_target(jax.random.fold_in(key_of[15], 71), 0)
    decode_source = draw_decode_source(jax.random.fold_in(key_of[15], 71), 0)
    decode_target = draw_decode_target(jax.random.fold_in(key_of[15], 71), 0)
    owner_fine = draw_owner_fine(jax.random.fold_in(key_of[15], 71), 0)
    owner_coarse = with_ends(jax.random.randint(key_of[9], (MIDDLE,), 0, TOP_NODES), jax.random.fold_in(key_of[9], 1), 0, TOP_NODES - 1).astype(jnp.int32)
    encode_weight = noise(key_of[10], (D, D), D ** -0.5, 0.25)
    decode_weight = noise(key_of[11], (D, D), D ** -0.5, 0.25)
    middle_weight = noise(key_of[12], (D, D), D ** -0.5, 0.25)
    summit_weight = noise(key_of[13], (D, D), D ** -0.5, 0.25)
    cotangent = noise(key_of[14], (GRID, D), 1.0, 6.0, ((0, 32),))
    return dict(grid_feats=grid_feats, mesh_feats=mesh_feats, encode_edges=encode_edges, decode_edges=decode_edges, encode_source=encode_source, encode_target=encode_target, decode_source=decode_source, decode_target=decode_target, owner_fine=owner_fine, owner_coarse=owner_coarse, encode_weight=encode_weight, decode_weight=decode_weight, middle_weight=middle_weight, summit_weight=summit_weight, cotangent=cotangent)


def silu_slope(values):
    sigmoid = jax.nn.sigmoid(values)
    return sigmoid * (1.0 + values * (1.0 - sigmoid))


def edge_sum(values, targets, segments):
    aimed = jnp.where(targets >= 0, targets, segments).astype(jnp.int32)
    return jax.ops.segment_sum(values, aimed, num_segments=segments + 1)[:segments]


def reference(grid_feats, mesh_feats, encode_edges, decode_edges, encode_source, encode_target, decode_source, decode_target, owner_fine, owner_coarse, encode_weight, decode_weight, middle_weight, summit_weight, cotangent):
    encode_factor = MESH_DEV / ENCODE_DEV
    decode_factor = GRID_DEV / DECODE_DEV
    middle_factor = MID_TILE / (MESH_DEV * N_SUB)
    summit_factor = TOP_NODES / (MID_TILE * N_TILE)
    encode_rows = grid_feats[encode_source]
    encode_pre = jnp.dot(encode_rows, encode_weight, preferred_element_type=jnp.float32) + encode_edges.astype(jnp.float32)
    mesh_mid = (mesh_feats.astype(jnp.float32) + encode_factor * edge_sum(jax.nn.silu(encode_pre), encode_target, MESH)).astype(jnp.bfloat16)
    middle_sum = jax.ops.segment_sum(mesh_mid.astype(jnp.float32), owner_fine, num_segments=MIDDLE)
    middle_in = (middle_factor * middle_sum).astype(jnp.bfloat16)
    middle_act = jnp.dot(middle_in, middle_weight, preferred_element_type=jnp.float32)
    middle_out = (middle_in.astype(jnp.float32) + jax.nn.silu(middle_act)).astype(jnp.bfloat16)
    summit_sum = jax.ops.segment_sum(middle_out.astype(jnp.float32), owner_coarse, num_segments=TOP_NODES)
    summit_in = (summit_factor * summit_sum).astype(jnp.bfloat16)
    summit_act = jnp.dot(summit_in, summit_weight, preferred_element_type=jnp.float32)
    summit_out = jax.nn.silu(summit_act).astype(jnp.bfloat16)
    lifted = middle_out.astype(jnp.float32)[owner_fine] + summit_out.astype(jnp.float32)[owner_coarse[owner_fine]]
    mesh_out = (mesh_mid.astype(jnp.float32) + lifted).astype(jnp.bfloat16)
    decode_rows = mesh_out[decode_source]
    decode_pre = jnp.dot(decode_rows, decode_weight, preferred_element_type=jnp.float32) + decode_edges.astype(jnp.float32)
    grid_update = (grid_feats.astype(jnp.float32) + decode_factor * edge_sum(jax.nn.silu(decode_pre), decode_target, GRID)).astype(jnp.bfloat16)
    decode_live = (decode_target >= 0)[:, None]
    incoming = cotangent[jnp.maximum(decode_target, 0)].astype(jnp.float32) * decode_factor
    decode_slope = jnp.where(decode_live, incoming * silu_slope(decode_pre), 0.0).astype(jnp.bfloat16)
    decode_grad = jnp.dot(decode_rows.T, decode_slope, preferred_element_type=jnp.float32)
    passed = jnp.dot(decode_slope, decode_weight.T, preferred_element_type=jnp.float32)
    mesh_grad = jax.ops.segment_sum(passed, decode_source, num_segments=MESH)
    level_grad = jax.ops.segment_sum(mesh_grad, owner_fine, num_segments=MIDDLE)
    summit_total = jax.ops.segment_sum(level_grad, owner_coarse, num_segments=TOP_NODES)
    summit_slope = (summit_total * silu_slope(summit_act)).astype(jnp.bfloat16)
    summit_grad = jnp.dot(summit_in.T, summit_slope, preferred_element_type=jnp.float32)
    summit_back = jnp.dot(summit_slope, summit_weight.T, preferred_element_type=jnp.float32).astype(jnp.bfloat16)
    level_total = level_grad + summit_factor * summit_back.astype(jnp.float32)[owner_coarse]
    middle_slope = (level_total * silu_slope(middle_act)).astype(jnp.bfloat16)
    middle_grad = jnp.dot(middle_in.T, middle_slope, preferred_element_type=jnp.float32)
    middle_back = level_total + jnp.dot(middle_slope, middle_weight.T, preferred_element_type=jnp.float32)
    mesh_total = mesh_grad + middle_factor * middle_back[owner_fine]
    encode_live = (encode_target >= 0)[:, None]
    upstream = mesh_total[jnp.maximum(encode_target, 0)] * encode_factor
    encode_slope = jnp.where(encode_live, upstream * silu_slope(encode_pre), 0.0).astype(jnp.bfloat16)
    encode_grad = jnp.dot(encode_rows.T, encode_slope, preferred_element_type=jnp.float32)
    return grid_update, encode_grad, decode_grad, middle_grad, summit_grad
```

```python
import functools

import jax
import jax.numpy as jnp
from jax import lax
from jax.experimental import pallas as pl
from jax.experimental.pallas import tpu as pltpu
from jax.sharding import Mesh, PartitionSpec as P

TOP_NODES = 512
ALL = ("tile", "row", "core")
CHIPS = ("tile", "row")
BF16 = jnp.bfloat16
F32 = jnp.float32
I32 = jnp.int32


def mm(left, right):
    return jnp.dot(left, right, preferred_element_type=F32)


def mm_tn(left, right):
    return lax.dot_general(left, right, (((0,), (0,)), ((), ())), preferred_element_type=F32)


def mm_nt(left, right):
    return lax.dot_general(left, right, (((1,), (1,)), ((), ())), preferred_element_type=F32)


def sigmoid(values):
    return 0.5 + 0.5 * jnp.tanh(0.5 * values)


def rows_onehot(ids, rows):
    n = ids.shape[1]
    hit = lax.broadcasted_iota(I32, (rows, n), 0) == ids
    return jnp.where(hit, 1.0, 0.0).astype(BF16)


def column(ids):
    n = ids.shape[1]
    wide = jnp.broadcast_to(ids.astype(F32), (8, n))
    return wide.T[:, :1].astype(I32)


def cols_onehot(ids, cols):
    n = ids.shape[1]
    hit = lax.broadcasted_iota(I32, (n, cols), 1) == column(ids)
    return jnp.where(hit, 1.0, 0.0).astype(BF16)


def slots(source, device, core, rows):
    rel = source - device * rows
    before = rel < 0
    after = rel >= rows
    shift_before = jnp.where(core == 0, 3 * rows, 2 * rows)
    shift_after = jnp.where(core == 0, 0, rows)
    return rel + jnp.where(before, shift_before, 0) + jnp.where(after, shift_after, 0)


def encode_kernel(
    dev_ref,
    grid_ref,
    partner_ref,
    far_ref,
    mesh_ref,
    edges_ref,
    source_ref,
    target_ref,
    fine_ref,
    weight_ref,
    fetched_ref,
    slope_ref,
    core_ref,
    farpkt_ref,
    keep_ref,
    *,
    subs,
    level_rows,
    factor,
):
    device = dev_ref[0]
    core = device % 2
    rows = grid_ref.shape[0]
    mesh_rows = mesh_ref.shape[0]
    half = level_rows // 2
    picks = cols_onehot(slots(source_ref[...], device, core, rows), 3 * rows)
    fetched = (
        mm(picks[:, :rows], grid_ref[...])
        + mm(picks[:, rows : 2 * rows], partner_ref[...])
        + mm(picks[:, 2 * rows :], far_ref[...])
    ).astype(BF16)
    fetched_ref[...] = fetched
    pre = mm(fetched, weight_ref[...]) + edges_ref[...].astype(F32)
    sig = sigmoid(pre)
    act = (pre * sig).astype(BF16)
    slope_ref[...] = (sig * (1.0 + pre * (1.0 - sig))).astype(BF16)
    raw = target_ref[...]
    aimed = jnp.where(raw >= 0, raw - device * mesh_rows, -1)
    summed = mm(rows_onehot(aimed, mesh_rows), act)
    mid = (mesh_ref[...].astype(F32) + factor * summed).astype(BF16)
    local = fine_ref[...] - (device // subs) * level_rows
    part = mm(rows_onehot(local, level_rows), mid)
    first = part[:half]
    second = part[half:]
    keep_ref[...] = jnp.where(core == 0, first, second)
    core_ref[:half] = jnp.where(core == 0, second, first).astype(BF16)
    core_ref[half : half + mesh_rows] = mid
    farpkt_ref[:mesh_rows] = mid
    features = grid_ref.shape[1]
    spot = (
        lax.broadcasted_iota(I32, (mesh_rows, features), 0)
        == lax.broadcasted_iota(I32, (mesh_rows, features), 1)
    )
    spread = jnp.where(spot, 1.0, 0.0).astype(BF16)
    fine_rows = mm(
        jnp.broadcast_to(local.astype(F32), (16, mesh_rows)).astype(BF16), spread
    ).astype(BF16)[:8]
    core_ref[half + mesh_rows :] = fine_rows
    farpkt_ref[mesh_rows:] = fine_rows


def spread_kernel(dev_ref, mine_ref, other_ref, coarse_ref, out_ref, *, subs, factor):
    device = dev_ref[0]
    core = device % 2
    tile = device // subs
    half, features = mine_ref.shape
    group = features // half
    total = mine_ref[...].astype(F32) + other_ref[...].astype(F32)
    mid = (factor * total).astype(BF16)
    level_rows = coarse_ref.shape[1]
    ids = coarse_ref[...]
    split = jnp.where(
        lax.broadcasted_iota(I32, (16, level_rows), 0) == 0, ids >> 4, ids & 15
    )
    j = lax.broadcasted_iota(I32, (level_rows, features), 0) - core * half
    lane = lax.broadcasted_iota(I32, (level_rows, features), 1) - (tile % group) * half
    sel = (j == lane) & (j >= 0) & (j < half)
    ids_rows = mm(split.astype(F32).astype(BF16), jnp.where(sel, 1.0, 0.0).astype(BF16))
    ids_rows = ids_rows.astype(BF16)[:8]
    for peer in range(out_ref.shape[0]):
        out_ref[peer, :half] = mid
        out_ref[peer, half:] = ids_rows


def middle_kernel(
    dev_ref,
    mine_ref,
    other_ref,
    core_ref,
    farpkt_ref,
    farin_ref,
    grid_ref,
    cot_ref,
    edges_ref,
    source_ref,
    target_ref,
    decode_weight_ref,
    middle_weight_ref,
    summit_weight_ref,
    update_ref,
    dgrad_ref,
    own_ref,
    partner_ref,
    far_ref,
    level_ref,
    middle_slope_ref,
    summit_in_ref,
    summit_slope_ref,
    ids_ref,
    out_scr,
    lift_scr,
    *,
    subs,
    level_rows,
    summit_factor,
    decode_factor,
):
    device = dev_ref[0]
    core = device % 2
    tile = device // subs
    tiles, _, features = mine_ref.shape
    half = level_rows // 2
    group = min(features // half, tiles)
    groups = tiles // group
    chunk = group * half
    for g in range(groups):
        for src, which in ((mine_ref, core), (other_ref, 1 - core)):
            block = src[g * group : (g + 1) * group]
            level_ref[which, g] = block[:, :half].reshape(chunk, features)
            codes = jnp.sum(block[:, half:].astype(F32), axis=0)
            ids = (codes[0:1] * 16.0 + codes[1:2]).astype(I32)[:, :chunk]
            ids_ref[which, g] = jnp.broadcast_to(ids, (8, chunk))
    summed = jnp.zeros((TOP_NODES, features), F32)
    for g in range(groups):
        for h in range(2):
            mid = level_ref[h, g]
            act = mm(mid, middle_weight_ref[...])
            sig = sigmoid(act)
            out = (mid.astype(F32) + act * sig).astype(BF16)
            middle_slope_ref[h, g] = (sig * (1.0 + act * (1.0 - sig))).astype(BF16)
            out_scr[h, pl.ds(g * chunk, chunk)] = out
            summed = summed + mm(rows_onehot(ids_ref[h, g][:1], TOP_NODES), out)
    summit_in = (summit_factor * summed).astype(BF16)
    summit_in_ref[...] = summit_in
    act = mm(summit_in, summit_weight_ref[...])
    sig = sigmoid(act)
    summit_slope_ref[...] = sig * (1.0 + act * (1.0 - sig))
    summit_out = (act * sig).astype(BF16)
    for g in range(groups):
        for h in range(2):
            lift_scr[h, pl.ds(g * chunk, chunk)] = mm_tn(
                rows_onehot(ids_ref[h, g][:1], TOP_NODES), summit_out
            ).astype(BF16)

    mesh_rows = farpkt_ref.shape[0] - 8
    rows = mesh_rows
    sub = device % subs
    far_tile = jnp.where(sub == 0, tile - 1, jnp.where(sub == subs - 1, tile + 1, tile))
    far_tile = jnp.clip(far_tile, 0, tiles - 1)

    def table(ref):
        pieces = []
        for at in (tile, far_tile):
            for h in range(2):
                pieces.append(ref[h, pl.ds(pl.multiple_of(at * half, half), half)])
        return jnp.concatenate(pieces, axis=0)

    own_fine = farpkt_ref[rows:, :rows].astype(F32)[:1].astype(I32)
    partner_fine = core_ref[half + rows :, :rows].astype(F32)[:1].astype(I32)
    far_fine = farin_ref[rows:, :rows].astype(F32)[:1].astype(I32) + level_rows
    fine = jnp.concatenate([own_fine, partner_fine, far_fine], axis=1)
    members = cols_onehot(fine, 2 * level_rows)
    lifted = mm(members, table(out_scr)) + mm(members, table(lift_scr))
    mids = jnp.concatenate(
        [farpkt_ref[:rows], core_ref[half : half + rows], farin_ref[:rows]], axis=0
    )
    wide = (mids.astype(F32) + lifted).astype(BF16)

    place = slots(source_ref[...], device, core, rows)
    fetched = mm(cols_onehot(place, 3 * rows), wide).astype(BF16)
    pre = mm(fetched, decode_weight_ref[...]) + edges_ref[...].astype(F32)
    sig = sigmoid(pre)
    grid_rows = grid_ref.shape[0]
    raw = target_ref[...]
    aimed = jnp.where(raw >= 0, raw - device * grid_rows, -1)
    summed = mm(rows_onehot(aimed, grid_rows), (pre * sig).astype(BF16))
    update_ref[...] = (grid_ref[...].astype(F32) + decode_factor * summed).astype(BF16)
    incoming = mm(cols_onehot(aimed, grid_rows), cot_ref[...]) * decode_factor
    slope = (incoming * (sig * (1.0 + pre * (1.0 - sig)))).astype(BF16)
    dgrad_ref[...] = mm_tn(fetched, slope)
    gathered = mm(rows_onehot(place, 3 * rows), slope).astype(BF16)
    returned = mm_nt(gathered, decode_weight_ref[...])
    own_ref[...] = returned[:rows]
    partner_ref[...] = returned[rows : 2 * rows]
    far_ref[...] = returned[2 * rows :].astype(BF16)


def level_kernel(
    dev_ref, own_ref, farin_ref, partner_ref, farpkt_ref, core_ref,
    sum_ref, pkt_ref, keep_ref, *, level_rows
):
    core = dev_ref[0] % 2
    rows = own_ref.shape[0]
    half = level_rows // 2
    grad = own_ref[...] + farin_ref[...].astype(F32)
    sum_ref[...] = grad
    own_fine = farpkt_ref[rows:, :rows].astype(F32)[:1].astype(I32)
    partner_fine = core_ref[half + rows :, :rows].astype(F32)[:1].astype(I32)
    partner = partner_ref[...].astype(BF16)
    part = mm(rows_onehot(own_fine, level_rows), grad.astype(BF16)) + mm(
        rows_onehot(partner_fine, level_rows), partner
    )
    first = part[:half]
    second = part[half:]
    keep_ref[...] = jnp.where(core == 0, first, second)
    pkt_ref[:half] = jnp.where(core == 0, second, first).astype(BF16)
    pkt_ref[half:] = partner


def copies_kernel(mine_ref, other_ref, out_ref):
    total = (mine_ref[...].astype(F32) + other_ref[...].astype(F32)).astype(BF16)
    for peer in range(out_ref.shape[0]):
        out_ref[peer] = total


def back_kernel(
    dev_ref,
    mine_ref,
    other_ref,
    level_ref,
    middle_slope_ref,
    summit_in_ref,
    summit_slope_ref,
    ids_ref,
    sum_ref,
    partnerin_ref,
    farpkt_ref,
    fetched_ref,
    slope_ref,
    target_ref,
    dgrad_ref,
    middle_weight_ref,
    summit_weight_ref,
    middle_grad_ref,
    summit_grad_ref,
    send_ref,
    keep_ref,
    grad_scr,
    back_scr,
    *,
    subs,
    level_rows,
    summit_factor,
    middle_factor,
    encode_factor,
):
    device = dev_ref[0]
    core = device % 2
    tile = device // subs
    tiles, half, features = mine_ref.shape
    _, groups, chunk, _ = level_ref.shape
    group = chunk // half
    for g in range(groups):
        for src, which in ((mine_ref, core), (other_ref, 1 - core)):
            grad_scr[which, g] = src[g * group : (g + 1) * group].reshape(chunk, features)
    total = jnp.zeros((TOP_NODES, features), F32)
    for g in range(groups):
        for h in range(2):
            total = total + mm(rows_onehot(ids_ref[h, g][:1], TOP_NODES), grad_scr[h, g])
    summit_slope = (total * summit_slope_ref[...]).astype(BF16)
    summit_grad_ref[...] = mm_tn(summit_in_ref[...], summit_slope)
    summit_back = mm_nt(summit_slope, summit_weight_ref[...]).astype(BF16)
    middle_grad = jnp.zeros((features, features), F32)
    for g in range(groups):
        for h in range(2):
            lifted = mm_tn(rows_onehot(ids_ref[h, g][:1], TOP_NODES), summit_back)
            level_total = grad_scr[h, g].astype(F32) + summit_factor * lifted
            back_scr[h, pl.ds(g * chunk, chunk)] = level_total
            slope = (level_total * middle_slope_ref[h, g].astype(F32)).astype(BF16)
            grad_scr[h, g] = slope
            middle_grad = middle_grad + mm_tn(level_ref[h, g], slope)
    middle_grad_ref[...] = middle_grad
    at = pl.multiple_of(tile * half, half)
    spot = pl.multiple_of((tile % group) * half, half)
    level_total = jnp.concatenate([back_scr[h, pl.ds(at, half)] for h in range(2)], axis=0)
    slope = jnp.concatenate(
        [grad_scr[h, tile // group, pl.ds(spot, half)] for h in range(2)], axis=0
    )
    back = (level_total + mm_nt(slope, middle_weight_ref[...])).astype(BF16)
    rows = sum_ref.shape[0]
    own_fine = farpkt_ref[rows:, :rows].astype(F32)[:1].astype(I32)
    mesh_total = (
        sum_ref[...]
        + partnerin_ref[half:].astype(F32)
        + middle_factor * mm(cols_onehot(own_fine, level_rows), back)
    )
    raw = target_ref[...]
    aimed = jnp.where(raw >= 0, raw - device * rows, -1)
    upstream = mm(cols_onehot(aimed, rows), mesh_total.astype(BF16)) * encode_factor
    slope = (upstream * slope_ref[...].astype(F32)).astype(BF16)
    egrad = mm_tn(fetched_ref[...], slope)
    dgrad = dgrad_ref[...]
    send_ref[...] = jnp.where(core == 0, dgrad, egrad).astype(BF16)
    keep_ref[...] = jnp.where(core == 0, egrad, dgrad)


def call(body, outs, args, scratch=(), **static):
    vmem = pl.BlockSpec(memory_space=pltpu.VMEM)
    smem = pl.BlockSpec(memory_space=pltpu.SMEM)
    specs = [smem if a.ndim == 1 else vmem for a in args]
    single = not isinstance(outs, (list, tuple))
    return pl.pallas_call(
        functools.partial(body, **static),
        out_shape=outs,
        in_specs=specs,
        out_specs=vmem if single else [vmem] * len(outs),
        scratch_shapes=list(scratch),
        compiler_params=pltpu.CompilerParams(vmem_limit_bytes=60 * 1024 * 1024),
        name=body.__name__,
    )(*args)


def shape(dims, dtype):
    return jax.ShapeDtypeStruct(dims, dtype)


def shards(
    grid_feats,
    mesh_feats,
    encode_edges,
    decode_edges,
    encode_source,
    encode_target,
    decode_source,
    decode_target,
    owner_fine,
    owner_coarse,
    encode_weight,
    decode_weight,
    middle_weight,
    summit_weight,
    cotangent,
):
    rows, features = grid_feats.shape
    mesh_rows = mesh_feats.shape[0]
    level_rows = owner_coarse.shape[0]
    half = level_rows // 2
    tiles = lax.axis_size("tile")
    subs = lax.axis_size("row") * lax.axis_size("core")
    devices = tiles * subs
    chips = devices // 2
    edges = encode_source.shape[0]
    swap = [(0, 1), (1, 0)]
    beside = []
    for left in range(1, devices - 1, 2):
        beside += [(left, left + 1), (left + 1, left)]
    device = lax.axis_index(ALL).astype(I32)
    dev = device.reshape(1)
    core = device % 2
    encode_factor = mesh_rows / edges
    decode_factor = rows / decode_source.shape[0]
    middle_factor = level_rows / (mesh_rows * subs)
    summit_factor = TOP_NODES / (level_rows * tiles)
    group = min(features // half, tiles)
    groups = tiles // group
    chunk = group * half

    grid_far = lax.ppermute(grid_feats, ALL, beside)
    grid_partner = lax.ppermute(grid_feats, "core", swap)
    fetched, slope, core_pkt, far_pkt, keep = call(
        encode_kernel,
        [
            shape((edges, features), BF16),
            shape((edges, features), BF16),
            shape((half + mesh_rows + 8, features), BF16),
            shape((mesh_rows + 8, features), BF16),
            shape((half, features), F32),
        ],
        [
            dev,
            grid_feats,
            grid_partner,
            grid_far,
            mesh_feats,
            encode_edges,
            encode_source[None],
            encode_target[None],
            owner_fine[None],
            encode_weight,
        ],
        subs=subs,
        level_rows=level_rows,
        factor=encode_factor,
    )
    core_in = lax.ppermute(core_pkt, "core", swap)
    far_in = lax.ppermute(far_pkt, ALL, beside)
    mine = (keep + core_in[:half].astype(F32)).astype(BF16)
    other = lax.ppermute(mine, "row", swap)
    packed = call(
        spread_kernel,
        shape((tiles, half + 8, features), BF16),
        [dev, mine, other, owner_coarse[None]],
        subs=subs,
        factor=middle_factor,
    )
    mids = lax.all_to_all(packed, "tile", 0, 0)
    mids_other = lax.ppermute(mids, "core", swap)
    full = (2, groups, chunk, features)
    (
        grid_update,
        dgrad,
        own,
        partner,
        far,
        level,
        middle_slope,
        summit_in,
        summit_slope,
        ids,
    ) = call(
        middle_kernel,
        [
            shape((rows, features), BF16),
            shape((features, features), F32),
            shape((mesh_rows, features), F32),
            shape((mesh_rows, features), F32),
            shape((mesh_rows, features), BF16),
            shape(full, BF16),
            shape(full, BF16),
            shape((TOP_NODES, features), BF16),
            shape((TOP_NODES, features), F32),
            shape((2, groups, 8, chunk), I32),
        ],
        [
            dev,
            mids,
            mids_other,
            core_in,
            far_pkt,
            far_in,
            grid_feats,
            cotangent,
            decode_edges,
            decode_source[None],
            decode_target[None],
            decode_weight,
            middle_weight,
            summit_weight,
        ],
        scratch=[
            pltpu.VMEM((2, tiles * half, features), BF16),
            pltpu.VMEM((2, tiles * half, features), BF16),
        ],
        subs=subs,
        level_rows=level_rows,
        summit_factor=summit_factor,
        decode_factor=decode_factor,
    )
    far_back = lax.ppermute(far, ALL, beside)
    grad_sum, core_pkt, keep = call(
        level_kernel,
        [
            shape((mesh_rows, features), F32),
            shape((half + mesh_rows, features), BF16),
            shape((half, features), F32),
        ],
        [dev, own, far_back, partner, far_pkt, core_in],
        level_rows=level_rows,
    )
    back_in = lax.ppermute(core_pkt, "core", swap)
    mine = (keep + back_in[:half].astype(F32)).astype(BF16)
    other = lax.ppermute(mine, "row", swap)
    packed = call(copies_kernel, shape((tiles, half, features), BF16), [mine, other])
    grads = lax.all_to_all(packed, "tile", 0, 0)
    grads_other = lax.ppermute(grads, "core", swap)
    middle_grad, summit_grad, send, keep = call(
        back_kernel,
        [
            shape((features, features), F32),
            shape((features, features), F32),
            shape((features, features), BF16),
            shape((features, features), F32),
        ],
        [
            dev,
            grads,
            grads_other,
            level,
            middle_slope,
            summit_in,
            summit_slope,
            ids,
            grad_sum,
            back_in,
            far_pkt,
            fetched,
            slope,
            encode_target[None],
            dgrad,
            middle_weight,
            summit_weight,
        ],
        scratch=[
            pltpu.VMEM(full, BF16),
            pltpu.VMEM((2, tiles * half, features), F32),
        ],
        subs=subs,
        level_rows=level_rows,
        summit_factor=summit_factor,
        middle_factor=middle_factor,
        encode_factor=encode_factor,
    )
    received = lax.ppermute(send, "core", swap)
    share = (keep + received.astype(F32)).astype(BF16)
    share = share.reshape(chips, features // chips, features)
    parts = lax.all_to_all(share, CHIPS, 0, 0)
    summed = jnp.sum(parts.astype(F32), axis=0).astype(BF16)
    copies = jnp.broadcast_to(summed[None], parts.shape)
    mine = lax.all_to_all(copies, CHIPS, 0, 0).reshape(features, features)
    other = lax.ppermute(mine, "core", swap)
    encode_grad = jnp.where(core == 0, mine, other).astype(F32)
    decode_grad = jnp.where(core == 0, other, mine).astype(F32)
    return (grid_update, encode_grad, decode_grad, middle_grad, summit_grad)


def solution(mesh):
    tiles, subs = mesh.devices.shape
    fine = Mesh(mesh.devices.reshape(tiles, subs // 2, 2), ALL)
    placed = (
        P(ALL, None),
        P(ALL, None),
        P(ALL, None),
        P(ALL, None),
        P(ALL),
        P(ALL),
        P(ALL),
        P(ALL),
        P(ALL),
        P("tile"),
        P(),
        P(),
        P(),
        P(),
        P(ALL, None),
    )
    return jax.shard_map(
        shards,
        mesh=fine,
        in_specs=placed,
        out_specs=(P(ALL, None), P(), P(), P(), P()),
        check_vma=False,
    )
```

```python
import functools

import jax
import jax.numpy as jnp
from jax import lax
from jax.experimental import pallas as pl
from jax.experimental.pallas import tpu as pltpu
from jax.sharding import Mesh, PartitionSpec as P

TOP_NODES = 512
LANES = 128
WORKING_BYTES = 10 * 2**20
ALL = ("tile", "row", "core")
CHIPS = ("tile", "row")
BF16 = jnp.bfloat16
F32 = jnp.float32
I32 = jnp.int32


def mm(left, right):
    return jnp.dot(left, right, preferred_element_type=F32)


def mm_tn(left, right):
    return lax.dot_general(left, right, (((0,), (0,)), ((), ())), preferred_element_type=F32)


def mm_nt(left, right):
    return lax.dot_general(left, right, (((1,), (1,)), ((), ())), preferred_element_type=F32)


def sigmoid(values):
    return 0.5 + 0.5 * jnp.tanh(0.5 * values)


def rows_onehot(ids, rows):
    n = ids.shape[1]
    hit = lax.broadcasted_iota(I32, (rows, n), 0) == ids
    return jnp.where(hit, 1.0, 0.0).astype(BF16)


def column(ids):
    n = ids.shape[1]
    wide = jnp.broadcast_to(ids.astype(F32), (8, n))
    return wide.T[:, :1].astype(I32)


def cols_onehot(ids, cols):
    n = ids.shape[1]
    hit = lax.broadcasted_iota(I32, (n, cols), 1) == column(ids)
    return jnp.where(hit, 1.0, 0.0).astype(BF16)


def coarse_split(ids):
    at = lax.broadcasted_iota(I32, (16, ids.shape[1]), 0)
    parts = jnp.where(at == 0, ids >> 4, jnp.where(at == 1, ids & 15, 0))
    return parts.astype(F32).astype(BF16)


def node_ids(block):
    codes = block.astype(F32)
    return (codes[2:3].astype(I32), (codes[0:1] * 16.0 + codes[1:2]).astype(I32))


def slots(source, device, core, rows):
    rel = source - device * rows
    before = rel < 0
    after = rel >= rows
    shift_before = jnp.where(core == 0, 3 * rows, 2 * rows)
    shift_after = jnp.where(core == 0, 0, rows)
    return rel + jnp.where(before, shift_before, 0) + jnp.where(after, shift_after, 0)


def encode_kernel(
    dev_ref,
    grid_ref,
    partner_ref,
    far_ref,
    mesh_ref,
    edges_ref,
    source_ref,
    target_ref,
    fine_ref,
    coarse_ref,
    weight_ref,
    fetched_ref,
    slope_ref,
    core_ref,
    farpkt_ref,
    keep_ref,
    *,
    subs,
    level_rows,
    factor,
):
    device = dev_ref[0]
    core = device % 2
    rows = grid_ref.shape[0]
    mesh_rows = mesh_ref.shape[0]
    half = level_rows // 2
    picks = cols_onehot(slots(source_ref[...], device, core, rows), 3 * rows)
    fetched = (
        mm(picks[:, :rows], grid_ref[...])
        + mm(picks[:, rows : 2 * rows], partner_ref[...])
        + mm(picks[:, 2 * rows :], far_ref[...])
    ).astype(BF16)
    fetched_ref[...] = fetched
    pre = mm(fetched, weight_ref[...]) + edges_ref[...].astype(F32)
    sig = sigmoid(pre)
    act = (pre * sig).astype(BF16)
    slope_ref[...] = (sig * (1.0 + pre * (1.0 - sig))).astype(BF16)
    raw = target_ref[...]
    aimed = jnp.where(raw >= 0, raw - device * mesh_rows, -1)
    summed = mm(rows_onehot(aimed, mesh_rows), act)
    mid = (mesh_ref[...].astype(F32) + factor * summed).astype(BF16)
    local = fine_ref[...] - (device // subs) * level_rows
    members = rows_onehot(local, level_rows)
    part = mm(members, mid)
    first = part[:half]
    second = part[half:]
    keep_ref[...] = jnp.where(core == 0, first, second)
    core_ref[:half] = jnp.where(core == 0, second, first).astype(BF16)
    core_ref[half : half + mesh_rows] = mid
    farpkt_ref[:mesh_rows] = mid
    features = grid_ref.shape[1]
    spot = (
        lax.broadcasted_iota(I32, (mesh_rows, features), 0)
        == lax.broadcasted_iota(I32, (mesh_rows, features), 1)
    )
    spread = jnp.where(spot, 1.0, 0.0).astype(BF16)
    at = lax.broadcasted_iota(I32, (16, mesh_rows), 0)
    codes = mm(coarse_split(coarse_ref[...]), members)
    codes = jnp.where(at == 2, local.astype(F32), codes)
    fine_rows = mm(codes.astype(BF16), spread).astype(BF16)[:8]
    core_ref[half + mesh_rows :] = fine_rows
    farpkt_ref[mesh_rows:] = fine_rows


def spread_kernel(dev_ref, mine_ref, other_ref, coarse_ref, out_ref, *, subs, factor):
    device = dev_ref[0]
    core = device % 2
    tile = device // subs
    half, features = mine_ref.shape
    group = features // half
    total = mine_ref[...].astype(F32) + other_ref[...].astype(F32)
    mid = (factor * total).astype(BF16)
    level_rows = coarse_ref.shape[1]
    j = lax.broadcasted_iota(I32, (level_rows, features), 0) - core * half
    lane = lax.broadcasted_iota(I32, (level_rows, features), 1) - (tile % group) * half
    sel = (j == lane) & (j >= 0) & (j < half)
    codes = mm(coarse_split(coarse_ref[...]), jnp.where(sel, 1.0, 0.0).astype(BF16))
    lanes = out_ref.shape[2]
    strips = features // lanes
    tail = jnp.concatenate(
        [codes[r : r + 1, i * lanes : (i + 1) * lanes] for r in range(2) for i in range(strips)],
        axis=0,
    ).astype(BF16)
    for peer in range(out_ref.shape[0]):
        for i in range(strips):
            out_ref[peer, i * half : (i + 1) * half] = mid[:, i * lanes : (i + 1) * lanes]
        out_ref[peer, strips * half :] = tail


def middle_kernel(
    dev_ref,
    mine_ref,
    other_ref,
    core_ref,
    farpkt_ref,
    farin_ref,
    grid_ref,
    cot_ref,
    edges_ref,
    source_ref,
    target_ref,
    decode_weight_ref,
    middle_weight_ref,
    summit_weight_ref,
    update_ref,
    dgrad_ref,
    own_ref,
    partner_ref,
    far_ref,
    level_ref,
    middle_slope_ref,
    summit_in_ref,
    summit_slope_ref,
    ids_ref,
    out_scr,
    *,
    subs,
    level_rows,
    summit_factor,
    decode_factor,
):
    device = dev_ref[0]
    core = device % 2
    tile = device // subs
    tiles, _, lanes = mine_ref.shape
    features = grid_ref.shape[1]
    strips = features // lanes
    half = level_rows // 2
    group = min(features // half, tiles)
    groups = tiles // group
    chunk = group * half
    for g in range(groups):
        for src, which in ((mine_ref, core), (other_ref, 1 - core)):
            block = src[g * group : (g + 1) * group]
            for i in range(strips):
                level_ref[which, g, :, i * lanes : (i + 1) * lanes] = block[
                    :, i * half : (i + 1) * half
                ].reshape(chunk, lanes)
            codes = jnp.sum(block[:, strips * half :].astype(F32), axis=0)
            ids = codes[:strips] * 16.0 + codes[strips : 2 * strips]
            ids = jnp.concatenate([ids[i : i + 1] for i in range(strips)], axis=1)
            ids_ref[which, g] = jnp.broadcast_to(ids.astype(I32)[:, :chunk], (8, chunk))
    summed = jnp.zeros((TOP_NODES, features), F32)
    for g in range(groups):
        for h in range(2):
            mid = level_ref[h, g]
            act = mm(mid, middle_weight_ref[...])
            sig = sigmoid(act)
            out = (mid.astype(F32) + act * sig).astype(BF16)
            middle_slope_ref[h, g] = (sig * (1.0 + act * (1.0 - sig))).astype(BF16)
            out_scr[h, pl.ds(g * chunk, chunk)] = out
            summed = summed + mm(rows_onehot(ids_ref[h, g][:1], TOP_NODES), out)
    summit_in = (summit_factor * summed).astype(BF16)
    summit_in_ref[...] = summit_in
    act = mm(summit_in, summit_weight_ref[...])
    sig = sigmoid(act)
    summit_slope_ref[...] = sig * (1.0 + act * (1.0 - sig))
    summit_out = (act * sig).astype(BF16)

    mesh_rows = farpkt_ref.shape[0] - 8
    rows = mesh_rows
    sub = device % subs
    far_tile = jnp.where(sub == 0, tile - 1, jnp.where(sub == subs - 1, tile + 1, tile))
    far_tile = jnp.clip(far_tile, 0, tiles - 1)

    def table(ref):
        pieces = []
        for at in (tile, far_tile):
            for h in range(2):
                pieces.append(ref[h, pl.ds(pl.multiple_of(at * half, half), half)])
        return jnp.concatenate(pieces, axis=0)

    own_fine, own_top = node_ids(farpkt_ref[rows:, :rows])
    partner_fine, partner_top = node_ids(core_ref[half + rows :, :rows])
    far_fine, far_top = node_ids(farin_ref[rows:, :rows])
    fine = jnp.concatenate([own_fine, partner_fine, far_fine + level_rows], axis=1)
    top = jnp.concatenate([own_top, partner_top, far_top], axis=1)
    lifted = mm(cols_onehot(fine, 2 * level_rows), table(out_scr)) + mm(
        cols_onehot(top, TOP_NODES), summit_out
    )
    mids = jnp.concatenate(
        [farpkt_ref[:rows], core_ref[half : half + rows], farin_ref[:rows]], axis=0
    )
    wide = (mids.astype(F32) + lifted).astype(BF16)

    place = slots(source_ref[...], device, core, rows)
    fetched = mm(cols_onehot(place, 3 * rows), wide).astype(BF16)
    pre = mm(fetched, decode_weight_ref[...]) + edges_ref[...].astype(F32)
    sig = sigmoid(pre)
    grid_rows = grid_ref.shape[0]
    raw = target_ref[...]
    aimed = jnp.where(raw >= 0, raw - device * grid_rows, -1)
    summed = mm(rows_onehot(aimed, grid_rows), (pre * sig).astype(BF16))
    update_ref[...] = (grid_ref[...].astype(F32) + decode_factor * summed).astype(BF16)
    incoming = mm(cols_onehot(aimed, grid_rows), cot_ref[...]) * decode_factor
    slope = (incoming * (sig * (1.0 + pre * (1.0 - sig)))).astype(BF16)
    dgrad_ref[...] = mm_tn(fetched, slope)
    gathered = mm(rows_onehot(place, 3 * rows), slope).astype(BF16)
    returned = mm_nt(gathered, decode_weight_ref[...])
    own_ref[...] = returned[:rows]
    partner_ref[...] = returned[rows : 2 * rows]
    far_ref[...] = returned[2 * rows :].astype(BF16)


def level_kernel(
    dev_ref, own_ref, farin_ref, partner_ref, farpkt_ref, core_ref,
    sum_ref, pkt_ref, keep_ref, *, level_rows
):
    core = dev_ref[0] % 2
    rows = own_ref.shape[0]
    half = level_rows // 2
    grad = own_ref[...] + farin_ref[...].astype(F32)
    sum_ref[...] = grad
    own_fine, _ = node_ids(farpkt_ref[rows:, :rows])
    partner_fine, _ = node_ids(core_ref[half + rows :, :rows])
    partner = partner_ref[...].astype(BF16)
    part = mm(rows_onehot(own_fine, level_rows), grad.astype(BF16)) + mm(
        rows_onehot(partner_fine, level_rows), partner
    )
    first = part[:half]
    second = part[half:]
    keep_ref[...] = jnp.where(core == 0, first, second)
    pkt_ref[:half] = jnp.where(core == 0, second, first).astype(BF16)
    pkt_ref[half:] = partner


def back_kernel(
    dev_ref,
    mine_ref,
    other_ref,
    level_ref,
    middle_slope_ref,
    summit_in_ref,
    summit_slope_ref,
    ids_ref,
    sum_ref,
    partnerin_ref,
    farpkt_ref,
    fetched_ref,
    slope_ref,
    target_ref,
    dgrad_ref,
    middle_weight_ref,
    summit_weight_ref,
    middle_grad_ref,
    summit_grad_ref,
    send_ref,
    keep_ref,
    grad_scr,
    back_scr,
    *,
    subs,
    level_rows,
    summit_factor,
    middle_factor,
    encode_factor,
):
    device = dev_ref[0]
    core = device % 2
    tile = device // subs
    tiles, half, features = mine_ref.shape
    _, groups, chunk, _ = level_ref.shape
    group = chunk // half
    for g in range(groups):
        for src, which in ((mine_ref, core), (other_ref, 1 - core)):
            grad_scr[which, g] = src[g * group : (g + 1) * group].reshape(chunk, features)
    total = jnp.zeros((TOP_NODES, features), F32)
    for g in range(groups):
        for h in range(2):
            total = total + mm(rows_onehot(ids_ref[h, g][:1], TOP_NODES), grad_scr[h, g])
    summit_slope = (total * summit_slope_ref[...]).astype(BF16)
    summit_grad_ref[...] = mm_tn(summit_in_ref[...], summit_slope)
    summit_back = mm_nt(summit_slope, summit_weight_ref[...]).astype(BF16)
    middle_grad = jnp.zeros((features, features), F32)
    for g in range(groups):
        for h in range(2):
            lifted = mm_tn(rows_onehot(ids_ref[h, g][:1], TOP_NODES), summit_back)
            level_total = grad_scr[h, g].astype(F32) + summit_factor * lifted
            back_scr[h, pl.ds(g * chunk, chunk)] = level_total
            slope = (level_total * middle_slope_ref[h, g].astype(F32)).astype(BF16)
            grad_scr[h, g] = slope
            middle_grad = middle_grad + mm_tn(level_ref[h, g], slope)
    middle_grad_ref[...] = middle_grad
    at = pl.multiple_of(tile * half, half)
    spot = pl.multiple_of((tile % group) * half, half)
    level_total = jnp.concatenate([back_scr[h, pl.ds(at, half)] for h in range(2)], axis=0)
    slope = jnp.concatenate(
        [grad_scr[h, tile // group, pl.ds(spot, half)] for h in range(2)], axis=0
    )
    back = (level_total + mm_nt(slope, middle_weight_ref[...])).astype(BF16)
    rows = sum_ref.shape[0]
    own_fine, _ = node_ids(farpkt_ref[rows:, :rows])
    mesh_total = (
        sum_ref[...]
        + partnerin_ref[half:].astype(F32)
        + middle_factor * mm(cols_onehot(own_fine, level_rows), back)
    )
    raw = target_ref[...]
    aimed = jnp.where(raw >= 0, raw - device * rows, -1)
    upstream = mm(cols_onehot(aimed, rows), mesh_total.astype(BF16)) * encode_factor
    slope = (upstream * slope_ref[...].astype(F32)).astype(BF16)
    egrad = mm_tn(fetched_ref[...], slope)
    dgrad = dgrad_ref[...]
    send_ref[...] = jnp.where(core == 0, dgrad, egrad).astype(BF16)
    keep_ref[...] = jnp.where(core == 0, egrad, dgrad)


def call(body, outs, args, scratch=(), **static):
    vmem = pl.BlockSpec(memory_space=pltpu.VMEM)
    smem = pl.BlockSpec(memory_space=pltpu.SMEM)
    specs = [smem if a.ndim == 1 else vmem for a in args]
    single = not isinstance(outs, (list, tuple))
    held = [a for a in args if a.ndim > 1] + ([outs] if single else list(outs)) + list(scratch)
    limit = sum(a.size * a.dtype.itemsize for a in held) + WORKING_BYTES
    limit = min(limit, 60 * 2**20)
    return pl.pallas_call(
        functools.partial(body, **static),
        out_shape=outs,
        in_specs=specs,
        out_specs=vmem if single else [vmem] * len(outs),
        scratch_shapes=[pltpu.VMEM(s.shape, s.dtype) for s in scratch],
        compiler_params=pltpu.CompilerParams(vmem_limit_bytes=limit),
        name=body.__name__,
    )(*args)


def shape(dims, dtype):
    return jax.ShapeDtypeStruct(dims, dtype)


def shards(
    grid_feats,
    mesh_feats,
    encode_edges,
    decode_edges,
    encode_source,
    encode_target,
    decode_source,
    decode_target,
    owner_fine,
    owner_coarse,
    encode_weight,
    decode_weight,
    middle_weight,
    summit_weight,
    cotangent,
):
    rows, features = grid_feats.shape
    mesh_rows = mesh_feats.shape[0]
    level_rows = owner_coarse.shape[0]
    half = level_rows // 2
    tiles = lax.axis_size("tile")
    subs = lax.axis_size("row") * lax.axis_size("core")
    devices = tiles * subs
    chips = devices // 2
    edges = encode_source.shape[0]
    swap = [(0, 1), (1, 0)]
    beside = []
    for left in range(1, devices - 1, 2):
        beside += [(left, left + 1), (left + 1, left)]
    device = lax.axis_index(ALL).astype(I32)
    dev = device.reshape(1)
    core = device % 2
    encode_factor = mesh_rows / edges
    decode_factor = rows / decode_source.shape[0]
    middle_factor = level_rows / (mesh_rows * subs)
    summit_factor = TOP_NODES / (level_rows * tiles)
    group = min(features // half, tiles)
    groups = tiles // group
    chunk = group * half

    grid_far = lax.ppermute(grid_feats, ALL, beside)
    grid_partner = lax.ppermute(grid_feats, "core", swap)
    fetched, slope, core_pkt, far_pkt, keep = call(
        encode_kernel,
        [
            shape((edges, features), BF16),
            shape((edges, features), BF16),
            shape((half + mesh_rows + 8, features), BF16),
            shape((mesh_rows + 8, features), BF16),
            shape((half, features), F32),
        ],
        [
            dev,
            grid_feats,
            grid_partner,
            grid_far,
            mesh_feats,
            encode_edges,
            encode_source[None],
            encode_target[None],
            owner_fine[None],
            owner_coarse[None],
            encode_weight,
        ],
        subs=subs,
        level_rows=level_rows,
        factor=encode_factor,
    )
    core_in = lax.ppermute(core_pkt, "core", swap)
    far_in = lax.ppermute(far_pkt, ALL, beside)
    mine = (keep + core_in[:half].astype(F32)).astype(BF16)
    other = lax.ppermute(mine, "row", swap)
    packed = call(
        spread_kernel,
        shape((tiles, (features // LANES) * half + 8, LANES), BF16),
        [dev, mine, other, owner_coarse[None]],
        subs=subs,
        factor=middle_factor,
    )
    mids = lax.all_to_all(packed, "tile", 0, 0)
    mids_other = lax.ppermute(mids, "core", swap)
    full = (2, groups, chunk, features)
    (
        grid_update,
        dgrad,
        own,
        partner,
        far,
        level,
        middle_slope,
        summit_in,
        summit_slope,
        ids,
    ) = call(
        middle_kernel,
        [
            shape((rows, features), BF16),
            shape((features, features), F32),
            shape((mesh_rows, features), F32),
            shape((mesh_rows, features), F32),
            shape((mesh_rows, features), BF16),
            shape(full, BF16),
            shape(full, BF16),
            shape((TOP_NODES, features), BF16),
            shape((TOP_NODES, features), F32),
            shape((2, groups, 8, chunk), I32),
        ],
        [
            dev,
            mids,
            mids_other,
            core_in,
            far_pkt,
            far_in,
            grid_feats,
            cotangent,
            decode_edges,
            decode_source[None],
            decode_target[None],
            decode_weight,
            middle_weight,
            summit_weight,
        ],
        scratch=[
            shape((2, tiles * half, features), BF16),
        ],
        subs=subs,
        level_rows=level_rows,
        summit_factor=summit_factor,
        decode_factor=decode_factor,
    )
    far_back = lax.ppermute(far, ALL, beside)
    grad_sum, core_pkt, keep = call(
        level_kernel,
        [
            shape((mesh_rows, features), F32),
            shape((half + mesh_rows, features), BF16),
            shape((half, features), F32),
        ],
        [dev, own, far_back, partner, far_pkt, core_in],
        level_rows=level_rows,
    )
    back_in = lax.ppermute(core_pkt, "core", swap)
    mine = (keep + back_in[:half].astype(F32)).astype(BF16)
    other = lax.ppermute(mine, "row", swap)
    total = (mine.astype(F32) + other.astype(F32)).astype(BF16)
    packed = jnp.broadcast_to(total[None], (tiles, half, features))
    grads = lax.all_to_all(packed, "tile", 0, 0)
    grads_other = lax.ppermute(grads, "core", swap)
    middle_grad, summit_grad, send, keep = call(
        back_kernel,
        [
            shape((features, features), F32),
            shape((features, features), F32),
            shape((features, features), BF16),
            shape((features, features), F32),
        ],
        [
            dev,
            grads,
            grads_other,
            level,
            middle_slope,
            summit_in,
            summit_slope,
            ids,
            grad_sum,
            back_in,
            far_pkt,
            fetched,
            slope,
            encode_target[None],
            dgrad,
            middle_weight,
            summit_weight,
        ],
        scratch=[
            shape(full, BF16),
            shape((2, tiles * half, features), F32),
        ],
        subs=subs,
        level_rows=level_rows,
        summit_factor=summit_factor,
        middle_factor=middle_factor,
        encode_factor=encode_factor,
    )
    received = lax.ppermute(send, "core", swap)
    share = (keep + received.astype(F32)).astype(BF16)
    share = share.reshape(chips, features // chips, features)
    parts = lax.all_to_all(share, CHIPS, 0, 0)
    summed = jnp.sum(parts.astype(F32), axis=0).astype(BF16)
    copies = jnp.broadcast_to(summed[None], parts.shape)
    mine = lax.all_to_all(copies, CHIPS, 0, 0).reshape(features, features)
    other = lax.ppermute(mine, "core", swap)
    encode_grad = jnp.where(core == 0, mine, other).astype(F32)
    decode_grad = jnp.where(core == 0, other, mine).astype(F32)
    return (grid_update, encode_grad, decode_grad, middle_grad, summit_grad)


def solution(mesh):
    tiles, subs = mesh.devices.shape
    fine = Mesh(mesh.devices.reshape(tiles, subs // 2, 2), ALL)
    placed = (
        P(ALL, None),
        P(ALL, None),
        P(ALL, None),
        P(ALL, None),
        P(ALL),
        P(ALL),
        P(ALL),
        P(ALL),
        P(ALL),
        P("tile"),
        P(),
        P(),
        P(),
        P(),
        P(ALL, None),
    )
    return jax.shard_map(
        shards,
        mesh=fine,
        in_specs=placed,
        out_specs=(P(ALL, None), P(), P(), P(), P()),
        check_vma=False,
    )
```

```python
import functools

import jax
import jax.numpy as jnp
from jax import lax
from jax.experimental import pallas as pl
from jax.experimental.pallas import tpu as pltpu
from jax.sharding import Mesh, PartitionSpec as P


TOP_NODES = 512
LANES = 128
WORKING_BYTES = 10 * 2**20
ALL = ("tile", "row", "core")
CHIPS = ("tile", "row")
BF16 = jnp.bfloat16
F32 = jnp.float32
I32 = jnp.int32


def mm(left, right):
    return jnp.dot(left, right, preferred_element_type=F32)


def mm_tn(left, right):
    return lax.dot_general(left, right, (((0,), (0,)), ((), ())), preferred_element_type=F32)


def mm_nt(left, right):
    return lax.dot_general(left, right, (((1,), (1,)), ((), ())), preferred_element_type=F32)


def sigmoid(values):
    return 0.5 + 0.5 * jnp.tanh(0.5 * values)


def rows_onehot(ids, rows):
    n = ids.shape[1]
    hit = lax.broadcasted_iota(I32, (rows, n), 0) == ids
    return jnp.where(hit, 1.0, 0.0).astype(BF16)


def column(ids):
    n = ids.shape[1]
    wide = jnp.broadcast_to(ids.astype(F32), (8, n))
    return wide.T[:, :1].astype(I32)


def cols_onehot(ids, cols):
    n = ids.shape[1]
    hit = lax.broadcasted_iota(I32, (n, cols), 1) == column(ids)
    return jnp.where(hit, 1.0, 0.0).astype(BF16)


def coarse_split(ids):
    at = lax.broadcasted_iota(I32, (16, ids.shape[1]), 0)
    parts = jnp.where(at == 0, ids >> 4, jnp.where(at == 1, ids & 15, 0))
    return parts.astype(F32).astype(BF16)


def node_ids(block):
    codes = block.astype(F32)
    return (codes[2:3].astype(I32), (codes[0:1] * 16.0 + codes[1:2]).astype(I32))


def slots(source, device, core, rows):
    rel = source - device * rows
    before = rel < 0
    after = rel >= rows
    shift_before = jnp.where(core == 0, 3 * rows, 2 * rows)
    shift_after = jnp.where(core == 0, 0, rows)
    return rel + jnp.where(before, shift_before, 0) + jnp.where(after, shift_after, 0)


def ready_kernel(
    dev_ref,
    grid_ref,
    edges_ref,
    weight_ref,
    source_ref,
    target_ref,
    fine_ref,
    coarse_ref,
    edges_out_ref,
    weight_out_ref,
    own_ref,
    picks_ref,
    aims_ref,
    members_ref,
    nodes_ref,
    *,
    subs,
):
    device = dev_ref[0]
    rows, features = grid_ref.shape
    mesh_rows = fine_ref.shape[1]
    level_rows = coarse_ref.shape[1]
    picks = cols_onehot(slots(source_ref[...], device, device % 2, rows), 3 * rows)
    picks_ref[...] = picks[:, rows:]
    raw = target_ref[...]
    aimed = jnp.where(raw >= 0, raw - device * mesh_rows, -1)
    aims_ref[...] = rows_onehot(aimed, mesh_rows)
    local = fine_ref[...] - (device // subs) * level_rows
    members = rows_onehot(local, level_rows)
    members_ref[...] = members
    spot = (
        lax.broadcasted_iota(I32, (mesh_rows, features), 0)
        == lax.broadcasted_iota(I32, (mesh_rows, features), 1)
    )
    spread = jnp.where(spot, 1.0, 0.0).astype(BF16)
    at = lax.broadcasted_iota(I32, (16, mesh_rows), 0)
    codes = mm(coarse_split(coarse_ref[...]), members)
    codes = jnp.where(at == 2, local.astype(F32), codes)
    nodes_ref[...] = mm(codes.astype(BF16), spread).astype(BF16)[:8]
    own_ref[...] = mm(picks[:, :rows], grid_ref[...]).astype(BF16)
    edges_out_ref[...] = edges_ref[...]
    weight_out_ref[...] = weight_ref[...]


def encode_kernel(
    dev_ref,
    partner_ref,
    far_ref,
    mesh_ref,
    edges_ref,
    weight_ref,
    own_ref,
    picks_ref,
    aims_ref,
    members_ref,
    nodes_ref,
    fetched_ref,
    slope_ref,
    core_ref,
    farpkt_ref,
    keep_ref,
    *,
    factor,
):
    core = dev_ref[0] % 2
    mesh_rows = mesh_ref.shape[0]
    half = keep_ref.shape[0]
    others = jnp.concatenate([partner_ref[...], far_ref[...]], axis=0)
    fetched = (own_ref[...].astype(F32) + mm(picks_ref[...], others)).astype(BF16)
    fetched_ref[...] = fetched
    pre = mm(fetched, weight_ref[...]) + edges_ref[...].astype(F32)
    sig = sigmoid(pre)
    act = (pre * sig).astype(BF16)
    slope_ref[...] = (sig * (1.0 + pre * (1.0 - sig))).astype(BF16)
    summed = mm(aims_ref[...], act)
    mid = (mesh_ref[...].astype(F32) + factor * summed).astype(BF16)
    part = mm(members_ref[...], mid)
    first = part[:half]
    second = part[half:]
    keep_ref[...] = jnp.where(core == 0, first, second)
    core_ref[:half] = jnp.where(core == 0, second, first).astype(BF16)
    core_ref[half : half + mesh_rows] = mid
    core_ref[half + mesh_rows :] = nodes_ref[...]
    farpkt_ref[:mesh_rows] = mid
    farpkt_ref[mesh_rows:] = nodes_ref[...]


def spread_kernel(dev_ref, mine_ref, other_ref, coarse_ref, out_ref, *, subs, factor):
    device = dev_ref[0]
    core = device % 2
    tile = device // subs
    half, features = mine_ref.shape
    group = features // half
    total = mine_ref[...].astype(F32) + other_ref[...].astype(F32)
    mid = (factor * total).astype(BF16)
    level_rows = coarse_ref.shape[1]
    j = lax.broadcasted_iota(I32, (level_rows, features), 0) - core * half
    lane = lax.broadcasted_iota(I32, (level_rows, features), 1) - (tile % group) * half
    sel = (j == lane) & (j >= 0) & (j < half)
    codes = mm(coarse_split(coarse_ref[...]), jnp.where(sel, 1.0, 0.0).astype(BF16))
    lanes = out_ref.shape[2]
    strips = features // lanes
    tail = jnp.concatenate(
        [codes[r : r + 1, i * lanes : (i + 1) * lanes] for r in range(2) for i in range(strips)],
        axis=0,
    ).astype(BF16)
    for peer in range(out_ref.shape[0]):
        for i in range(strips):
            out_ref[peer, i * half : (i + 1) * half] = mid[:, i * lanes : (i + 1) * lanes]
        out_ref[peer, strips * half :] = tail


def middle_kernel(
    dev_ref,
    mine_ref,
    other_ref,
    core_ref,
    farpkt_ref,
    farin_ref,
    grid_ref,
    cot_ref,
    edges_ref,
    source_ref,
    target_ref,
    decode_weight_ref,
    middle_weight_ref,
    summit_weight_ref,
    update_ref,
    dgrad_ref,
    own_ref,
    partner_ref,
    far_ref,
    level_ref,
    middle_slope_ref,
    summit_in_ref,
    summit_slope_ref,
    ids_ref,
    out_scr,
    *,
    subs,
    level_rows,
    summit_factor,
    decode_factor,
):
    device = dev_ref[0]
    core = device % 2
    tile = device // subs
    tiles, _, lanes = mine_ref.shape
    features = grid_ref.shape[1]
    strips = features // lanes
    half = level_rows // 2
    group = min(features // half, tiles)
    groups = tiles // group
    chunk = group * half
    for g in range(groups):
        for src, which in ((mine_ref, core), (other_ref, 1 - core)):
            block = src[g * group : (g + 1) * group]
            for i in range(strips):
                level_ref[which, g, :, i * lanes : (i + 1) * lanes] = block[
                    :, i * half : (i + 1) * half
                ].reshape(chunk, lanes)
            codes = jnp.sum(block[:, strips * half :].astype(F32), axis=0)
            ids = codes[:strips] * 16.0 + codes[strips : 2 * strips]
            ids = jnp.concatenate([ids[i : i + 1] for i in range(strips)], axis=1)
            ids_ref[which, g] = jnp.broadcast_to(ids.astype(I32)[:, :chunk], (8, chunk))
    summed = jnp.zeros((TOP_NODES, features), F32)
    for g in range(groups):
        for h in range(2):
            mid = level_ref[h, g]
            act = mm(mid, middle_weight_ref[...])
            sig = sigmoid(act)
            out = (mid.astype(F32) + act * sig).astype(BF16)
            middle_slope_ref[h, g] = (sig * (1.0 + act * (1.0 - sig))).astype(BF16)
            out_scr[h, pl.ds(g * chunk, chunk)] = out
            summed = summed + mm(rows_onehot(ids_ref[h, g][:1], TOP_NODES), out)
    summit_in = (summit_factor * summed).astype(BF16)
    summit_in_ref[...] = summit_in
    act = mm(summit_in, summit_weight_ref[...])
    sig = sigmoid(act)
    summit_slope_ref[...] = sig * (1.0 + act * (1.0 - sig))
    summit_out = (act * sig).astype(BF16)

    mesh_rows = farpkt_ref.shape[0] - 8
    rows = mesh_rows
    sub = device % subs
    far_tile = jnp.where(sub == 0, tile - 1, jnp.where(sub == subs - 1, tile + 1, tile))
    far_tile = jnp.clip(far_tile, 0, tiles - 1)

    def table(ref):
        pieces = []
        for at in (tile, far_tile):
            for h in range(2):
                pieces.append(ref[h, pl.ds(pl.multiple_of(at * half, half), half)])
        return jnp.concatenate(pieces, axis=0)

    own_fine, own_top = node_ids(farpkt_ref[rows:, :rows])
    partner_fine, partner_top = node_ids(core_ref[half + rows :, :rows])
    far_fine, far_top = node_ids(farin_ref[rows:, :rows])
    fine = jnp.concatenate([own_fine, partner_fine, far_fine + level_rows], axis=1)
    top = jnp.concatenate([own_top, partner_top, far_top], axis=1)
    lifted = mm(cols_onehot(fine, 2 * level_rows), table(out_scr)) + mm(
        cols_onehot(top, TOP_NODES), summit_out
    )
    mids = jnp.concatenate(
        [farpkt_ref[:rows], core_ref[half : half + rows], farin_ref[:rows]], axis=0
    )
    wide = (mids.astype(F32) + lifted).astype(BF16)

    place = slots(source_ref[...], device, core, rows)
    fetched = mm(cols_onehot(place, 3 * rows), wide).astype(BF16)
    pre = mm(fetched, decode_weight_ref[...]) + edges_ref[...].astype(F32)
    sig = sigmoid(pre)
    grid_rows = grid_ref.shape[0]
    raw = target_ref[...]
    aimed = jnp.where(raw >= 0, raw - device * grid_rows, -1)
    summed = mm(rows_onehot(aimed, grid_rows), (pre * sig).astype(BF16))
    update_ref[...] = (grid_ref[...].astype(F32) + decode_factor * summed).astype(BF16)
    incoming = mm(cols_onehot(aimed, grid_rows), cot_ref[...]) * decode_factor
    slope = (incoming * (sig * (1.0 + pre * (1.0 - sig)))).astype(BF16)
    dgrad_ref[...] = mm_tn(fetched, slope)
    gathered = mm(rows_onehot(place, 3 * rows), slope).astype(BF16)
    returned = mm_nt(gathered, decode_weight_ref[...])
    own_ref[...] = returned[:rows]
    partner_ref[...] = returned[rows : 2 * rows]
    far_ref[...] = returned[2 * rows :].astype(BF16)


def level_kernel(
    dev_ref, own_ref, farin_ref, partner_ref, farpkt_ref, core_ref,
    sum_ref, pkt_ref, keep_ref, *, level_rows
):
    core = dev_ref[0] % 2
    rows = own_ref.shape[0]
    half = level_rows // 2
    grad = own_ref[...] + farin_ref[...].astype(F32)
    sum_ref[...] = grad
    own_fine, _ = node_ids(farpkt_ref[rows:, :rows])
    partner_fine, _ = node_ids(core_ref[half + rows :, :rows])
    partner = partner_ref[...].astype(BF16)
    part = mm(rows_onehot(own_fine, level_rows), grad.astype(BF16)) + mm(
        rows_onehot(partner_fine, level_rows), partner
    )
    first = part[:half]
    second = part[half:]
    keep_ref[...] = jnp.where(core == 0, first, second)
    pkt_ref[:half] = jnp.where(core == 0, second, first).astype(BF16)
    pkt_ref[half:] = partner


def back_kernel(
    dev_ref,
    mine_ref,
    other_ref,
    middle_slope_ref,
    summit_slope_ref,
    ids_ref,
    sum_ref,
    partnerin_ref,
    farpkt_ref,
    coarse_ref,
    fetched_ref,
    slope_ref,
    target_ref,
    dgrad_ref,
    middle_weight_ref,
    summit_weight_ref,
    send_ref,
    keep_ref,
    grad_ref,
    top_ref,
    top_back_ref,
    *,
    subs,
    level_rows,
    summit_factor,
    middle_factor,
    encode_factor,
):
    device = dev_ref[0]
    core = device % 2
    tile = device // subs
    _, half, features = mine_ref.shape
    _, groups, chunk, _ = grad_ref.shape
    group = chunk // half
    for g in range(groups):
        for src, which in ((mine_ref, core), (other_ref, 1 - core)):
            grad_ref[which, g] = src[g * group : (g + 1) * group].reshape(chunk, features)
    total = jnp.zeros((TOP_NODES, features), F32)
    for g in range(groups):
        for h in range(2):
            total = total + mm(rows_onehot(ids_ref[h, g][:1], TOP_NODES), grad_ref[h, g])
    summit_slope = (total * summit_slope_ref[...]).astype(BF16)
    top_ref[...] = summit_slope
    summit_back = mm_nt(summit_slope, summit_weight_ref[...]).astype(BF16)
    top_back_ref[...] = summit_back
    spot = pl.multiple_of((tile % group) * half, half)

    def own(ref):
        pieces = [ref[h, tile // group, pl.ds(spot, half)] for h in range(2)]
        return jnp.concatenate(pieces, axis=0).astype(F32)

    level_total = own(grad_ref) + summit_factor * mm(
        cols_onehot(coarse_ref[...], TOP_NODES), summit_back
    )
    slope = (level_total * own(middle_slope_ref)).astype(BF16)
    back = (level_total + mm_nt(slope, middle_weight_ref[...])).astype(BF16)
    rows = sum_ref.shape[0]
    own_fine, _ = node_ids(farpkt_ref[rows:, :rows])
    mesh_total = (
        sum_ref[...]
        + partnerin_ref[half:].astype(F32)
        + middle_factor * mm(cols_onehot(own_fine, level_rows), back)
    )
    raw = target_ref[...]
    aimed = jnp.where(raw >= 0, raw - device * rows, -1)
    upstream = mm(cols_onehot(aimed, rows), mesh_total.astype(BF16)) * encode_factor
    slope = (upstream * slope_ref[...].astype(F32)).astype(BF16)
    egrad = mm_tn(fetched_ref[...], slope)
    dgrad = dgrad_ref[...]
    send_ref[...] = jnp.where(core == 0, dgrad, egrad).astype(BF16)
    keep_ref[...] = jnp.where(core == 0, egrad, dgrad)


def late_kernel(
    dev_ref,
    grad_ref,
    level_ref,
    middle_slope_ref,
    summit_in_ref,
    top_ref,
    top_back_ref,
    ids_ref,
    middle_grad_ref,
    summit_grad_ref,
    *,
    summit_factor,
):
    _, groups, _, features = grad_ref.shape
    summit_grad_ref[...] = mm_tn(summit_in_ref[...], top_ref[...])
    middle_grad = jnp.zeros((features, features), F32)
    for g in range(groups):
        for h in range(2):
            lifted = mm_tn(rows_onehot(ids_ref[h, g][:1], TOP_NODES), top_back_ref[...])
            level_total = grad_ref[h, g].astype(F32) + summit_factor * lifted
            slope = (level_total * middle_slope_ref[h, g].astype(F32)).astype(BF16)
            middle_grad = middle_grad + mm_tn(level_ref[h, g], slope)
    middle_grad_ref[...] = middle_grad


def call(body, outs, args, scratch=(), **static):
    vmem = pl.BlockSpec(memory_space=pltpu.VMEM)
    smem = pl.BlockSpec(memory_space=pltpu.SMEM)
    specs = [smem if a.ndim == 1 else vmem for a in args]
    single = not isinstance(outs, (list, tuple))
    held = [a for a in args if a.ndim > 1] + ([outs] if single else list(outs)) + list(scratch)
    limit = sum(a.size * a.dtype.itemsize for a in held) + WORKING_BYTES
    limit = min(limit, 60 * 2**20)
    return pl.pallas_call(
        functools.partial(body, **static),
        out_shape=outs,
        in_specs=specs,
        out_specs=vmem if single else [vmem] * len(outs),
        scratch_shapes=[pltpu.VMEM(s.shape, s.dtype) for s in scratch],
        compiler_params=pltpu.CompilerParams(vmem_limit_bytes=limit),
    )(*args)


def shape(dims, dtype):
    return jax.ShapeDtypeStruct(dims, dtype)


def shards(
    grid_feats,
    mesh_feats,
    encode_edges,
    decode_edges,
    encode_source,
    encode_target,
    decode_source,
    decode_target,
    owner_fine,
    owner_coarse,
    encode_weight,
    decode_weight,
    middle_weight,
    summit_weight,
    cotangent,
):
    rows, features = grid_feats.shape
    mesh_rows = mesh_feats.shape[0]
    level_rows = owner_coarse.shape[0]
    half = level_rows // 2
    tiles = lax.axis_size("tile")
    subs = lax.axis_size("row") * lax.axis_size("core")
    devices = tiles * subs
    chips = devices // 2
    edges = encode_source.shape[0]
    swap = [(0, 1), (1, 0)]
    beside = []
    for left in range(1, devices - 1, 2):
        beside += [(left, left + 1), (left + 1, left)]
    device = lax.axis_index(ALL).astype(I32)
    dev = device.reshape(1)
    core = device % 2
    encode_factor = mesh_rows / edges
    decode_factor = rows / decode_source.shape[0]
    middle_factor = level_rows / (mesh_rows * subs)
    summit_factor = TOP_NODES / (level_rows * tiles)
    group = min(features // half, tiles)
    groups = tiles // group
    chunk = group * half

    grid_far = lax.ppermute(grid_feats, ALL, beside)
    grid_partner = lax.ppermute(grid_feats, "core", swap)
    edges_in, weight_in, own_rows, picks, aims, members, nodes = call(
        ready_kernel,
        [
            shape((edges, features), BF16),
            shape((features, features), BF16),
            shape((edges, features), BF16),
            shape((edges, 2 * rows), BF16),
            shape((mesh_rows, edges), BF16),
            shape((level_rows, mesh_rows), BF16),
            shape((8, features), BF16),
        ],
        [
            dev,
            grid_feats,
            encode_edges,
            encode_weight,
            encode_source[None],
            encode_target[None],
            owner_fine[None],
            owner_coarse[None],
        ],
        subs=subs,
    )
    fetched, slope, core_pkt, far_pkt, keep = call(
        encode_kernel,
        [
            shape((edges, features), BF16),
            shape((edges, features), BF16),
            shape((half + mesh_rows + 8, features), BF16),
            shape((mesh_rows + 8, features), BF16),
            shape((half, features), F32),
        ],
        [
            dev,
            grid_partner,
            grid_far,
            mesh_feats,
            edges_in,
            weight_in,
            own_rows,
            picks,
            aims,
            members,
            nodes,
        ],
        factor=encode_factor,
    )
    core_in = lax.ppermute(core_pkt, "core", swap)
    far_in = lax.ppermute(far_pkt, ALL, beside)
    mine = (keep + core_in[:half].astype(F32)).astype(BF16)
    other = lax.ppermute(mine, "row", swap)
    packed = call(
        spread_kernel,
        shape((tiles, (features // LANES) * half + 8, LANES), BF16),
        [dev, mine, other, owner_coarse[None]],
        subs=subs,
        factor=middle_factor,
    )
    mids = lax.all_to_all(packed, "tile", 0, 0)
    mids_other = lax.ppermute(mids, "core", swap)
    full = (2, groups, chunk, features)
    (
        grid_update,
        dgrad,
        own,
        partner,
        far,
        level,
        middle_slope,
        summit_in,
        summit_slope,
        ids,
    ) = call(
        middle_kernel,
        [
            shape((rows, features), BF16),
            shape((features, features), F32),
            shape((mesh_rows, features), F32),
            shape((mesh_rows, features), F32),
            shape((mesh_rows, features), BF16),
            shape(full, BF16),
            shape(full, BF16),
            shape((TOP_NODES, features), BF16),
            shape((TOP_NODES, features), F32),
            shape((2, groups, 8, chunk), I32),
        ],
        [
            dev,
            mids,
            mids_other,
            core_in,
            far_pkt,
            far_in,
            grid_feats,
            cotangent,
            decode_edges,
            decode_source[None],
            decode_target[None],
            decode_weight,
            middle_weight,
            summit_weight,
        ],
        scratch=[
            shape((2, tiles * half, features), BF16),
        ],
        subs=subs,
        level_rows=level_rows,
        summit_factor=summit_factor,
        decode_factor=decode_factor,
    )
    far_back = lax.ppermute(far, ALL, beside)
    grad_sum, core_pkt, keep = call(
        level_kernel,
        [
            shape((mesh_rows, features), F32),
            shape((half + mesh_rows, features), BF16),
            shape((half, features), F32),
        ],
        [dev, own, far_back, partner, far_pkt, core_in],
        level_rows=level_rows,
    )
    back_in = lax.ppermute(core_pkt, "core", swap)
    mine = (keep + back_in[:half].astype(F32)).astype(BF16)
    other = lax.ppermute(mine, "row", swap)
    total = (mine.astype(F32) + other.astype(F32)).astype(BF16)
    packed = jnp.broadcast_to(total[None], (tiles, half, features))
    grads = lax.all_to_all(packed, "tile", 0, 0)
    grads_other = lax.ppermute(grads, "core", swap)
    send, keep, level_back, top, top_back = call(
        back_kernel,
        [
            shape((features, features), BF16),
            shape((features, features), F32),
            shape(full, BF16),
            shape((TOP_NODES, features), BF16),
            shape((TOP_NODES, features), BF16),
        ],
        [
            dev,
            grads,
            grads_other,
            middle_slope,
            summit_slope,
            ids,
            grad_sum,
            back_in,
            far_pkt,
            owner_coarse[None],
            fetched,
            slope,
            encode_target[None],
            dgrad,
            middle_weight,
            summit_weight,
        ],
        subs=subs,
        level_rows=level_rows,
        summit_factor=summit_factor,
        middle_factor=middle_factor,
        encode_factor=encode_factor,
    )
    received = lax.ppermute(send, "core", swap)
    middle_grad, summit_grad = call(
        late_kernel,
        [shape((features, features), F32), shape((features, features), F32)],
        [dev, level_back, level, middle_slope, summit_in, top, top_back, ids],
        summit_factor=summit_factor,
    )
    share = (keep + received.astype(F32)).astype(BF16)
    share = share.reshape(chips, features // chips, features)
    parts = lax.all_to_all(share, CHIPS, 0, 0)
    summed = jnp.sum(parts.astype(F32), axis=0).astype(BF16)
    copies = jnp.broadcast_to(summed[None], parts.shape)
    mine = lax.all_to_all(copies, CHIPS, 0, 0).reshape(features, features)
    other = lax.ppermute(mine, "core", swap)
    encode_grad = jnp.where(core == 0, mine, other).astype(F32)
    decode_grad = jnp.where(core == 0, other, mine).astype(F32)
    return (grid_update, encode_grad, decode_grad, middle_grad, summit_grad)


def solution(mesh):
    tiles, subs = mesh.devices.shape
    fine = Mesh(mesh.devices.reshape(tiles, subs // 2, 2), ALL)
    placed = (
        P(ALL, None),
        P(ALL, None),
        P(ALL, None),
        P(ALL, None),
        P(ALL),
        P(ALL),
        P(ALL),
        P(ALL),
        P(ALL),
        P("tile"),
        P(),
        P(),
        P(),
        P(),
        P(ALL, None),
    )
    return jax.shard_map(
        shards,
        mesh=fine,
        in_specs=placed,
        out_specs=(P(ALL, None), P(), P(), P(), P()),
        check_vma=False,
    )
```

```python
import functools

import jax
import jax.numpy as jnp
from jax import lax
from jax.experimental import pallas as pl
from jax.experimental.pallas import tpu as pltpu
from jax.sharding import Mesh, PartitionSpec as P


TOP_NODES = 512
LANES = 128
WORKING_BYTES = 10 * 2**20
TILE = ("half", "near")
ALL = TILE + ("row", "core")
NEAR = ("near", "row")
BF16 = jnp.bfloat16
F32 = jnp.float32
I32 = jnp.int32


def mm(left, right):
    return jnp.dot(left, right, preferred_element_type=F32)


def mm_tn(left, right):
    return lax.dot_general(left, right, (((0,), (0,)), ((), ())), preferred_element_type=F32)


def mm_nt(left, right):
    return lax.dot_general(left, right, (((1,), (1,)), ((), ())), preferred_element_type=F32)


def sigmoid(values):
    return 0.5 + 0.5 * jnp.tanh(0.5 * values)


def rows_onehot(ids, rows):
    n = ids.shape[1]
    hit = lax.broadcasted_iota(I32, (rows, n), 0) == ids
    return jnp.where(hit, 1.0, 0.0).astype(BF16)


def column(ids):
    n = ids.shape[1]
    wide = jnp.broadcast_to(ids.astype(F32), (8, n))
    return wide.T[:, :1].astype(I32)


def cols_onehot(ids, cols):
    n = ids.shape[1]
    hit = lax.broadcasted_iota(I32, (n, cols), 1) == column(ids)
    return jnp.where(hit, 1.0, 0.0).astype(BF16)


def coarse_split(ids):
    at = lax.broadcasted_iota(I32, (16, ids.shape[1]), 0)
    parts = jnp.where(at == 0, ids >> 4, jnp.where(at == 1, ids & 15, 0))
    return parts.astype(F32).astype(BF16)


def node_ids(block):
    codes = block.astype(F32)
    return (codes[2:3].astype(I32), (codes[0:1] * 16.0 + codes[1:2]).astype(I32))


def slots(source, device, core, rows):
    rel = source - device * rows
    before = rel < 0
    after = rel >= rows
    shift_before = jnp.where(core == 0, 3 * rows, 2 * rows)
    shift_after = jnp.where(core == 0, 0, rows)
    return rel + jnp.where(before, shift_before, 0) + jnp.where(after, shift_after, 0)


def ready_kernel(
    dev_ref,
    grid_ref,
    edges_ref,
    weight_ref,
    source_ref,
    target_ref,
    fine_ref,
    coarse_ref,
    edges_out_ref,
    weight_out_ref,
    own_ref,
    picks_ref,
    aims_ref,
    members_ref,
    nodes_ref,
    *,
    subs,
):
    device = dev_ref[0]
    rows, features = grid_ref.shape
    mesh_rows = fine_ref.shape[1]
    level_rows = coarse_ref.shape[1]
    picks = cols_onehot(slots(source_ref[...], device, device % 2, rows), 3 * rows)
    picks_ref[...] = picks[:, rows:]
    raw = target_ref[...]
    aimed = jnp.where(raw >= 0, raw - device * mesh_rows, -1)
    aims_ref[...] = rows_onehot(aimed, mesh_rows)
    local = fine_ref[...] - (device // subs) * level_rows
    members = rows_onehot(local, level_rows)
    members_ref[...] = members
    spot = (
        lax.broadcasted_iota(I32, (mesh_rows, features), 0)
        == lax.broadcasted_iota(I32, (mesh_rows, features), 1)
    )
    spread = jnp.where(spot, 1.0, 0.0).astype(BF16)
    at = lax.broadcasted_iota(I32, (16, mesh_rows), 0)
    codes = mm(coarse_split(coarse_ref[...]), members)
    codes = jnp.where(at == 2, local.astype(F32), codes)
    nodes_ref[...] = mm(codes.astype(BF16), spread).astype(BF16)[:8]
    own_ref[...] = mm(picks[:, :rows], grid_ref[...]).astype(BF16)
    edges_out_ref[...] = edges_ref[...]
    weight_out_ref[...] = weight_ref[...]


def encode_kernel(
    dev_ref,
    partner_ref,
    far_ref,
    mesh_ref,
    edges_ref,
    weight_ref,
    own_ref,
    picks_ref,
    aims_ref,
    members_ref,
    nodes_ref,
    fetched_ref,
    slope_ref,
    core_ref,
    farpkt_ref,
    keep_ref,
    *,
    factor,
):
    core = dev_ref[0] % 2
    mesh_rows = mesh_ref.shape[0]
    half = keep_ref.shape[0]
    others = jnp.concatenate([partner_ref[...], far_ref[...]], axis=0)
    fetched = (own_ref[...].astype(F32) + mm(picks_ref[...], others)).astype(BF16)
    fetched_ref[...] = fetched
    pre = mm(fetched, weight_ref[...]) + edges_ref[...].astype(F32)
    sig = sigmoid(pre)
    act = (pre * sig).astype(BF16)
    slope_ref[...] = (sig * (1.0 + pre * (1.0 - sig))).astype(BF16)
    summed = mm(aims_ref[...], act)
    mid = (mesh_ref[...].astype(F32) + factor * summed).astype(BF16)
    part = mm(members_ref[...], mid)
    first = part[:half]
    second = part[half:]
    keep_ref[...] = jnp.where(core == 0, first, second)
    core_ref[:half] = jnp.where(core == 0, second, first).astype(BF16)
    core_ref[half : half + mesh_rows] = mid
    core_ref[half + mesh_rows :] = nodes_ref[...]
    farpkt_ref[:mesh_rows] = mid
    farpkt_ref[mesh_rows:] = nodes_ref[...]


def spread_kernel(dev_ref, mine_ref, other_ref, coarse_ref, out_ref, *, subs, factor):
    device = dev_ref[0]
    core = device % 2
    tile = device // subs
    half, features = mine_ref.shape
    group = features // half
    total = mine_ref[...].astype(F32) + other_ref[...].astype(F32)
    mid = (factor * total).astype(BF16)
    level_rows = coarse_ref.shape[1]
    j = lax.broadcasted_iota(I32, (level_rows, features), 0) - core * half
    lane = lax.broadcasted_iota(I32, (level_rows, features), 1) - (tile % group) * half
    sel = (j == lane) & (j >= 0) & (j < half)
    codes = mm(coarse_split(coarse_ref[...]), jnp.where(sel, 1.0, 0.0).astype(BF16))
    lanes = out_ref.shape[2]
    strips = features // lanes
    tail = jnp.concatenate(
        [codes[r : r + 1, i * lanes : (i + 1) * lanes] for r in range(2) for i in range(strips)],
        axis=0,
    ).astype(BF16)
    for peer in range(out_ref.shape[0]):
        for i in range(strips):
            out_ref[peer, i * half : (i + 1) * half] = mid[:, i * lanes : (i + 1) * lanes]
        out_ref[peer, strips * half :] = tail


def middle_kernel(
    dev_ref,
    mine_ref,
    other_ref,
    core_ref,
    farpkt_ref,
    farin_ref,
    cot_ref,
    edges_ref,
    source_ref,
    target_ref,
    decode_weight_ref,
    middle_weight_ref,
    summit_weight_ref,
    fetched_ref,
    slope_ref,
    act_ref,
    own_ref,
    partner_ref,
    far_ref,
    level_ref,
    middle_slope_ref,
    summit_in_ref,
    summit_slope_ref,
    ids_ref,
    out_scr,
    *,
    subs,
    level_rows,
    summit_factor,
    decode_factor,
):
    device = dev_ref[0]
    core = device % 2
    tile = device // subs
    tiles, _, lanes = mine_ref.shape
    features = cot_ref.shape[1]
    strips = features // lanes
    half = level_rows // 2
    group = min(features // half, tiles)
    groups = tiles // group
    chunk = group * half
    for g in range(groups):
        for src, which in ((mine_ref, core), (other_ref, 1 - core)):
            block = src[g * group : (g + 1) * group]
            for i in range(strips):
                level_ref[which, g, :, i * lanes : (i + 1) * lanes] = block[
                    :, i * half : (i + 1) * half
                ].reshape(chunk, lanes)
            codes = jnp.sum(block[:, strips * half :].astype(F32), axis=0)
            ids = codes[:strips] * 16.0 + codes[strips : 2 * strips]
            ids = jnp.concatenate([ids[i : i + 1] for i in range(strips)], axis=1)
            ids_ref[which, g] = jnp.broadcast_to(ids.astype(I32)[:, :chunk], (8, chunk))
    summed = jnp.zeros((TOP_NODES, features), F32)
    for g in range(groups):
        for h in range(2):
            mid = level_ref[h, g]
            act = mm(mid, middle_weight_ref[...])
            sig = sigmoid(act)
            out = (mid.astype(F32) + act * sig).astype(BF16)
            middle_slope_ref[h, g] = (sig * (1.0 + act * (1.0 - sig))).astype(BF16)
            out_scr[h, pl.ds(g * chunk, chunk)] = out
            summed = summed + mm(rows_onehot(ids_ref[h, g][:1], TOP_NODES), out)
    summit_in = (summit_factor * summed).astype(BF16)
    summit_in_ref[...] = summit_in
    act = mm(summit_in, summit_weight_ref[...])
    sig = sigmoid(act)
    summit_slope_ref[...] = sig * (1.0 + act * (1.0 - sig))
    summit_out = (act * sig).astype(BF16)

    mesh_rows = farpkt_ref.shape[0] - 8
    rows = mesh_rows
    sub = device % subs
    far_tile = jnp.where(sub == 0, tile - 1, jnp.where(sub == subs - 1, tile + 1, tile))
    far_tile = jnp.clip(far_tile, 0, tiles - 1)

    def table(ref):
        pieces = []
        for at in (tile, far_tile):
            for h in range(2):
                pieces.append(ref[h, pl.ds(pl.multiple_of(at * half, half), half)])
        return jnp.concatenate(pieces, axis=0)

    own_fine, own_top = node_ids(farpkt_ref[rows:, :rows])
    partner_fine, partner_top = node_ids(core_ref[half + rows :, :rows])
    far_fine, far_top = node_ids(farin_ref[rows:, :rows])
    fine = jnp.concatenate([own_fine, partner_fine, far_fine + level_rows], axis=1)
    top = jnp.concatenate([own_top, partner_top, far_top], axis=1)
    lifted = mm(cols_onehot(fine, 2 * level_rows), table(out_scr)) + mm(
        cols_onehot(top, TOP_NODES), summit_out
    )
    mids = jnp.concatenate(
        [farpkt_ref[:rows], core_ref[half : half + rows], farin_ref[:rows]], axis=0
    )
    wide = (mids.astype(F32) + lifted).astype(BF16)

    place = slots(source_ref[...], device, core, rows)
    fetched = mm(cols_onehot(place, 3 * rows), wide).astype(BF16)
    pre = mm(fetched, decode_weight_ref[...]) + edges_ref[...].astype(F32)
    sig = sigmoid(pre)
    grid_rows = cot_ref.shape[0]
    raw = target_ref[...]
    aimed = jnp.where(raw >= 0, raw - device * grid_rows, -1)
    fetched_ref[...] = fetched
    act_ref[...] = (pre * sig).astype(BF16)
    incoming = mm(cols_onehot(aimed, grid_rows), cot_ref[...]) * decode_factor
    slope = (incoming * (sig * (1.0 + pre * (1.0 - sig)))).astype(BF16)
    slope_ref[...] = slope
    gathered = mm(rows_onehot(place, 3 * rows), slope).astype(BF16)
    returned = mm_nt(gathered, decode_weight_ref[...])
    own_ref[...] = returned[:rows]
    partner_ref[...] = returned[rows : 2 * rows]
    far_ref[...] = returned[2 * rows :].astype(BF16)


def update_kernel(
    dev_ref, grid_ref, target_ref, act_ref, fetched_ref, slope_ref, update_ref, dgrad_ref, *, factor
):
    grid_rows = grid_ref.shape[0]
    raw = target_ref[...]
    aimed = jnp.where(raw >= 0, raw - dev_ref[0] * grid_rows, -1)
    summed = mm(rows_onehot(aimed, grid_rows), act_ref[...])
    update_ref[...] = (grid_ref[...].astype(F32) + factor * summed).astype(BF16)
    dgrad_ref[...] = mm_tn(fetched_ref[...], slope_ref[...])


def level_kernel(
    dev_ref, own_ref, farin_ref, partner_ref, farpkt_ref, core_ref,
    sum_ref, pkt_ref, keep_ref, *, level_rows
):
    core = dev_ref[0] % 2
    rows = own_ref.shape[0]
    half = level_rows // 2
    grad = own_ref[...] + farin_ref[...].astype(F32)
    sum_ref[...] = grad
    own_fine, _ = node_ids(farpkt_ref[rows:, :rows])
    partner_fine, _ = node_ids(core_ref[half + rows :, :rows])
    partner = partner_ref[...].astype(BF16)
    part = mm(rows_onehot(own_fine, level_rows), grad.astype(BF16)) + mm(
        rows_onehot(partner_fine, level_rows), partner
    )
    first = part[:half]
    second = part[half:]
    keep_ref[...] = jnp.where(core == 0, first, second)
    pkt_ref[:half] = jnp.where(core == 0, second, first).astype(BF16)
    pkt_ref[half:] = partner


def back_kernel(
    dev_ref,
    mine_ref,
    other_ref,
    middle_slope_ref,
    summit_slope_ref,
    ids_ref,
    sum_ref,
    partnerin_ref,
    farpkt_ref,
    coarse_ref,
    fetched_ref,
    slope_ref,
    target_ref,
    dgrad_ref,
    middle_weight_ref,
    summit_weight_ref,
    send_ref,
    keep_ref,
    grad_ref,
    top_ref,
    top_back_ref,
    *,
    subs,
    level_rows,
    summit_factor,
    middle_factor,
    encode_factor,
):
    device = dev_ref[0]
    core = device % 2
    tile = device // subs
    _, half, features = mine_ref.shape
    _, groups, chunk, _ = grad_ref.shape
    group = chunk // half
    for g in range(groups):
        for src, which in ((mine_ref, core), (other_ref, 1 - core)):
            grad_ref[which, g] = src[g * group : (g + 1) * group].reshape(chunk, features)
    total = jnp.zeros((TOP_NODES, features), F32)
    for g in range(groups):
        for h in range(2):
            total = total + mm(rows_onehot(ids_ref[h, g][:1], TOP_NODES), grad_ref[h, g])
    summit_slope = (total * summit_slope_ref[...]).astype(BF16)
    top_ref[...] = summit_slope
    summit_back = mm_nt(summit_slope, summit_weight_ref[...]).astype(BF16)
    top_back_ref[...] = summit_back
    spot = pl.multiple_of((tile % group) * half, half)

    def own(ref):
        pieces = [ref[h, tile // group, pl.ds(spot, half)] for h in range(2)]
        return jnp.concatenate(pieces, axis=0).astype(F32)

    level_total = own(grad_ref) + summit_factor * mm(
        cols_onehot(coarse_ref[...], TOP_NODES), summit_back
    )
    slope = (level_total * own(middle_slope_ref)).astype(BF16)
    back = (level_total + mm_nt(slope, middle_weight_ref[...])).astype(BF16)
    rows = sum_ref.shape[0]
    own_fine, _ = node_ids(farpkt_ref[rows:, :rows])
    mesh_total = (
        sum_ref[...]
        + partnerin_ref[half:].astype(F32)
        + middle_factor * mm(cols_onehot(own_fine, level_rows), back)
    )
    raw = target_ref[...]
    aimed = jnp.where(raw >= 0, raw - device * rows, -1)
    upstream = mm(cols_onehot(aimed, rows), mesh_total.astype(BF16)) * encode_factor
    slope = (upstream * slope_ref[...].astype(F32)).astype(BF16)
    egrad = mm_tn(fetched_ref[...], slope)
    dgrad = dgrad_ref[...]
    send_ref[...] = jnp.where(core == 0, dgrad, egrad).astype(BF16)
    keep_ref[...] = jnp.where(core == 0, egrad, dgrad)


def late_kernel(
    dev_ref,
    grad_ref,
    level_ref,
    middle_slope_ref,
    top_back_ref,
    ids_ref,
    middle_grad_ref,
    *,
    summit_factor,
):
    _, groups, _, features = grad_ref.shape
    middle_grad = jnp.zeros((features, features), F32)
    for g in range(groups):
        for h in range(2):
            lifted = mm_tn(rows_onehot(ids_ref[h, g][:1], TOP_NODES), top_back_ref[...])
            level_total = grad_ref[h, g].astype(F32) + summit_factor * lifted
            slope = (level_total * middle_slope_ref[h, g].astype(F32)).astype(BF16)
            middle_grad = middle_grad + mm_tn(level_ref[h, g], slope)
    middle_grad_ref[...] = middle_grad


def top_kernel(dev_ref, summit_in_ref, top_ref, summit_grad_ref):
    summit_grad_ref[...] = mm_tn(summit_in_ref[...], top_ref[...])


def call(body, outs, args, scratch=(), **static):
    vmem = pl.BlockSpec(memory_space=pltpu.VMEM)
    smem = pl.BlockSpec(memory_space=pltpu.SMEM)
    specs = [smem if a.ndim == 1 else vmem for a in args]
    single = not isinstance(outs, (list, tuple))
    held = [a for a in args if a.ndim > 1] + ([outs] if single else list(outs)) + list(scratch)
    limit = sum(a.size * a.dtype.itemsize for a in held) + WORKING_BYTES
    limit = min(limit, 60 * 2**20)
    return pl.pallas_call(
        functools.partial(body, **static),
        out_shape=outs,
        in_specs=specs,
        out_specs=vmem if single else [vmem] * len(outs),
        scratch_shapes=[pltpu.VMEM(s.shape, s.dtype) for s in scratch],
        compiler_params=pltpu.CompilerParams(vmem_limit_bytes=limit),
    )(*args)


def shape(dims, dtype):
    return jax.ShapeDtypeStruct(dims, dtype)


def shards(
    grid_feats,
    mesh_feats,
    encode_edges,
    decode_edges,
    encode_source,
    encode_target,
    decode_source,
    decode_target,
    owner_fine,
    owner_coarse,
    encode_weight,
    decode_weight,
    middle_weight,
    summit_weight,
    cotangent,
):
    rows, features = grid_feats.shape
    mesh_rows = mesh_feats.shape[0]
    level_rows = owner_coarse.shape[0]
    half = level_rows // 2
    tiles = lax.axis_size(TILE)
    subs = lax.axis_size("row") * lax.axis_size("core")
    devices = tiles * subs
    peers = devices // 4
    edges = encode_source.shape[0]
    swap = [(0, 1), (1, 0)]
    beside = []
    for left in range(1, devices - 1, 2):
        beside += [(left, left + 1), (left + 1, left)]
    device = lax.axis_index(ALL).astype(I32)
    dev = device.reshape(1)
    core = device % 2
    encode_factor = mesh_rows / edges
    decode_factor = rows / decode_source.shape[0]
    middle_factor = level_rows / (mesh_rows * subs)
    summit_factor = TOP_NODES / (level_rows * tiles)
    group = min(features // half, tiles)
    groups = tiles // group
    chunk = group * half

    grid_far = lax.ppermute(grid_feats, ALL, beside)
    grid_partner = lax.ppermute(grid_feats, "core", swap)
    edges_in, weight_in, own_rows, picks, aims, members, nodes = call(
        ready_kernel,
        [
            shape((edges, features), BF16),
            shape((features, features), BF16),
            shape((edges, features), BF16),
            shape((edges, 2 * rows), BF16),
            shape((mesh_rows, edges), BF16),
            shape((level_rows, mesh_rows), BF16),
            shape((8, features), BF16),
        ],
        [
            dev,
            grid_feats,
            encode_edges,
            encode_weight,
            encode_source[None],
            encode_target[None],
            owner_fine[None],
            owner_coarse[None],
        ],
        subs=subs,
    )
    fetched, slope, core_pkt, far_pkt, keep = call(
        encode_kernel,
        [
            shape((edges, features), BF16),
            shape((edges, features), BF16),
            shape((half + mesh_rows + 8, features), BF16),
            shape((mesh_rows + 8, features), BF16),
            shape((half, features), F32),
        ],
        [
            dev,
            grid_partner,
            grid_far,
            mesh_feats,
            edges_in,
            weight_in,
            own_rows,
            picks,
            aims,
            members,
            nodes,
        ],
        factor=encode_factor,
    )
    core_in = lax.ppermute(core_pkt, "core", swap)
    far_in = lax.ppermute(far_pkt, ALL, beside)
    mine = (keep + core_in[:half].astype(F32)).astype(BF16)
    other = lax.ppermute(mine, "row", swap)
    packed = call(
        spread_kernel,
        shape((tiles, (features // LANES) * half + 8, LANES), BF16),
        [dev, mine, other, owner_coarse[None]],
        subs=subs,
        factor=middle_factor,
    )
    mids = lax.all_to_all(packed, TILE, 0, 0)
    mids_other = lax.ppermute(mids, "core", swap)
    full = (2, groups, chunk, features)
    (
        decode_fetched,
        decode_slope,
        decode_act,
        own,
        partner,
        far,
        level,
        middle_slope,
        summit_in,
        summit_slope,
        ids,
    ) = call(
        middle_kernel,
        [
            shape(decode_edges.shape, BF16),
            shape(decode_edges.shape, BF16),
            shape(decode_edges.shape, BF16),
            shape((mesh_rows, features), F32),
            shape((mesh_rows, features), F32),
            shape((mesh_rows, features), BF16),
            shape(full, BF16),
            shape(full, BF16),
            shape((TOP_NODES, features), BF16),
            shape((TOP_NODES, features), F32),
            shape((2, groups, 8, chunk), I32),
        ],
        [
            dev,
            mids,
            mids_other,
            core_in,
            far_pkt,
            far_in,
            cotangent,
            decode_edges,
            decode_source[None],
            decode_target[None],
            decode_weight,
            middle_weight,
            summit_weight,
        ],
        scratch=[
            shape((2, tiles * half, features), BF16),
        ],
        subs=subs,
        level_rows=level_rows,
        summit_factor=summit_factor,
        decode_factor=decode_factor,
    )
    far_back = lax.ppermute(far, ALL, beside)
    grid_update, dgrad = call(
        update_kernel,
        [shape((rows, features), BF16), shape((features, features), F32)],
        [
            dev,
            grid_feats,
            decode_target[None],
            decode_act,
            decode_fetched,
            decode_slope,
        ],
        factor=decode_factor,
    )
    grad_sum, core_pkt, keep = call(
        level_kernel,
        [
            shape((mesh_rows, features), F32),
            shape((half + mesh_rows, features), BF16),
            shape((half, features), F32),
        ],
        [dev, own, far_back, partner, far_pkt, core_in],
        level_rows=level_rows,
    )
    back_in = lax.ppermute(core_pkt, "core", swap)
    mine = (keep + back_in[:half].astype(F32)).astype(BF16)
    other = lax.ppermute(mine, "row", swap)
    total = (mine.astype(F32) + other.astype(F32)).astype(BF16)
    packed = jnp.broadcast_to(total[None], (tiles, half, features))
    grads = lax.all_to_all(packed, TILE, 0, 0)
    grads_other = lax.ppermute(grads, "core", swap)
    send, keep, level_back, top, top_back = call(
        back_kernel,
        [
            shape((features, features), BF16),
            shape((features, features), F32),
            shape(full, BF16),
            shape((TOP_NODES, features), BF16),
            shape((TOP_NODES, features), BF16),
        ],
        [
            dev,
            grads,
            grads_other,
            middle_slope,
            summit_slope,
            ids,
            grad_sum,
            back_in,
            far_pkt,
            owner_coarse[None],
            fetched,
            slope,
            encode_target[None],
            dgrad,
            middle_weight,
            summit_weight,
        ],
        subs=subs,
        level_rows=level_rows,
        summit_factor=summit_factor,
        middle_factor=middle_factor,
        encode_factor=encode_factor,
    )
    received = lax.ppermute(send, "core", swap)
    middle_grad = call(
        late_kernel,
        shape((features, features), F32),
        [dev, level_back, level, middle_slope, top_back, ids],
        summit_factor=summit_factor,
    )
    share = (keep + received.astype(F32)).astype(BF16)
    share = share.reshape(peers, features // peers, features)
    parts = lax.all_to_all(share, NEAR, 0, 0)
    near = jnp.sum(parts.astype(F32), axis=0).astype(BF16)
    away = lax.ppermute(near, "half", swap)
    summed = (near.astype(F32) + away.astype(F32)).astype(BF16)
    copies = jnp.broadcast_to(summed[None], parts.shape)
    mine = lax.all_to_all(copies, NEAR, 0, 0).reshape(features, features)
    other = lax.ppermute(mine, "core", swap)
    summit_grad = call(
        top_kernel, shape((features, features), F32), [dev, summit_in, top]
    )
    encode_grad = jnp.where(core == 0, mine, other).astype(F32)
    decode_grad = jnp.where(core == 0, other, mine).astype(F32)
    return (grid_update, encode_grad, decode_grad, middle_grad, summit_grad)


def solution(mesh):
    tiles, subs = mesh.devices.shape
    fine = Mesh(mesh.devices.reshape(2, tiles // 2, subs // 2, 2), ALL)
    placed = (
        P(ALL, None),
        P(ALL, None),
        P(ALL, None),
        P(ALL, None),
        P(ALL),
        P(ALL),
        P(ALL),
        P(ALL),
        P(ALL),
        P(TILE),
        P(),
        P(),
        P(),
        P(),
        P(ALL, None),
    )
    return jax.shard_map(
        shards,
        mesh=fine,
        in_specs=placed,
        out_specs=(P(ALL, None), P(), P(), P(), P()),
        check_vma=False,
    )
```

```python
import functools

import jax
import jax.numpy as jnp
from jax import lax
from jax.experimental import pallas as pl
from jax.experimental.pallas import tpu as pltpu
from jax.sharding import Mesh, PartitionSpec as P


TOP_NODES = 512
LANES = 128
WORKING_BYTES = 10 * 2**20
TILE = ("half", "near")
ALL = TILE + ("row", "core")
NEAR = ("near", "row")
BF16 = jnp.bfloat16
F32 = jnp.float32
I32 = jnp.int32


def mm(left, right):
    return jnp.dot(left, right, preferred_element_type=F32)


def mm_tn(left, right):
    return lax.dot_general(left, right, (((0,), (0,)), ((), ())), preferred_element_type=F32)


def mm_nt(left, right):
    return lax.dot_general(left, right, (((1,), (1,)), ((), ())), preferred_element_type=F32)


def sigmoid(values):
    return 0.5 + 0.5 * jnp.tanh(0.5 * values)


def rows_onehot(ids, rows):
    n = ids.shape[1]
    hit = lax.broadcasted_iota(I32, (rows, n), 0) == ids
    return jnp.where(hit, 1.0, 0.0).astype(BF16)


def column(ids):
    n = ids.shape[1]
    wide = jnp.broadcast_to(ids.astype(F32), (8, n))
    return wide.T[:, :1].astype(I32)


def cols_onehot(ids, cols):
    n = ids.shape[1]
    hit = lax.broadcasted_iota(I32, (n, cols), 1) == column(ids)
    return jnp.where(hit, 1.0, 0.0).astype(BF16)


def coarse_split(ids):
    at = lax.broadcasted_iota(I32, (16, ids.shape[1]), 0)
    parts = jnp.where(at == 0, ids >> 4, jnp.where(at == 1, ids & 15, 0))
    return parts.astype(F32).astype(BF16)


def node_ids(block):
    codes = block.astype(F32)
    return (codes[2:3].astype(I32), (codes[0:1] * 16.0 + codes[1:2]).astype(I32))


def slots(source, device, core, rows):
    rel = source - device * rows
    before = rel < 0
    after = rel >= rows
    shift_before = jnp.where(core == 0, 3 * rows, 2 * rows)
    shift_after = jnp.where(core == 0, 0, rows)
    return rel + jnp.where(before, shift_before, 0) + jnp.where(after, shift_after, 0)


def ready_kernel(
    dev_ref,
    grid_ref,
    edges_ref,
    weight_ref,
    source_ref,
    target_ref,
    fine_ref,
    coarse_ref,
    edges_out_ref,
    weight_out_ref,
    own_ref,
    picks_ref,
    aims_ref,
    members_ref,
    nodes_ref,
    *,
    subs,
):
    device = dev_ref[0]
    rows, features = grid_ref.shape
    mesh_rows = fine_ref.shape[1]
    level_rows = coarse_ref.shape[1]
    picks = cols_onehot(slots(source_ref[...], device, device % 2, rows), 3 * rows)
    picks_ref[...] = picks[:, rows:]
    raw = target_ref[...]
    aimed = jnp.where(raw >= 0, raw - device * mesh_rows, -1)
    aims_ref[...] = rows_onehot(aimed, mesh_rows)
    local = fine_ref[...] - (device // subs) * level_rows
    members = rows_onehot(local, level_rows)
    members_ref[...] = members
    spot = (
        lax.broadcasted_iota(I32, (mesh_rows, features), 0)
        == lax.broadcasted_iota(I32, (mesh_rows, features), 1)
    )
    spread = jnp.where(spot, 1.0, 0.0).astype(BF16)
    at = lax.broadcasted_iota(I32, (16, mesh_rows), 0)
    codes = mm(coarse_split(coarse_ref[...]), members)
    codes = jnp.where(at == 2, local.astype(F32), codes)
    nodes_ref[...] = mm(codes.astype(BF16), spread).astype(BF16)[:8]
    own_ref[...] = mm(picks[:, :rows], grid_ref[...]).astype(BF16)
    edges_out_ref[...] = edges_ref[...]
    weight_out_ref[...] = weight_ref[...]


def encode_kernel(
    dev_ref,
    partner_ref,
    far_ref,
    mesh_ref,
    edges_ref,
    weight_ref,
    own_ref,
    picks_ref,
    aims_ref,
    members_ref,
    nodes_ref,
    fetched_ref,
    core_ref,
    farpkt_ref,
    keep_ref,
    *,
    factor,
):
    core = dev_ref[0] % 2
    mesh_rows = mesh_ref.shape[0]
    half = keep_ref.shape[0]
    others = jnp.concatenate([partner_ref[...], far_ref[...]], axis=0)
    fetched = (own_ref[...].astype(F32) + mm(picks_ref[...], others)).astype(BF16)
    fetched_ref[...] = fetched
    pre = mm(fetched, weight_ref[...]) + edges_ref[...].astype(F32)
    sig = sigmoid(pre)
    act = (pre * sig).astype(BF16)
    summed = mm(aims_ref[...], act)
    mid = (mesh_ref[...].astype(F32) + factor * summed).astype(BF16)
    part = mm(members_ref[...], mid)
    first = part[:half]
    second = part[half:]
    keep_ref[...] = jnp.where(core == 0, first, second)
    core_ref[:half] = jnp.where(core == 0, second, first).astype(BF16)
    core_ref[half : half + mesh_rows] = mid
    core_ref[half + mesh_rows :] = nodes_ref[...]
    farpkt_ref[:mesh_rows] = mid
    farpkt_ref[mesh_rows:] = nodes_ref[...]


def spread_kernel(dev_ref, mine_ref, other_ref, coarse_ref, out_ref, *, subs, factor):
    device = dev_ref[0]
    core = device % 2
    tile = device // subs
    half, features = mine_ref.shape
    group = features // half
    total = mine_ref[...].astype(F32) + other_ref[...].astype(F32)
    mid = (factor * total).astype(BF16)
    level_rows = coarse_ref.shape[1]
    j = lax.broadcasted_iota(I32, (level_rows, features), 0) - core * half
    lane = lax.broadcasted_iota(I32, (level_rows, features), 1) - (tile % group) * half
    sel = (j == lane) & (j >= 0) & (j < half)
    codes = mm(coarse_split(coarse_ref[...]), jnp.where(sel, 1.0, 0.0).astype(BF16))
    lanes = out_ref.shape[1]
    strips = features // lanes
    tail = jnp.concatenate(
        [codes[r : r + 1, i * lanes : (i + 1) * lanes] for r in range(2) for i in range(strips)],
        axis=0,
    ).astype(BF16)
    for i in range(strips):
        out_ref[i * half : (i + 1) * half] = mid[:, i * lanes : (i + 1) * lanes]
    out_ref[strips * half :] = tail


def pair_kernel(dev_ref, mine_ref, away_ref, out_ref):
    span = mine_ref.shape[0]
    for peer in range(out_ref.shape[0]):
        out_ref[peer, :span] = mine_ref[...]
        out_ref[peer, span:] = away_ref[...]


def placed_blocks(tile, near, group, half):
    count = min(group, near)
    mine = tile // near
    for part in range(2):
        side = mine if part == 0 else 1 - mine
        for first in range(0, near, count):
            at = side * near + first
            yield part, first, count, at // group, pl.multiple_of((at % group) * half, half)


def middle_kernel(
    dev_ref,
    mine_ref,
    other_ref,
    core_ref,
    farpkt_ref,
    farin_ref,
    cot_ref,
    edges_ref,
    source_ref,
    target_ref,
    decode_weight_ref,
    middle_weight_ref,
    summit_weight_ref,
    fetched_ref,
    slope_ref,
    act_ref,
    own_ref,
    partner_ref,
    far_ref,
    level_ref,
    summit_in_ref,
    ids_ref,
    out_scr,
    *,
    subs,
    level_rows,
    summit_factor,
    decode_factor,
):
    device = dev_ref[0]
    core = device % 2
    tile = device // subs
    near, span, lanes = mine_ref.shape
    tiles = 2 * near
    features = cot_ref.shape[1]
    strips = features // lanes
    half = level_rows // 2
    group = min(features // half, tiles)
    groups = tiles // group
    chunk = group * half
    unit = span // 2
    ids_ref[...] = jnp.zeros(ids_ref.shape, I32)
    for part, first, count, g, row in placed_blocks(tile, near, group, half):
        for src, which in ((mine_ref, core), (other_ref, 1 - core)):
            block = src[first : first + count, part * unit : (part + 1) * unit]
            for i in range(strips):
                level_ref[which, g, pl.ds(row, count * half), i * lanes : (i + 1) * lanes] = block[
                    :, i * half : (i + 1) * half
                ].reshape(count * half, lanes)
            codes = jnp.sum(block[:, strips * half :].astype(F32), axis=0)
            ids = codes[:strips] * 16.0 + codes[strips : 2 * strips]
            ids = jnp.concatenate([ids[i : i + 1] for i in range(strips)], axis=1)
            ids_ref[which, g] += jnp.broadcast_to(ids.astype(I32)[:, :chunk], (8, chunk))
    summed = jnp.zeros((TOP_NODES, features), F32)
    for g in range(groups):
        for h in range(2):
            mid = level_ref[h, g]
            act = mm(mid, middle_weight_ref[...])
            sig = sigmoid(act)
            out = (mid.astype(F32) + act * sig).astype(BF16)
            out_scr[h, pl.ds(g * chunk, chunk)] = out
            summed = summed + mm(rows_onehot(ids_ref[h, g][:1], TOP_NODES), out)
    summit_in = (summit_factor * summed).astype(BF16)
    summit_in_ref[...] = summit_in
    act = mm(summit_in, summit_weight_ref[...])
    sig = sigmoid(act)
    summit_out = (act * sig).astype(BF16)

    mesh_rows = farpkt_ref.shape[0] - 8
    rows = mesh_rows
    sub = device % subs
    far_tile = jnp.where(sub == 0, tile - 1, jnp.where(sub == subs - 1, tile + 1, tile))
    far_tile = jnp.clip(far_tile, 0, tiles - 1)

    def table(ref):
        pieces = []
        for at in (tile, far_tile):
            for h in range(2):
                pieces.append(ref[h, pl.ds(pl.multiple_of(at * half, half), half)])
        return jnp.concatenate(pieces, axis=0)

    own_fine, own_top = node_ids(farpkt_ref[rows:, :rows])
    partner_fine, partner_top = node_ids(core_ref[half + rows :, :rows])
    far_fine, far_top = node_ids(farin_ref[rows:, :rows])
    fine = jnp.concatenate([own_fine, partner_fine, far_fine + level_rows], axis=1)
    top = jnp.concatenate([own_top, partner_top, far_top], axis=1)
    lifted = mm(cols_onehot(fine, 2 * level_rows), table(out_scr)) + mm(
        cols_onehot(top, TOP_NODES), summit_out
    )
    mids = jnp.concatenate(
        [farpkt_ref[:rows], core_ref[half : half + rows], farin_ref[:rows]], axis=0
    )
    wide = (mids.astype(F32) + lifted).astype(BF16)

    place = slots(source_ref[...], device, core, rows)
    fetched = mm(cols_onehot(place, 3 * rows), wide).astype(BF16)
    pre = mm(fetched, decode_weight_ref[...]) + edges_ref[...].astype(F32)
    sig = sigmoid(pre)
    grid_rows = cot_ref.shape[0]
    raw = target_ref[...]
    aimed = jnp.where(raw >= 0, raw - device * grid_rows, -1)
    fetched_ref[...] = fetched
    act_ref[...] = (pre * sig).astype(BF16)
    incoming = mm(cols_onehot(aimed, grid_rows), cot_ref[...]) * decode_factor
    slope = (incoming * (sig * (1.0 + pre * (1.0 - sig)))).astype(BF16)
    slope_ref[...] = slope
    gathered = mm(rows_onehot(place, 3 * rows), slope).astype(BF16)
    returned = mm_nt(gathered, decode_weight_ref[...])
    own_ref[...] = returned[:rows]
    partner_ref[...] = returned[rows : 2 * rows]
    far_ref[...] = returned[2 * rows :].astype(BF16)


def silu_slope(values):
    sig = sigmoid(values)
    return sig * (1.0 + values * (1.0 - sig))


def slope_kernel(dev_ref, fetched_ref, edges_ref, weight_ref, slope_ref):
    pre = mm(fetched_ref[...], weight_ref[...]) + edges_ref[...].astype(F32)
    slope_ref[...] = silu_slope(pre).astype(BF16)


def update_kernel(
    dev_ref,
    grid_ref,
    target_ref,
    act_ref,
    fetched_ref,
    slope_ref,
    level_ref,
    summit_in_ref,
    middle_weight_ref,
    summit_weight_ref,
    update_ref,
    dgrad_ref,
    middle_slope_ref,
    summit_slope_ref,
    *,
    factor,
):
    grid_rows = grid_ref.shape[0]
    raw = target_ref[...]
    aimed = jnp.where(raw >= 0, raw - dev_ref[0] * grid_rows, -1)
    summed = mm(rows_onehot(aimed, grid_rows), act_ref[...])
    update_ref[...] = (grid_ref[...].astype(F32) + factor * summed).astype(BF16)
    dgrad_ref[...] = mm_tn(fetched_ref[...], slope_ref[...])
    for h in range(2):
        for g in range(level_ref.shape[1]):
            act = mm(level_ref[h, g], middle_weight_ref[...])
            middle_slope_ref[h, g] = silu_slope(act).astype(BF16)
    summit_slope_ref[...] = silu_slope(mm(summit_in_ref[...], summit_weight_ref[...]))


def level_kernel(
    dev_ref, own_ref, farin_ref, partner_ref, farpkt_ref, core_ref,
    sum_ref, pkt_ref, keep_ref, *, level_rows
):
    core = dev_ref[0] % 2
    rows = own_ref.shape[0]
    half = level_rows // 2
    grad = own_ref[...] + farin_ref[...].astype(F32)
    sum_ref[...] = grad
    own_fine, _ = node_ids(farpkt_ref[rows:, :rows])
    partner_fine, _ = node_ids(core_ref[half + rows :, :rows])
    partner = partner_ref[...].astype(BF16)
    part = mm(rows_onehot(own_fine, level_rows), grad.astype(BF16)) + mm(
        rows_onehot(partner_fine, level_rows), partner
    )
    first = part[:half]
    second = part[half:]
    keep_ref[...] = jnp.where(core == 0, first, second)
    pkt_ref[:half] = jnp.where(core == 0, second, first).astype(BF16)
    pkt_ref[half:] = partner


def back_kernel(
    dev_ref,
    mine_ref,
    other_ref,
    middle_slope_ref,
    summit_slope_ref,
    ids_ref,
    sum_ref,
    partnerin_ref,
    farpkt_ref,
    coarse_ref,
    fetched_ref,
    slope_ref,
    target_ref,
    dgrad_ref,
    middle_weight_ref,
    summit_weight_ref,
    send_ref,
    keep_ref,
    grad_ref,
    top_ref,
    top_back_ref,
    *,
    subs,
    level_rows,
    summit_factor,
    middle_factor,
    encode_factor,
):
    device = dev_ref[0]
    core = device % 2
    tile = device // subs
    near, pair, features = mine_ref.shape
    half = pair // 2
    _, groups, chunk, _ = grad_ref.shape
    group = chunk // half
    for part, first, count, g, row in placed_blocks(tile, near, group, half):
        for src, which in ((mine_ref, core), (other_ref, 1 - core)):
            grad_ref[which, g, pl.ds(row, count * half)] = src[
                first : first + count, part * half : (part + 1) * half
            ].reshape(count * half, features)
    total = jnp.zeros((TOP_NODES, features), F32)
    for g in range(groups):
        for h in range(2):
            total = total + mm(rows_onehot(ids_ref[h, g][:1], TOP_NODES), grad_ref[h, g])
    summit_slope = (total * summit_slope_ref[...]).astype(BF16)
    top_ref[...] = summit_slope
    summit_back = mm_nt(summit_slope, summit_weight_ref[...]).astype(BF16)
    top_back_ref[...] = summit_back
    spot = pl.multiple_of((tile % group) * half, half)

    def own(ref):
        pieces = [ref[h, tile // group, pl.ds(spot, half)] for h in range(2)]
        return jnp.concatenate(pieces, axis=0).astype(F32)

    level_total = own(grad_ref) + summit_factor * mm(
        cols_onehot(coarse_ref[...], TOP_NODES), summit_back
    )
    slope = (level_total * own(middle_slope_ref)).astype(BF16)
    back = (level_total + mm_nt(slope, middle_weight_ref[...])).astype(BF16)
    rows = sum_ref.shape[0]
    own_fine, _ = node_ids(farpkt_ref[rows:, :rows])
    mesh_total = (
        sum_ref[...]
        + partnerin_ref[half:].astype(F32)
        + middle_factor * mm(cols_onehot(own_fine, level_rows), back)
    )
    raw = target_ref[...]
    aimed = jnp.where(raw >= 0, raw - device * rows, -1)
    upstream = mm(cols_onehot(aimed, rows), mesh_total.astype(BF16)) * encode_factor
    slope = (upstream * slope_ref[...].astype(F32)).astype(BF16)
    egrad = mm_tn(fetched_ref[...], slope)
    dgrad = dgrad_ref[...]
    send_ref[...] = jnp.where(core == 0, dgrad, egrad).astype(BF16)
    keep_ref[...] = jnp.where(core == 0, egrad, dgrad)


def late_kernel(
    dev_ref,
    grad_ref,
    level_ref,
    middle_slope_ref,
    top_back_ref,
    ids_ref,
    middle_grad_ref,
    *,
    summit_factor,
):
    _, groups, _, features = grad_ref.shape
    middle_grad = jnp.zeros((features, features), F32)
    for g in range(groups):
        for h in range(2):
            lifted = mm_tn(rows_onehot(ids_ref[h, g][:1], TOP_NODES), top_back_ref[...])
            level_total = grad_ref[h, g].astype(F32) + summit_factor * lifted
            slope = (level_total * middle_slope_ref[h, g].astype(F32)).astype(BF16)
            middle_grad = middle_grad + mm_tn(level_ref[h, g], slope)
    middle_grad_ref[...] = middle_grad


def top_kernel(dev_ref, summit_in_ref, top_ref, summit_grad_ref):
    summit_grad_ref[...] = mm_tn(summit_in_ref[...], top_ref[...])


def call(body, outs, args, scratch=(), **static):
    vmem = pl.BlockSpec(memory_space=pltpu.VMEM)
    smem = pl.BlockSpec(memory_space=pltpu.SMEM)
    specs = [smem if a.ndim == 1 else vmem for a in args]
    single = not isinstance(outs, (list, tuple))
    held = [a for a in args if a.ndim > 1] + ([outs] if single else list(outs)) + list(scratch)
    limit = sum(a.size * a.dtype.itemsize for a in held) + WORKING_BYTES
    limit = min(limit, 60 * 2**20)
    return pl.pallas_call(
        functools.partial(body, **static),
        out_shape=outs,
        in_specs=specs,
        out_specs=vmem if single else [vmem] * len(outs),
        scratch_shapes=[pltpu.VMEM(s.shape, s.dtype) for s in scratch],
        compiler_params=pltpu.CompilerParams(vmem_limit_bytes=limit),
    )(*args)


def shape(dims, dtype):
    return jax.ShapeDtypeStruct(dims, dtype)


def shards(
    grid_feats,
    mesh_feats,
    encode_edges,
    decode_edges,
    encode_source,
    encode_target,
    decode_source,
    decode_target,
    owner_fine,
    owner_coarse,
    encode_weight,
    decode_weight,
    middle_weight,
    summit_weight,
    cotangent,
):
    rows, features = grid_feats.shape
    mesh_rows = mesh_feats.shape[0]
    level_rows = owner_coarse.shape[0]
    half = level_rows // 2
    tiles = lax.axis_size(TILE)
    subs = lax.axis_size("row") * lax.axis_size("core")
    devices = tiles * subs
    peers = devices // 4
    near = tiles // 2
    edges = encode_source.shape[0]
    swap = [(0, 1), (1, 0)]
    beside = []
    for left in range(1, devices - 1, 2):
        beside += [(left, left + 1), (left + 1, left)]
    device = lax.axis_index(ALL).astype(I32)
    dev = device.reshape(1)
    core = device % 2
    encode_factor = mesh_rows / edges
    decode_factor = rows / decode_source.shape[0]
    middle_factor = level_rows / (mesh_rows * subs)
    summit_factor = TOP_NODES / (level_rows * tiles)
    group = min(features // half, tiles)
    groups = tiles // group
    chunk = group * half

    grid_far = lax.ppermute(grid_feats, ALL, beside)
    grid_partner = lax.ppermute(grid_feats, "core", swap)
    edges_in, weight_in, own_rows, picks, aims, members, nodes = call(
        ready_kernel,
        [
            shape((edges, features), BF16),
            shape((features, features), BF16),
            shape((edges, features), BF16),
            shape((edges, 2 * rows), BF16),
            shape((mesh_rows, edges), BF16),
            shape((level_rows, mesh_rows), BF16),
            shape((8, features), BF16),
        ],
        [
            dev,
            grid_feats,
            encode_edges,
            encode_weight,
            encode_source[None],
            encode_target[None],
            owner_fine[None],
            owner_coarse[None],
        ],
        subs=subs,
    )
    fetched, core_pkt, far_pkt, keep = call(
        encode_kernel,
        [
            shape((edges, features), BF16),
            shape((half + mesh_rows + 8, features), BF16),
            shape((mesh_rows + 8, features), BF16),
            shape((half, features), F32),
        ],
        [
            dev,
            grid_partner,
            grid_far,
            mesh_feats,
            edges_in,
            weight_in,
            own_rows,
            picks,
            aims,
            members,
            nodes,
        ],
        factor=encode_factor,
    )
    core_in = lax.ppermute(core_pkt, "core", swap)
    far_in = lax.ppermute(far_pkt, ALL, beside)
    mine = (keep + core_in[:half].astype(F32)).astype(BF16)
    other = lax.ppermute(mine, "row", swap)
    packet = call(
        spread_kernel,
        shape(((features // LANES) * half + 8, LANES), BF16),
        [dev, mine, other, owner_coarse[None]],
        subs=subs,
        factor=middle_factor,
    )
    away = lax.ppermute(packet, "half", swap)
    slope = call(
        slope_kernel, shape((edges, features), BF16), [dev, fetched, edges_in, weight_in]
    )
    packed = call(
        pair_kernel, shape((near, 2 * packet.shape[0], LANES), BF16), [dev, packet, away]
    )
    mids = lax.all_to_all(packed, "near", 0, 0)
    mids_other = lax.ppermute(mids, "core", swap)
    full = (2, groups, chunk, features)
    (
        decode_fetched,
        decode_slope,
        decode_act,
        own,
        partner,
        far,
        level,
        summit_in,
        ids,
    ) = call(
        middle_kernel,
        [
            shape(decode_edges.shape, BF16),
            shape(decode_edges.shape, BF16),
            shape(decode_edges.shape, BF16),
            shape((mesh_rows, features), F32),
            shape((mesh_rows, features), F32),
            shape((mesh_rows, features), BF16),
            shape(full, BF16),
            shape((TOP_NODES, features), BF16),
            shape((2, groups, 8, chunk), I32),
        ],
        [
            dev,
            mids,
            mids_other,
            core_in,
            far_pkt,
            far_in,
            cotangent,
            decode_edges,
            decode_source[None],
            decode_target[None],
            decode_weight,
            middle_weight,
            summit_weight,
        ],
        scratch=[
            shape((2, tiles * half, features), BF16),
        ],
        subs=subs,
        level_rows=level_rows,
        summit_factor=summit_factor,
        decode_factor=decode_factor,
    )
    far_back = lax.ppermute(far, ALL, beside)
    grid_update, dgrad, middle_slope, summit_slope = call(
        update_kernel,
        [
            shape((rows, features), BF16),
            shape((features, features), F32),
            shape(full, BF16),
            shape((TOP_NODES, features), F32),
        ],
        [
            dev,
            grid_feats,
            decode_target[None],
            decode_act,
            decode_fetched,
            decode_slope,
            level,
            summit_in,
            middle_weight,
            summit_weight,
        ],
        factor=decode_factor,
    )
    grad_sum, core_pkt, keep = call(
        level_kernel,
        [
            shape((mesh_rows, features), F32),
            shape((half + mesh_rows, features), BF16),
            shape((half, features), F32),
        ],
        [dev, own, far_back, partner, far_pkt, core_in],
        level_rows=level_rows,
    )
    back_in = lax.ppermute(core_pkt, "core", swap)
    mine = (keep + back_in[:half].astype(F32)).astype(BF16)
    other = lax.ppermute(mine, "row", swap)
    total = (mine.astype(F32) + other.astype(F32)).astype(BF16)
    away = lax.ppermute(total, "half", swap)
    packed = call(pair_kernel, shape((near, 2 * half, features), BF16), [dev, total, away])
    grads = lax.all_to_all(packed, "near", 0, 0)
    grads_other = lax.ppermute(grads, "core", swap)
    send, keep, level_back, top, top_back = call(
        back_kernel,
        [
            shape((features, features), BF16),
            shape((features, features), F32),
            shape(full, BF16),
            shape((TOP_NODES, features), BF16),
            shape((TOP_NODES, features), BF16),
        ],
        [
            dev,
            grads,
            grads_other,
            middle_slope,
            summit_slope,
            ids,
            grad_sum,
            back_in,
            far_pkt,
            owner_coarse[None],
            fetched,
            slope,
            encode_target[None],
            dgrad,
            middle_weight,
            summit_weight,
        ],
        subs=subs,
        level_rows=level_rows,
        summit_factor=summit_factor,
        middle_factor=middle_factor,
        encode_factor=encode_factor,
    )
    received = lax.ppermute(send, "core", swap)
    middle_grad = call(
        late_kernel,
        shape((features, features), F32),
        [dev, level_back, level, middle_slope, top_back, ids],
        summit_factor=summit_factor,
    )
    share = (keep + received.astype(F32)).astype(BF16)
    share = share.reshape(peers, features // peers, features)
    parts = lax.all_to_all(share, NEAR, 0, 0)
    inside = jnp.sum(parts.astype(F32), axis=0).astype(BF16)
    away = lax.ppermute(inside, "half", swap)
    summed = (inside.astype(F32) + away.astype(F32)).astype(BF16)
    copies = jnp.broadcast_to(summed[None], parts.shape)
    mine = lax.all_to_all(copies, NEAR, 0, 0).reshape(features, features)
    other = lax.ppermute(mine, "core", swap)
    summit_grad = call(
        top_kernel, shape((features, features), F32), [dev, summit_in, top]
    )
    encode_grad = jnp.where(core == 0, mine, other).astype(F32)
    decode_grad = jnp.where(core == 0, other, mine).astype(F32)
    return (grid_update, encode_grad, decode_grad, middle_grad, summit_grad)


def solution(mesh):
    tiles, subs = mesh.devices.shape
    fine = Mesh(mesh.devices.reshape(2, tiles // 2, subs // 2, 2), ALL)
    placed = (
        P(ALL, None),
        P(ALL, None),
        P(ALL, None),
        P(ALL, None),
        P(ALL),
        P(ALL),
        P(ALL),
        P(ALL),
        P(ALL),
        P(TILE),
        P(),
        P(),
        P(),
        P(),
        P(ALL, None),
    )
    return jax.shard_map(
        shards,
        mesh=fine,
        in_specs=placed,
        out_specs=(P(ALL, None), P(), P(), P(), P()),
        check_vma=False,
    )
```

```python
import functools

import jax
import jax.numpy as jnp
from jax import lax
from jax.experimental import pallas as pl
from jax.experimental.pallas import tpu as pltpu
from jax.sharding import Mesh, PartitionSpec as P


TOP_NODES = 512
LANES = 128
WORKING_BYTES = 10 * 2**20
TILE = ("half", "near")
ALL = TILE + ("row", "core")
NEAR = ("near", "row")
BF16 = jnp.bfloat16
F32 = jnp.float32
I32 = jnp.int32


def mm(left, right):
    return jnp.dot(left, right, preferred_element_type=F32)


def mm_tn(left, right):
    return lax.dot_general(left, right, (((0,), (0,)), ((), ())), preferred_element_type=F32)


def mm_nt(left, right):
    return lax.dot_general(left, right, (((1,), (1,)), ((), ())), preferred_element_type=F32)


def sigmoid(values):
    return 0.5 + 0.5 * jnp.tanh(0.5 * values)


def rows_onehot(ids, rows):
    n = ids.shape[1]
    hit = lax.broadcasted_iota(I32, (rows, n), 0) == ids
    return jnp.where(hit, 1.0, 0.0).astype(BF16)


def column(ids):
    n = ids.shape[1]
    wide = jnp.broadcast_to(ids.astype(F32), (8, n))
    return wide.T[:, :1].astype(I32)


def cols_onehot(ids, cols):
    n = ids.shape[1]
    hit = lax.broadcasted_iota(I32, (n, cols), 1) == column(ids)
    return jnp.where(hit, 1.0, 0.0).astype(BF16)


def coarse_split(ids):
    at = lax.broadcasted_iota(I32, (16, ids.shape[1]), 0)
    parts = jnp.where(at == 0, ids >> 4, jnp.where(at == 1, ids & 15, 0))
    return parts.astype(F32).astype(BF16)


def node_ids(block):
    codes = block.astype(F32)
    return (codes[2:3].astype(I32), (codes[0:1] * 16.0 + codes[1:2]).astype(I32))


def slots(source, device, core, rows):
    rel = source - device * rows
    before = rel < 0
    after = rel >= rows
    shift_before = jnp.where(core == 0, 3 * rows, 2 * rows)
    shift_after = jnp.where(core == 0, 0, rows)
    return rel + jnp.where(before, shift_before, 0) + jnp.where(after, shift_after, 0)


def ready_kernel(
    dev_ref,
    grid_ref,
    edges_ref,
    weight_ref,
    source_ref,
    target_ref,
    fine_ref,
    coarse_ref,
    edges_out_ref,
    weight_out_ref,
    own_ref,
    picks_ref,
    aims_ref,
    members_ref,
    nodes_ref,
    *,
    subs,
):
    device = dev_ref[0]
    rows, features = grid_ref.shape
    mesh_rows = fine_ref.shape[1]
    level_rows = coarse_ref.shape[1]
    picks = cols_onehot(slots(source_ref[...], device, device % 2, rows), 3 * rows)
    picks_ref[...] = picks[:, rows:]
    raw = target_ref[...]
    aimed = jnp.where(raw >= 0, raw - device * mesh_rows, -1)
    aims_ref[...] = rows_onehot(aimed, mesh_rows)
    local = fine_ref[...] - (device // subs) * level_rows
    members = rows_onehot(local, level_rows)
    members_ref[...] = members
    spot = (
        lax.broadcasted_iota(I32, (mesh_rows, features), 0)
        == lax.broadcasted_iota(I32, (mesh_rows, features), 1)
    )
    spread = jnp.where(spot, 1.0, 0.0).astype(BF16)
    at = lax.broadcasted_iota(I32, (16, mesh_rows), 0)
    codes = mm(coarse_split(coarse_ref[...]), members)
    codes = jnp.where(at == 2, local.astype(F32), codes)
    nodes_ref[...] = mm(codes.astype(BF16), spread).astype(BF16)[:8]
    own_ref[...] = mm(picks[:, :rows], grid_ref[...]).astype(BF16)
    edges_out_ref[...] = edges_ref[...]
    weight_out_ref[...] = weight_ref[...]


def encode_kernel(
    dev_ref,
    partner_ref,
    far_ref,
    mesh_ref,
    edges_ref,
    weight_ref,
    own_ref,
    picks_ref,
    aims_ref,
    members_ref,
    nodes_ref,
    fetched_ref,
    core_ref,
    farpkt_ref,
    keep_ref,
    *,
    factor,
):
    core = dev_ref[0] % 2
    mesh_rows = mesh_ref.shape[0]
    half = keep_ref.shape[0]
    others = jnp.concatenate([partner_ref[...], far_ref[...]], axis=0)
    fetched = (own_ref[...].astype(F32) + mm(picks_ref[...], others)).astype(BF16)
    fetched_ref[...] = fetched
    pre = mm(fetched, weight_ref[...]) + edges_ref[...].astype(F32)
    sig = sigmoid(pre)
    act = (pre * sig).astype(BF16)
    summed = mm(aims_ref[...], act)
    mid = (mesh_ref[...].astype(F32) + factor * summed).astype(BF16)
    part = mm(members_ref[...], mid)
    first = part[:half]
    second = part[half:]
    keep_ref[...] = jnp.where(core == 0, first, second)
    core_ref[:half] = jnp.where(core == 0, second, first).astype(BF16)
    core_ref[half : half + mesh_rows] = mid
    core_ref[half + mesh_rows :] = nodes_ref[...]
    farpkt_ref[:mesh_rows] = mid
    farpkt_ref[mesh_rows:] = nodes_ref[...]


def spread_kernel(dev_ref, mine_ref, other_ref, coarse_ref, out_ref, *, subs, factor):
    device = dev_ref[0]
    core = device % 2
    tile = device // subs
    half, features = mine_ref.shape
    group = features // half
    total = mine_ref[...].astype(F32) + other_ref[...].astype(F32)
    mid = (factor * total).astype(BF16)
    level_rows = coarse_ref.shape[1]
    j = lax.broadcasted_iota(I32, (level_rows, features), 0) - core * half
    lane = lax.broadcasted_iota(I32, (level_rows, features), 1) - (tile % group) * half
    sel = (j == lane) & (j >= 0) & (j < half)
    codes = mm(coarse_split(coarse_ref[...]), jnp.where(sel, 1.0, 0.0).astype(BF16))
    lanes = out_ref.shape[1]
    strips = features // lanes
    tail = jnp.concatenate(
        [codes[r : r + 1, i * lanes : (i + 1) * lanes] for r in range(2) for i in range(strips)],
        axis=0,
    ).astype(BF16)
    for i in range(strips):
        out_ref[i * half : (i + 1) * half] = mid[:, i * lanes : (i + 1) * lanes]
    out_ref[strips * half :] = tail


def pair_kernel(dev_ref, mine_ref, away_ref, out_ref):
    span = mine_ref.shape[0]
    for peer in range(out_ref.shape[0]):
        out_ref[peer, :span] = mine_ref[...]
        out_ref[peer, span:] = away_ref[...]


def placed_blocks(tile, near, group, half):
    count = min(group, near)
    mine = tile // near
    for part in range(2):
        side = mine if part == 0 else 1 - mine
        for first in range(0, near, count):
            at = side * near + first
            yield part, first, count, at // group, pl.multiple_of((at % group) * half, half)


def unpack_half(src_ref, tile, level_ref, ids_ref, half):
    near, span, lanes = src_ref.shape
    _, chunk, features = level_ref.shape
    strips = features // lanes
    unit = span // 2
    ids_ref[...] = jnp.zeros(ids_ref.shape, I32)
    for part, first, count, g, row in placed_blocks(tile, near, chunk // half, half):
        block = src_ref[first : first + count, part * unit : (part + 1) * unit]
        for i in range(strips):
            level_ref[g, pl.ds(row, count * half), i * lanes : (i + 1) * lanes] = block[
                :, i * half : (i + 1) * half
            ].reshape(count * half, lanes)
        codes = jnp.sum(block[:, strips * half :].astype(F32), axis=0)
        ids = codes[:strips] * 16.0 + codes[strips : 2 * strips]
        ids = jnp.concatenate([ids[i : i + 1] for i in range(strips)], axis=1)
        ids_ref[g] += jnp.broadcast_to(ids.astype(I32)[:, :chunk], (8, chunk))


def pooled(mid, ids, weight_ref):
    act = mm(mid, weight_ref[...])
    out = (mid.astype(F32) + act * sigmoid(act)).astype(BF16)
    return out, mm(rows_onehot(ids[:1], TOP_NODES), out)


def first_kernel(
    dev_ref, mine_ref, weight_ref, level_ref, ids_ref, out_ref, part_ref, *, subs, half
):
    unpack_half(mine_ref, dev_ref[0] // subs, level_ref, ids_ref, half)
    part = jnp.zeros(part_ref.shape, F32)
    for g in range(level_ref.shape[0]):
        out, add = pooled(level_ref[g], ids_ref[g], weight_ref)
        out_ref[g] = out
        part = part + add
    part_ref[...] = part


def middle_kernel(
    dev_ref,
    first_level_ref,
    first_ids_ref,
    first_out_ref,
    first_part_ref,
    other_ref,
    core_ref,
    farpkt_ref,
    farin_ref,
    cot_ref,
    edges_ref,
    source_ref,
    target_ref,
    decode_weight_ref,
    middle_weight_ref,
    summit_weight_ref,
    fetched_ref,
    slope_ref,
    act_ref,
    own_ref,
    partner_ref,
    far_ref,
    level_ref,
    summit_in_ref,
    ids_ref,
    out_scr,
    *,
    subs,
    level_rows,
    summit_factor,
    decode_factor,
):
    device = dev_ref[0]
    core = device % 2
    tile = device // subs
    near = other_ref.shape[0]
    tiles = 2 * near
    half = level_rows // 2
    _, groups, chunk, _ = level_ref.shape
    level_ref[core] = first_level_ref[...]
    ids_ref[core] = first_ids_ref[...]
    for g in range(groups):
        out_scr[core, pl.ds(g * chunk, chunk)] = first_out_ref[g]
    away = 1 - core
    unpack_half(other_ref, tile, level_ref.at[away], ids_ref.at[away], half)
    part = jnp.zeros(first_part_ref.shape, F32)
    for g in range(groups):
        out, add = pooled(level_ref[away, g], ids_ref[away, g], middle_weight_ref)
        out_scr[away, pl.ds(g * chunk, chunk)] = out
        part = part + add
    summed = first_part_ref[...] + part
    summit_in = (summit_factor * summed).astype(BF16)
    summit_in_ref[...] = summit_in
    act = mm(summit_in, summit_weight_ref[...])
    sig = sigmoid(act)
    summit_out = (act * sig).astype(BF16)

    mesh_rows = farpkt_ref.shape[0] - 8
    rows = mesh_rows
    sub = device % subs
    far_tile = jnp.where(sub == 0, tile - 1, jnp.where(sub == subs - 1, tile + 1, tile))
    far_tile = jnp.clip(far_tile, 0, tiles - 1)

    def table(ref):
        pieces = []
        for at in (tile, far_tile):
            for h in range(2):
                pieces.append(ref[h, pl.ds(pl.multiple_of(at * half, half), half)])
        return jnp.concatenate(pieces, axis=0)

    own_fine, own_top = node_ids(farpkt_ref[rows:, :rows])
    partner_fine, partner_top = node_ids(core_ref[half + rows :, :rows])
    far_fine, far_top = node_ids(farin_ref[rows:, :rows])
    fine = jnp.concatenate([own_fine, partner_fine, far_fine + level_rows], axis=1)
    top = jnp.concatenate([own_top, partner_top, far_top], axis=1)
    lifted = mm(cols_onehot(fine, 2 * level_rows), table(out_scr)) + mm(
        cols_onehot(top, TOP_NODES), summit_out
    )
    mids = jnp.concatenate(
        [farpkt_ref[:rows], core_ref[half : half + rows], farin_ref[:rows]], axis=0
    )
    wide = (mids.astype(F32) + lifted).astype(BF16)

    place = slots(source_ref[...], device, core, rows)
    fetched = mm(cols_onehot(place, 3 * rows), wide).astype(BF16)
    pre = mm(fetched, decode_weight_ref[...]) + edges_ref[...].astype(F32)
    sig = sigmoid(pre)
    grid_rows = cot_ref.shape[0]
    raw = target_ref[...]
    aimed = jnp.where(raw >= 0, raw - device * grid_rows, -1)
    fetched_ref[...] = fetched
    act_ref[...] = (pre * sig).astype(BF16)
    incoming = mm(cols_onehot(aimed, grid_rows), cot_ref[...]) * decode_factor
    slope = (incoming * (sig * (1.0 + pre * (1.0 - sig)))).astype(BF16)
    slope_ref[...] = slope
    gathered = mm(rows_onehot(place, 3 * rows), slope).astype(BF16)
    returned = mm_nt(gathered, decode_weight_ref[...])
    own_ref[...] = returned[:rows]
    partner_ref[...] = returned[rows : 2 * rows]
    far_ref[...] = returned[2 * rows :].astype(BF16)


def silu_slope(values):
    sig = sigmoid(values)
    return sig * (1.0 + values * (1.0 - sig))


def slope_kernel(dev_ref, fetched_ref, edges_ref, weight_ref, slope_ref):
    pre = mm(fetched_ref[...], weight_ref[...]) + edges_ref[...].astype(F32)
    slope_ref[...] = silu_slope(pre).astype(BF16)


def update_kernel(
    dev_ref,
    grid_ref,
    target_ref,
    act_ref,
    fetched_ref,
    slope_ref,
    level_ref,
    summit_in_ref,
    middle_weight_ref,
    summit_weight_ref,
    update_ref,
    dgrad_ref,
    middle_slope_ref,
    summit_slope_ref,
    *,
    factor,
):
    grid_rows = grid_ref.shape[0]
    raw = target_ref[...]
    aimed = jnp.where(raw >= 0, raw - dev_ref[0] * grid_rows, -1)
    summed = mm(rows_onehot(aimed, grid_rows), act_ref[...])
    update_ref[...] = (grid_ref[...].astype(F32) + factor * summed).astype(BF16)
    dgrad_ref[...] = mm_tn(fetched_ref[...], slope_ref[...])
    for h in range(2):
        for g in range(level_ref.shape[1]):
            act = mm(level_ref[h, g], middle_weight_ref[...])
            middle_slope_ref[h, g] = silu_slope(act).astype(BF16)
    summit_slope_ref[...] = silu_slope(mm(summit_in_ref[...], summit_weight_ref[...]))


def level_kernel(
    dev_ref, own_ref, farin_ref, partner_ref, farpkt_ref, core_ref,
    sum_ref, pkt_ref, keep_ref, *, level_rows
):
    core = dev_ref[0] % 2
    rows = own_ref.shape[0]
    half = level_rows // 2
    grad = own_ref[...] + farin_ref[...].astype(F32)
    sum_ref[...] = grad
    own_fine, _ = node_ids(farpkt_ref[rows:, :rows])
    partner_fine, _ = node_ids(core_ref[half + rows :, :rows])
    partner = partner_ref[...].astype(BF16)
    part = mm(rows_onehot(own_fine, level_rows), grad.astype(BF16)) + mm(
        rows_onehot(partner_fine, level_rows), partner
    )
    first = part[:half]
    second = part[half:]
    keep_ref[...] = jnp.where(core == 0, first, second)
    pkt_ref[:half] = jnp.where(core == 0, second, first).astype(BF16)
    pkt_ref[half:] = partner


def back_kernel(
    dev_ref,
    mine_ref,
    other_ref,
    middle_slope_ref,
    summit_slope_ref,
    ids_ref,
    sum_ref,
    partnerin_ref,
    farpkt_ref,
    coarse_ref,
    fetched_ref,
    slope_ref,
    target_ref,
    dgrad_ref,
    middle_weight_ref,
    summit_weight_ref,
    send_ref,
    keep_ref,
    grad_ref,
    top_ref,
    top_back_ref,
    *,
    subs,
    level_rows,
    summit_factor,
    middle_factor,
    encode_factor,
):
    device = dev_ref[0]
    core = device % 2
    tile = device // subs
    near, pair, features = mine_ref.shape
    half = pair // 2
    _, groups, chunk, _ = grad_ref.shape
    group = chunk // half
    for part, first, count, g, row in placed_blocks(tile, near, group, half):
        for src, which in ((mine_ref, core), (other_ref, 1 - core)):
            grad_ref[which, g, pl.ds(row, count * half)] = src[
                first : first + count, part * half : (part + 1) * half
            ].reshape(count * half, features)
    total = jnp.zeros((TOP_NODES, features), F32)
    for g in range(groups):
        for h in range(2):
            total = total + mm(rows_onehot(ids_ref[h, g][:1], TOP_NODES), grad_ref[h, g])
    summit_slope = (total * summit_slope_ref[...]).astype(BF16)
    top_ref[...] = summit_slope
    summit_back = mm_nt(summit_slope, summit_weight_ref[...]).astype(BF16)
    top_back_ref[...] = summit_back
    spot = pl.multiple_of((tile % group) * half, half)

    def own(ref):
        pieces = [ref[h, tile // group, pl.ds(spot, half)] for h in range(2)]
        return jnp.concatenate(pieces, axis=0).astype(F32)

    level_total = own(grad_ref) + summit_factor * mm(
        cols_onehot(coarse_ref[...], TOP_NODES), summit_back
    )
    slope = (level_total * own(middle_slope_ref)).astype(BF16)
    back = (level_total + mm_nt(slope, middle_weight_ref[...])).astype(BF16)
    rows = sum_ref.shape[0]
    own_fine, _ = node_ids(farpkt_ref[rows:, :rows])
    mesh_total = (
        sum_ref[...]
        + partnerin_ref[half:].astype(F32)
        + middle_factor * mm(cols_onehot(own_fine, level_rows), back)
    )
    raw = target_ref[...]
    aimed = jnp.where(raw >= 0, raw - device * rows, -1)
    upstream = mm(cols_onehot(aimed, rows), mesh_total.astype(BF16)) * encode_factor
    slope = (upstream * slope_ref[...].astype(F32)).astype(BF16)
    egrad = mm_tn(fetched_ref[...], slope)
    dgrad = dgrad_ref[...]
    send_ref[...] = jnp.where(core == 0, dgrad, egrad).astype(BF16)
    keep_ref[...] = jnp.where(core == 0, egrad, dgrad)


def lift_kernel(
    dev_ref, grad_ref, middle_slope_ref, top_back_ref, ids_ref, slope_ref, *, summit_factor
):
    for g in range(grad_ref.shape[1]):
        for h in range(2):
            lifted = mm_tn(rows_onehot(ids_ref[h, g][:1], TOP_NODES), top_back_ref[...])
            level_total = grad_ref[h, g].astype(F32) + summit_factor * lifted
            slope_ref[h, g] = (level_total * middle_slope_ref[h, g].astype(F32)).astype(BF16)


def late_kernel(dev_ref, level_ref, slope_ref, middle_grad_ref):
    middle_grad = jnp.zeros(middle_grad_ref.shape, F32)
    for g in range(level_ref.shape[1]):
        for h in range(2):
            middle_grad = middle_grad + mm_tn(level_ref[h, g], slope_ref[h, g])
    middle_grad_ref[...] = middle_grad


def add_kernel(dev_ref, mine_ref, other_ref, out_ref):
    rows = out_ref.shape[0]
    total = mine_ref[...].astype(F32) + other_ref[:rows].astype(F32)
    out_ref[...] = total.astype(BF16)


def gather_kernel(dev_ref, parts_ref, out_ref):
    total = parts_ref[0].astype(F32)
    for peer in range(1, parts_ref.shape[0]):
        total = total + parts_ref[peer].astype(F32)
    out_ref[...] = total.astype(BF16)


def copies_kernel(dev_ref, mine_ref, other_ref, out_ref):
    total = (mine_ref[...].astype(F32) + other_ref[...].astype(F32)).astype(BF16)
    for peer in range(out_ref.shape[0]):
        out_ref[peer] = total


def top_kernel(dev_ref, summit_in_ref, top_ref, summit_grad_ref):
    summit_grad_ref[...] = mm_tn(summit_in_ref[...], top_ref[...])


def call(body, outs, args, scratch=(), **static):
    vmem = pl.BlockSpec(memory_space=pltpu.VMEM)
    smem = pl.BlockSpec(memory_space=pltpu.SMEM)
    specs = [smem if a.ndim == 1 else vmem for a in args]
    single = not isinstance(outs, (list, tuple))
    held = [a for a in args if a.ndim > 1] + ([outs] if single else list(outs)) + list(scratch)
    limit = sum(a.size * a.dtype.itemsize for a in held) + WORKING_BYTES
    limit = min(limit, 60 * 2**20)
    return pl.pallas_call(
        functools.partial(body, **static),
        out_shape=outs,
        in_specs=specs,
        out_specs=vmem if single else [vmem] * len(outs),
        scratch_shapes=[pltpu.VMEM(s.shape, s.dtype) for s in scratch],
        compiler_params=pltpu.CompilerParams(vmem_limit_bytes=limit),
    )(*args)


def shape(dims, dtype):
    return jax.ShapeDtypeStruct(dims, dtype)


def shards(
    grid_feats,
    mesh_feats,
    encode_edges,
    decode_edges,
    encode_source,
    encode_target,
    decode_source,
    decode_target,
    owner_fine,
    owner_coarse,
    encode_weight,
    decode_weight,
    middle_weight,
    summit_weight,
    cotangent,
):
    rows, features = grid_feats.shape
    mesh_rows = mesh_feats.shape[0]
    level_rows = owner_coarse.shape[0]
    half = level_rows // 2
    tiles = lax.axis_size(TILE)
    subs = lax.axis_size("row") * lax.axis_size("core")
    devices = tiles * subs
    peers = devices // 4
    near = tiles // 2
    edges = encode_source.shape[0]
    swap = [(0, 1), (1, 0)]
    beside = []
    for left in range(1, devices - 1, 2):
        beside += [(left, left + 1), (left + 1, left)]
    device = lax.axis_index(ALL).astype(I32)
    dev = device.reshape(1)
    core = device % 2
    encode_factor = mesh_rows / edges
    decode_factor = rows / decode_source.shape[0]
    middle_factor = level_rows / (mesh_rows * subs)
    summit_factor = TOP_NODES / (level_rows * tiles)
    group = min(features // half, tiles)
    groups = tiles // group
    chunk = group * half

    grid_far = lax.ppermute(grid_feats, ALL, beside)
    grid_partner = lax.ppermute(grid_feats, "core", swap)
    edges_in, weight_in, own_rows, picks, aims, members, nodes = call(
        ready_kernel,
        [
            shape((edges, features), BF16),
            shape((features, features), BF16),
            shape((edges, features), BF16),
            shape((edges, 2 * rows), BF16),
            shape((mesh_rows, edges), BF16),
            shape((level_rows, mesh_rows), BF16),
            shape((8, features), BF16),
        ],
        [
            dev,
            grid_feats,
            encode_edges,
            encode_weight,
            encode_source[None],
            encode_target[None],
            owner_fine[None],
            owner_coarse[None],
        ],
        subs=subs,
    )
    fetched, core_pkt, far_pkt, keep = call(
        encode_kernel,
        [
            shape((edges, features), BF16),
            shape((half + mesh_rows + 8, features), BF16),
            shape((mesh_rows + 8, features), BF16),
            shape((half, features), F32),
        ],
        [
            dev,
            grid_partner,
            grid_far,
            mesh_feats,
            edges_in,
            weight_in,
            own_rows,
            picks,
            aims,
            members,
            nodes,
        ],
        factor=encode_factor,
    )
    core_in = lax.ppermute(core_pkt, "core", swap)
    far_in = lax.ppermute(far_pkt, ALL, beside)
    mine = call(add_kernel, shape((half, features), BF16), [dev, keep, core_in])
    other = lax.ppermute(mine, "row", swap)
    packet = call(
        spread_kernel,
        shape(((features // LANES) * half + 8, LANES), BF16),
        [dev, mine, other, owner_coarse[None]],
        subs=subs,
        factor=middle_factor,
    )
    away = lax.ppermute(packet, "half", swap)
    slope = call(
        slope_kernel, shape((edges, features), BF16), [dev, fetched, edges_in, weight_in]
    )
    packed = call(
        pair_kernel, shape((near, 2 * packet.shape[0], LANES), BF16), [dev, packet, away]
    )
    mids = lax.all_to_all(packed, "near", 0, 0)
    mids_other = lax.ppermute(mids, "core", swap)
    firsts = call(
        first_kernel,
        [
            shape((groups, chunk, features), BF16),
            shape((groups, 8, chunk), I32),
            shape((groups, chunk, features), BF16),
            shape((TOP_NODES, features), F32),
        ],
        [dev, mids, middle_weight],
        subs=subs,
        half=half,
    )
    full = (2, groups, chunk, features)
    (
        decode_fetched,
        decode_slope,
        decode_act,
        own,
        partner,
        far,
        level,
        summit_in,
        ids,
    ) = call(
        middle_kernel,
        [
            shape(decode_edges.shape, BF16),
            shape(decode_edges.shape, BF16),
            shape(decode_edges.shape, BF16),
            shape((mesh_rows, features), F32),
            shape((mesh_rows, features), F32),
            shape((mesh_rows, features), BF16),
            shape(full, BF16),
            shape((TOP_NODES, features), BF16),
            shape((2, groups, 8, chunk), I32),
        ],
        [
            dev,
            *firsts,
            mids_other,
            core_in,
            far_pkt,
            far_in,
            cotangent,
            decode_edges,
            decode_source[None],
            decode_target[None],
            decode_weight,
            middle_weight,
            summit_weight,
        ],
        scratch=[
            shape((2, tiles * half, features), BF16),
        ],
        subs=subs,
        level_rows=level_rows,
        summit_factor=summit_factor,
        decode_factor=decode_factor,
    )
    far_back = lax.ppermute(far, ALL, beside)
    grid_update, dgrad, middle_slope, summit_slope = call(
        update_kernel,
        [
            shape((rows, features), BF16),
            shape((features, features), F32),
            shape(full, BF16),
            shape((TOP_NODES, features), F32),
        ],
        [
            dev,
            grid_feats,
            decode_target[None],
            decode_act,
            decode_fetched,
            decode_slope,
            level,
            summit_in,
            middle_weight,
            summit_weight,
        ],
        factor=decode_factor,
    )
    grad_sum, core_pkt, keep = call(
        level_kernel,
        [
            shape((mesh_rows, features), F32),
            shape((half + mesh_rows, features), BF16),
            shape((half, features), F32),
        ],
        [dev, own, far_back, partner, far_pkt, core_in],
        level_rows=level_rows,
    )
    back_in = lax.ppermute(core_pkt, "core", swap)
    mine = call(add_kernel, shape((half, features), BF16), [dev, keep, back_in])
    other = lax.ppermute(mine, "row", swap)
    total = call(add_kernel, shape((half, features), BF16), [dev, mine, other])
    away = lax.ppermute(total, "half", swap)
    packed = call(pair_kernel, shape((near, 2 * half, features), BF16), [dev, total, away])
    grads = lax.all_to_all(packed, "near", 0, 0)
    grads_other = lax.ppermute(grads, "core", swap)
    send, keep, level_back, top, top_back = call(
        back_kernel,
        [
            shape((features, features), BF16),
            shape((features, features), F32),
            shape(full, BF16),
            shape((TOP_NODES, features), BF16),
            shape((TOP_NODES, features), BF16),
        ],
        [
            dev,
            grads,
            grads_other,
            middle_slope,
            summit_slope,
            ids,
            grad_sum,
            back_in,
            far_pkt,
            owner_coarse[None],
            fetched,
            slope,
            encode_target[None],
            dgrad,
            middle_weight,
            summit_weight,
        ],
        subs=subs,
        level_rows=level_rows,
        summit_factor=summit_factor,
        middle_factor=middle_factor,
        encode_factor=encode_factor,
    )
    received = lax.ppermute(send, "core", swap)
    lift_slope = call(
        lift_kernel,
        shape(full, BF16),
        [dev, level_back, middle_slope, top_back, ids],
        summit_factor=summit_factor,
    )
    share = call(add_kernel, shape((features, features), BF16), [dev, keep, received])
    share = share.reshape(peers, features // peers, features)
    parts = lax.all_to_all(share, NEAR, 0, 0)
    inside = call(gather_kernel, shape(parts.shape[1:], BF16), [dev, parts])
    away = lax.ppermute(inside, "half", swap)
    copies = call(copies_kernel, shape(parts.shape, BF16), [dev, inside, away])
    mine = lax.all_to_all(copies, NEAR, 0, 0).reshape(features, features)
    other = lax.ppermute(mine, "core", swap)
    summit_grad = call(
        top_kernel, shape((features, features), F32), [dev, summit_in, top]
    )
    middle_grad = call(
        late_kernel, shape((features, features), F32), [dev, level, lift_slope]
    )
    encode_grad = jnp.where(core == 0, mine, other).astype(F32)
    decode_grad = jnp.where(core == 0, other, mine).astype(F32)
    return (grid_update, encode_grad, decode_grad, middle_grad, summit_grad)


def solution(mesh):
    tiles, subs = mesh.devices.shape
    fine = Mesh(mesh.devices.reshape(2, tiles // 2, subs // 2, 2), ALL)
    placed = (
        P(ALL, None),
        P(ALL, None),
        P(ALL, None),
        P(ALL, None),
        P(ALL),
        P(ALL),
        P(ALL),
        P(ALL),
        P(ALL),
        P(TILE),
        P(),
        P(),
        P(),
        P(),
        P(ALL, None),
    )
    return jax.shard_map(
        shards,
        mesh=fine,
        in_specs=placed,
        out_specs=(P(ALL, None), P(), P(), P(), P()),
        check_vma=False,
    )
```

```python
import functools

import jax
import jax.numpy as jnp
from jax import lax
from jax.experimental import pallas as pl
from jax.experimental.pallas import tpu as pltpu
from jax.sharding import Mesh, PartitionSpec as P


TOP_NODES = 512
LANES = 128
WORKING_BYTES = 10 * 2**20
TILE = ("half", "near")
ALL = TILE + ("row", "core")
NEAR = ("near", "row")
BF16 = jnp.bfloat16
F32 = jnp.float32
I32 = jnp.int32


def mm(left, right):
    return jnp.dot(left, right, preferred_element_type=F32)


def mm_tn(left, right):
    return lax.dot_general(left, right, (((0,), (0,)), ((), ())), preferred_element_type=F32)


def mm_nt(left, right):
    return lax.dot_general(left, right, (((1,), (1,)), ((), ())), preferred_element_type=F32)


def sigmoid(values):
    return 0.5 + 0.5 * jnp.tanh(0.5 * values)


def rows_onehot(ids, rows):
    n = ids.shape[1]
    hit = lax.broadcasted_iota(I32, (rows, n), 0) == ids
    return jnp.where(hit, 1.0, 0.0).astype(BF16)


def column(ids):
    n = ids.shape[1]
    wide = jnp.broadcast_to(ids.astype(F32), (8, n))
    return wide.T[:, :1].astype(I32)


def cols_onehot(ids, cols):
    n = ids.shape[1]
    hit = lax.broadcasted_iota(I32, (n, cols), 1) == column(ids)
    return jnp.where(hit, 1.0, 0.0).astype(BF16)


def coarse_split(ids):
    at = lax.broadcasted_iota(I32, (16, ids.shape[1]), 0)
    parts = jnp.where(at == 0, ids >> 4, jnp.where(at == 1, ids & 15, 0))
    return parts.astype(F32).astype(BF16)


def node_ids(block):
    codes = block.astype(F32)
    return (codes[2:3].astype(I32), (codes[0:1] * 16.0 + codes[1:2]).astype(I32))


def slots(source, device, core, rows):
    rel = source - device * rows
    before = rel < 0
    after = rel >= rows
    shift_before = jnp.where(core == 0, 3 * rows, 2 * rows)
    shift_after = jnp.where(core == 0, 0, rows)
    return rel + jnp.where(before, shift_before, 0) + jnp.where(after, shift_after, 0)


def ready_kernel(
    dev_ref,
    grid_ref,
    edges_ref,
    weight_ref,
    source_ref,
    target_ref,
    fine_ref,
    coarse_ref,
    edges_out_ref,
    weight_out_ref,
    own_ref,
    picks_ref,
    aims_ref,
    members_ref,
    nodes_ref,
    *,
    subs,
):
    device = dev_ref[0]
    rows, features = grid_ref.shape
    mesh_rows = fine_ref.shape[1]
    level_rows = coarse_ref.shape[1]
    picks = cols_onehot(slots(source_ref[...], device, device % 2, rows), 3 * rows)
    picks_ref[...] = picks[:, rows:]
    raw = target_ref[...]
    aimed = jnp.where(raw >= 0, raw - device * mesh_rows, -1)
    aims_ref[...] = rows_onehot(aimed, mesh_rows)
    local = fine_ref[...] - (device // subs) * level_rows
    members = rows_onehot(local, level_rows)
    members_ref[...] = members
    spot = (
        lax.broadcasted_iota(I32, (mesh_rows, features), 0)
        == lax.broadcasted_iota(I32, (mesh_rows, features), 1)
    )
    spread = jnp.where(spot, 1.0, 0.0).astype(BF16)
    at = lax.broadcasted_iota(I32, (16, mesh_rows), 0)
    codes = mm(coarse_split(coarse_ref[...]), members)
    codes = jnp.where(at == 2, local.astype(F32), codes)
    nodes_ref[...] = mm(codes.astype(BF16), spread).astype(BF16)[:8]
    own_ref[...] = mm(picks[:, :rows], grid_ref[...]).astype(BF16)
    edges_out_ref[...] = edges_ref[...]
    weight_out_ref[...] = weight_ref[...]


def encode_kernel(
    dev_ref,
    partner_ref,
    far_ref,
    mesh_ref,
    edges_ref,
    weight_ref,
    own_ref,
    picks_ref,
    aims_ref,
    members_ref,
    nodes_ref,
    fetched_ref,
    core_ref,
    farpkt_ref,
    keep_ref,
    *,
    factor,
):
    core = dev_ref[0] % 2
    mesh_rows = mesh_ref.shape[0]
    half = keep_ref.shape[0]
    others = jnp.concatenate([partner_ref[...], far_ref[...]], axis=0)
    fetched = (own_ref[...].astype(F32) + mm(picks_ref[...], others)).astype(BF16)
    fetched_ref[...] = fetched
    pre = mm(fetched, weight_ref[...]) + edges_ref[...].astype(F32)
    sig = sigmoid(pre)
    act = (pre * sig).astype(BF16)
    summed = mm(aims_ref[...], act)
    mid = (mesh_ref[...].astype(F32) + factor * summed).astype(BF16)
    part = mm(members_ref[...], mid)
    first = part[:half]
    second = part[half:]
    keep_ref[...] = jnp.where(core == 0, first, second)
    core_ref[:half] = jnp.where(core == 0, second, first).astype(BF16)
    core_ref[half : half + mesh_rows] = mid
    core_ref[half + mesh_rows :] = nodes_ref[...]
    farpkt_ref[:mesh_rows] = mid
    farpkt_ref[mesh_rows:] = nodes_ref[...]


def spread_kernel(dev_ref, mine_ref, other_ref, coarse_ref, out_ref, *, subs, factor):
    device = dev_ref[0]
    core = device % 2
    tile = device // subs
    half, features = mine_ref.shape
    group = features // half
    total = mine_ref[...].astype(F32) + other_ref[...].astype(F32)
    mid = (factor * total).astype(BF16)
    level_rows = coarse_ref.shape[1]
    j = lax.broadcasted_iota(I32, (level_rows, features), 0) - core * half
    lane = lax.broadcasted_iota(I32, (level_rows, features), 1) - (tile % group) * half
    sel = (j == lane) & (j >= 0) & (j < half)
    codes = mm(coarse_split(coarse_ref[...]), jnp.where(sel, 1.0, 0.0).astype(BF16))
    lanes = out_ref.shape[1]
    strips = features // lanes
    tail = jnp.concatenate(
        [codes[r : r + 1, i * lanes : (i + 1) * lanes] for r in range(2) for i in range(strips)],
        axis=0,
    ).astype(BF16)
    for i in range(strips):
        out_ref[i * half : (i + 1) * half] = mid[:, i * lanes : (i + 1) * lanes]
    out_ref[strips * half :] = tail


def pair_kernel(dev_ref, mine_ref, away_ref, out_ref):
    span = mine_ref.shape[0]
    for peer in range(out_ref.shape[0]):
        out_ref[peer, :span] = mine_ref[...]
        out_ref[peer, span:] = away_ref[...]


def placed_blocks(tile, near, group, half):
    count = min(group, near)
    mine = tile // near
    for part in range(2):
        side = mine if part == 0 else 1 - mine
        for first in range(0, near, count):
            at = side * near + first
            yield part, first, count, at // group, pl.multiple_of((at % group) * half, half)


def unpack_half(src_ref, tile, level_ref, ids_ref, half):
    near, span, lanes = src_ref.shape
    _, chunk, features = level_ref.shape
    strips = features // lanes
    unit = span // 2
    ids_ref[...] = jnp.zeros(ids_ref.shape, I32)
    for part, first, count, g, row in placed_blocks(tile, near, chunk // half, half):
        block = src_ref[first : first + count, part * unit : (part + 1) * unit]
        for i in range(strips):
            level_ref[g, pl.ds(row, count * half), i * lanes : (i + 1) * lanes] = block[
                :, i * half : (i + 1) * half
            ].reshape(count * half, lanes)
        codes = jnp.sum(block[:, strips * half :].astype(F32), axis=0)
        ids = codes[:strips] * 16.0 + codes[strips : 2 * strips]
        ids = jnp.concatenate([ids[i : i + 1] for i in range(strips)], axis=1)
        ids_ref[g] += jnp.broadcast_to(ids.astype(I32)[:, :chunk], (8, chunk))


def pooled(mid, ids, weight_ref):
    act = mm(mid, weight_ref[...])
    out = (mid.astype(F32) + act * sigmoid(act)).astype(BF16)
    return out, mm(rows_onehot(ids[:1], TOP_NODES), out)


def first_kernel(
    dev_ref, mine_ref, weight_ref, level_ref, ids_ref, out_ref, part_ref, *, subs, half
):
    unpack_half(mine_ref, dev_ref[0] // subs, level_ref, ids_ref, half)
    part = jnp.zeros(part_ref.shape, F32)
    for g in range(level_ref.shape[0]):
        out, add = pooled(level_ref[g], ids_ref[g], weight_ref)
        out_ref[g] = out
        part = part + add
    part_ref[...] = part


def middle_kernel(
    dev_ref,
    first_level_ref,
    first_ids_ref,
    first_out_ref,
    first_part_ref,
    other_ref,
    core_ref,
    farpkt_ref,
    farin_ref,
    picks_ref,
    returns_ref,
    incoming_ref,
    edges_ref,
    decode_weight_ref,
    middle_weight_ref,
    summit_weight_ref,
    fetched_ref,
    slope_ref,
    act_ref,
    own_ref,
    partner_ref,
    far_ref,
    level_ref,
    summit_in_ref,
    ids_ref,
    out_scr,
    *,
    subs,
    level_rows,
    summit_factor,
):
    device = dev_ref[0]
    core = device % 2
    tile = device // subs
    near = other_ref.shape[0]
    tiles = 2 * near
    half = level_rows // 2
    _, groups, chunk, _ = level_ref.shape
    level_ref[core] = first_level_ref[...]
    ids_ref[core] = first_ids_ref[...]
    for g in range(groups):
        out_scr[core, pl.ds(g * chunk, chunk)] = first_out_ref[g]
    away = 1 - core
    unpack_half(other_ref, tile, level_ref.at[away], ids_ref.at[away], half)
    part = jnp.zeros(first_part_ref.shape, F32)
    for g in range(groups):
        out, add = pooled(level_ref[away, g], ids_ref[away, g], middle_weight_ref)
        out_scr[away, pl.ds(g * chunk, chunk)] = out
        part = part + add
    summed = first_part_ref[...] + part
    summit_in = (summit_factor * summed).astype(BF16)
    summit_in_ref[...] = summit_in
    act = mm(summit_in, summit_weight_ref[...])
    sig = sigmoid(act)
    summit_out = (act * sig).astype(BF16)

    mesh_rows = farpkt_ref.shape[0] - 8
    rows = mesh_rows
    sub = device % subs
    far_tile = jnp.where(sub == 0, tile - 1, jnp.where(sub == subs - 1, tile + 1, tile))
    far_tile = jnp.clip(far_tile, 0, tiles - 1)

    def table(ref):
        pieces = []
        for at in (tile, far_tile):
            for h in range(2):
                pieces.append(ref[h, pl.ds(pl.multiple_of(at * half, half), half)])
        return jnp.concatenate(pieces, axis=0)

    own_fine, own_top = node_ids(farpkt_ref[rows:, :rows])
    partner_fine, partner_top = node_ids(core_ref[half + rows :, :rows])
    far_fine, far_top = node_ids(farin_ref[rows:, :rows])
    fine = jnp.concatenate([own_fine, partner_fine, far_fine + level_rows], axis=1)
    top = jnp.concatenate([own_top, partner_top, far_top], axis=1)
    lifted = mm(cols_onehot(fine, 2 * level_rows), table(out_scr)) + mm(
        cols_onehot(top, TOP_NODES), summit_out
    )
    mids = jnp.concatenate(
        [farpkt_ref[:rows], core_ref[half : half + rows], farin_ref[:rows]], axis=0
    )
    wide = (mids.astype(F32) + lifted).astype(BF16)

    fetched = mm(picks_ref[...], wide).astype(BF16)
    pre = mm(fetched, decode_weight_ref[...]) + edges_ref[...].astype(F32)
    sig = sigmoid(pre)
    fetched_ref[...] = fetched
    act_ref[...] = (pre * sig).astype(BF16)
    slope = (incoming_ref[...] * (sig * (1.0 + pre * (1.0 - sig)))).astype(BF16)
    slope_ref[...] = slope
    gathered = mm(returns_ref[...], slope).astype(BF16)
    returned = mm_nt(gathered, decode_weight_ref[...])
    own_ref[...] = returned[:rows]
    partner_ref[...] = returned[rows : 2 * rows]
    far_ref[...] = returned[2 * rows :].astype(BF16)


def silu_slope(values):
    sig = sigmoid(values)
    return sig * (1.0 + values * (1.0 - sig))


def slope_kernel(
    dev_ref,
    fetched_ref,
    edges_ref,
    weight_ref,
    source_ref,
    target_ref,
    encode_target_ref,
    cot_ref,
    slope_ref,
    picks_ref,
    returns_ref,
    aims_ref,
    incoming_ref,
    back_aims_ref,
    *,
    factor,
):
    device = dev_ref[0]
    rows = cot_ref.shape[0]
    place = slots(source_ref[...], device, device % 2, rows)
    picks_ref[...] = cols_onehot(place, 3 * rows)
    returns_ref[...] = rows_onehot(place, 3 * rows)
    raw = target_ref[...]
    aimed = jnp.where(raw >= 0, raw - device * rows, -1)
    aims_ref[...] = rows_onehot(aimed, rows)
    incoming_ref[...] = mm(cols_onehot(aimed, rows), cot_ref[...]) * factor
    raw = encode_target_ref[...]
    mesh_rows = back_aims_ref.shape[1]
    aimed = jnp.where(raw >= 0, raw - device * mesh_rows, -1)
    back_aims_ref[...] = cols_onehot(aimed, mesh_rows)
    pre = mm(fetched_ref[...], weight_ref[...]) + edges_ref[...].astype(F32)
    slope_ref[...] = silu_slope(pre).astype(BF16)


def update_kernel(
    dev_ref,
    grid_ref,
    aims_ref,
    act_ref,
    fetched_ref,
    slope_ref,
    level_ref,
    summit_in_ref,
    middle_weight_ref,
    summit_weight_ref,
    update_ref,
    dgrad_ref,
    middle_slope_ref,
    summit_slope_ref,
    *,
    factor,
):
    summed = mm(aims_ref[...], act_ref[...])
    update_ref[...] = (grid_ref[...].astype(F32) + factor * summed).astype(BF16)
    dgrad_ref[...] = mm_tn(fetched_ref[...], slope_ref[...])
    for h in range(2):
        for g in range(level_ref.shape[1]):
            act = mm(level_ref[h, g], middle_weight_ref[...])
            middle_slope_ref[h, g] = silu_slope(act).astype(BF16)
    summit_slope_ref[...] = silu_slope(mm(summit_in_ref[...], summit_weight_ref[...]))


def level_kernel(
    dev_ref, own_ref, farin_ref, partner_ref, farpkt_ref, core_ref,
    sum_ref, pkt_ref, keep_ref, *, level_rows
):
    core = dev_ref[0] % 2
    rows = own_ref.shape[0]
    half = level_rows // 2
    grad = own_ref[...] + farin_ref[...].astype(F32)
    sum_ref[...] = grad
    own_fine, _ = node_ids(farpkt_ref[rows:, :rows])
    partner_fine, _ = node_ids(core_ref[half + rows :, :rows])
    partner = partner_ref[...].astype(BF16)
    part = mm(rows_onehot(own_fine, level_rows), grad.astype(BF16)) + mm(
        rows_onehot(partner_fine, level_rows), partner
    )
    first = part[:half]
    second = part[half:]
    keep_ref[...] = jnp.where(core == 0, first, second)
    pkt_ref[:half] = jnp.where(core == 0, second, first).astype(BF16)
    pkt_ref[half:] = partner


def tops_kernel(dev_ref, ids_ref, coarse_ref, farpkt_ref, tops_ref, lifts_ref, fine_ref):
    for h in range(2):
        for g in range(ids_ref.shape[1]):
            tops_ref[h, g] = rows_onehot(ids_ref[h, g][:1], TOP_NODES)
    lifts_ref[...] = cols_onehot(coarse_ref[...], TOP_NODES)
    rows = fine_ref.shape[0]
    own_fine, _ = node_ids(farpkt_ref[rows:, :rows])
    fine_ref[...] = cols_onehot(own_fine, fine_ref.shape[1])


def back_kernel(
    dev_ref,
    mine_ref,
    other_ref,
    middle_slope_ref,
    summit_slope_ref,
    tops_ref,
    sum_ref,
    partnerin_ref,
    fine_ref,
    lifts_ref,
    fetched_ref,
    slope_ref,
    aims_ref,
    dgrad_ref,
    middle_weight_ref,
    summit_weight_ref,
    send_ref,
    keep_ref,
    grad_ref,
    top_ref,
    top_back_ref,
    *,
    subs,
    summit_factor,
    middle_factor,
    encode_factor,
):
    device = dev_ref[0]
    core = device % 2
    tile = device // subs
    near, pair, features = mine_ref.shape
    half = pair // 2
    _, groups, chunk, _ = grad_ref.shape
    group = chunk // half
    for part, first, count, g, row in placed_blocks(tile, near, group, half):
        for src, which in ((mine_ref, core), (other_ref, 1 - core)):
            grad_ref[which, g, pl.ds(row, count * half)] = src[
                first : first + count, part * half : (part + 1) * half
            ].reshape(count * half, features)
    total = jnp.zeros((TOP_NODES, features), F32)
    for g in range(groups):
        for h in range(2):
            total = total + mm(tops_ref[h, g], grad_ref[h, g])
    summit_slope = (total * summit_slope_ref[...]).astype(BF16)
    top_ref[...] = summit_slope
    summit_back = mm_nt(summit_slope, summit_weight_ref[...]).astype(BF16)
    top_back_ref[...] = summit_back
    spot = pl.multiple_of((tile % group) * half, half)

    def own(ref):
        pieces = [ref[h, tile // group, pl.ds(spot, half)] for h in range(2)]
        return jnp.concatenate(pieces, axis=0).astype(F32)

    level_total = own(grad_ref) + summit_factor * mm(lifts_ref[...], summit_back)
    slope = (level_total * own(middle_slope_ref)).astype(BF16)
    back = (level_total + mm_nt(slope, middle_weight_ref[...])).astype(BF16)
    mesh_total = (
        sum_ref[...]
        + partnerin_ref[half:].astype(F32)
        + middle_factor * mm(fine_ref[...], back)
    )
    upstream = mm(aims_ref[...], mesh_total.astype(BF16)) * encode_factor
    slope = (upstream * slope_ref[...].astype(F32)).astype(BF16)
    egrad = mm_tn(fetched_ref[...], slope)
    dgrad = dgrad_ref[...]
    send_ref[...] = jnp.where(core == 0, dgrad, egrad).astype(BF16)
    keep_ref[...] = jnp.where(core == 0, egrad, dgrad)


def lift_kernel(
    dev_ref, grad_ref, middle_slope_ref, top_back_ref, tops_ref, slope_ref, *, summit_factor
):
    for g in range(grad_ref.shape[1]):
        for h in range(2):
            lifted = mm_tn(tops_ref[h, g], top_back_ref[...])
            level_total = grad_ref[h, g].astype(F32) + summit_factor * lifted
            slope_ref[h, g] = (level_total * middle_slope_ref[h, g].astype(F32)).astype(BF16)


def late_kernel(dev_ref, level_ref, slope_ref, middle_grad_ref):
    middle_grad = jnp.zeros(middle_grad_ref.shape, F32)
    for g in range(level_ref.shape[1]):
        for h in range(2):
            middle_grad = middle_grad + mm_tn(level_ref[h, g], slope_ref[h, g])
    middle_grad_ref[...] = middle_grad


def add_kernel(dev_ref, mine_ref, other_ref, out_ref):
    rows = out_ref.shape[0]
    total = mine_ref[...].astype(F32) + other_ref[:rows].astype(F32)
    out_ref[...] = total.astype(BF16)


def gather_kernel(dev_ref, parts_ref, out_ref):
    total = parts_ref[0].astype(F32)
    for peer in range(1, parts_ref.shape[0]):
        total = total + parts_ref[peer].astype(F32)
    out_ref[...] = total.astype(BF16)


def copies_kernel(dev_ref, mine_ref, other_ref, out_ref):
    total = (mine_ref[...].astype(F32) + other_ref[...].astype(F32)).astype(BF16)
    for peer in range(out_ref.shape[0]):
        out_ref[peer] = total


def top_kernel(dev_ref, summit_in_ref, top_ref, summit_grad_ref):
    summit_grad_ref[...] = mm_tn(summit_in_ref[...], top_ref[...])


def call(body, outs, args, scratch=(), **static):
    vmem = pl.BlockSpec(memory_space=pltpu.VMEM)
    smem = pl.BlockSpec(memory_space=pltpu.SMEM)
    specs = [smem if a.ndim == 1 else vmem for a in args]
    single = not isinstance(outs, (list, tuple))
    held = [a for a in args if a.ndim > 1] + ([outs] if single else list(outs)) + list(scratch)
    limit = sum(a.size * a.dtype.itemsize for a in held) + WORKING_BYTES
    limit = min(limit, 60 * 2**20)
    return pl.pallas_call(
        functools.partial(body, **static),
        out_shape=outs,
        in_specs=specs,
        out_specs=vmem if single else [vmem] * len(outs),
        scratch_shapes=[pltpu.VMEM(s.shape, s.dtype) for s in scratch],
        compiler_params=pltpu.CompilerParams(vmem_limit_bytes=limit),
    )(*args)


def shape(dims, dtype):
    return jax.ShapeDtypeStruct(dims, dtype)


def shards(
    grid_feats,
    mesh_feats,
    encode_edges,
    decode_edges,
    encode_source,
    encode_target,
    decode_source,
    decode_target,
    owner_fine,
    owner_coarse,
    encode_weight,
    decode_weight,
    middle_weight,
    summit_weight,
    cotangent,
):
    rows, features = grid_feats.shape
    mesh_rows = mesh_feats.shape[0]
    level_rows = owner_coarse.shape[0]
    half = level_rows // 2
    tiles = lax.axis_size(TILE)
    subs = lax.axis_size("row") * lax.axis_size("core")
    devices = tiles * subs
    peers = devices // 4
    near = tiles // 2
    edges = encode_source.shape[0]
    swap = [(0, 1), (1, 0)]
    beside = []
    for left in range(1, devices - 1, 2):
        beside += [(left, left + 1), (left + 1, left)]
    device = lax.axis_index(ALL).astype(I32)
    dev = device.reshape(1)
    core = device % 2
    encode_factor = mesh_rows / edges
    decode_factor = rows / decode_source.shape[0]
    middle_factor = level_rows / (mesh_rows * subs)
    summit_factor = TOP_NODES / (level_rows * tiles)
    group = min(features // half, tiles)
    groups = tiles // group
    chunk = group * half

    grid_far = lax.ppermute(grid_feats, ALL, beside)
    grid_partner = lax.ppermute(grid_feats, "core", swap)
    edges_in, weight_in, own_rows, picks, aims, members, nodes = call(
        ready_kernel,
        [
            shape((edges, features), BF16),
            shape((features, features), BF16),
            shape((edges, features), BF16),
            shape((edges, 2 * rows), BF16),
            shape((mesh_rows, edges), BF16),
            shape((level_rows, mesh_rows), BF16),
            shape((8, features), BF16),
        ],
        [
            dev,
            grid_feats,
            encode_edges,
            encode_weight,
            encode_source[None],
            encode_target[None],
            owner_fine[None],
            owner_coarse[None],
        ],
        subs=subs,
    )
    fetched, core_pkt, far_pkt, keep = call(
        encode_kernel,
        [
            shape((edges, features), BF16),
            shape((half + mesh_rows + 8, features), BF16),
            shape((mesh_rows + 8, features), BF16),
            shape((half, features), F32),
        ],
        [
            dev,
            grid_partner,
            grid_far,
            mesh_feats,
            edges_in,
            weight_in,
            own_rows,
            picks,
            aims,
            members,
            nodes,
        ],
        factor=encode_factor,
    )
    core_in = lax.ppermute(core_pkt, "core", swap)
    far_in = lax.ppermute(far_pkt, ALL, beside)
    mine = call(add_kernel, shape((half, features), BF16), [dev, keep, core_in])
    other = lax.ppermute(mine, "row", swap)
    packet = call(
        spread_kernel,
        shape(((features // LANES) * half + 8, LANES), BF16),
        [dev, mine, other, owner_coarse[None]],
        subs=subs,
        factor=middle_factor,
    )
    away = lax.ppermute(packet, "half", swap)
    slope, picks, returns, aims, incoming, back_aims = call(
        slope_kernel,
        [
            shape((edges, features), BF16),
            shape((decode_source.shape[0], 3 * mesh_rows), BF16),
            shape((3 * mesh_rows, decode_source.shape[0]), BF16),
            shape((rows, decode_source.shape[0]), BF16),
            shape(decode_edges.shape, F32),
            shape((edges, mesh_rows), BF16),
        ],
        [
            dev,
            fetched,
            edges_in,
            weight_in,
            decode_source[None],
            decode_target[None],
            encode_target[None],
            cotangent,
        ],
        factor=decode_factor,
    )
    packed = call(
        pair_kernel, shape((near, 2 * packet.shape[0], LANES), BF16), [dev, packet, away]
    )
    mids = lax.all_to_all(packed, "near", 0, 0)
    mids_other = lax.ppermute(mids, "core", swap)
    firsts = call(
        first_kernel,
        [
            shape((groups, chunk, features), BF16),
            shape((groups, 8, chunk), I32),
            shape((groups, chunk, features), BF16),
            shape((TOP_NODES, features), F32),
        ],
        [dev, mids, middle_weight],
        subs=subs,
        half=half,
    )
    full = (2, groups, chunk, features)
    (
        decode_fetched,
        decode_slope,
        decode_act,
        own,
        partner,
        far,
        level,
        summit_in,
        ids,
    ) = call(
        middle_kernel,
        [
            shape(decode_edges.shape, BF16),
            shape(decode_edges.shape, BF16),
            shape(decode_edges.shape, BF16),
            shape((mesh_rows, features), F32),
            shape((mesh_rows, features), F32),
            shape((mesh_rows, features), BF16),
            shape(full, BF16),
            shape((TOP_NODES, features), BF16),
            shape((2, groups, 8, chunk), I32),
        ],
        [
            dev,
            *firsts,
            mids_other,
            core_in,
            far_pkt,
            far_in,
            picks,
            returns,
            incoming,
            decode_edges,
            decode_weight,
            middle_weight,
            summit_weight,
        ],
        scratch=[
            shape((2, tiles * half, features), BF16),
        ],
        subs=subs,
        level_rows=level_rows,
        summit_factor=summit_factor,
    )
    far_back = lax.ppermute(far, ALL, beside)
    grid_update, dgrad, middle_slope, summit_slope = call(
        update_kernel,
        [
            shape((rows, features), BF16),
            shape((features, features), F32),
            shape(full, BF16),
            shape((TOP_NODES, features), F32),
        ],
        [
            dev,
            grid_feats,
            aims,
            decode_act,
            decode_fetched,
            decode_slope,
            level,
            summit_in,
            middle_weight,
            summit_weight,
        ],
        factor=decode_factor,
    )
    grad_sum, core_pkt, keep = call(
        level_kernel,
        [
            shape((mesh_rows, features), F32),
            shape((half + mesh_rows, features), BF16),
            shape((half, features), F32),
        ],
        [dev, own, far_back, partner, far_pkt, core_in],
        level_rows=level_rows,
    )
    back_in = lax.ppermute(core_pkt, "core", swap)
    mine = call(add_kernel, shape((half, features), BF16), [dev, keep, back_in])
    other = lax.ppermute(mine, "row", swap)
    total = call(add_kernel, shape((half, features), BF16), [dev, mine, other])
    away = lax.ppermute(total, "half", swap)
    tops, lifts, fines = call(
        tops_kernel,
        [
            shape((2, groups, TOP_NODES, chunk), BF16),
            shape((level_rows, TOP_NODES), BF16),
            shape((mesh_rows, level_rows), BF16),
        ],
        [dev, ids, owner_coarse[None], far_pkt],
    )
    packed = call(pair_kernel, shape((near, 2 * half, features), BF16), [dev, total, away])
    grads = lax.all_to_all(packed, "near", 0, 0)
    grads_other = lax.ppermute(grads, "core", swap)
    send, keep, level_back, top, top_back = call(
        back_kernel,
        [
            shape((features, features), BF16),
            shape((features, features), F32),
            shape(full, BF16),
            shape((TOP_NODES, features), BF16),
            shape((TOP_NODES, features), BF16),
        ],
        [
            dev,
            grads,
            grads_other,
            middle_slope,
            summit_slope,
            tops,
            grad_sum,
            back_in,
            fines,
            lifts,
            fetched,
            slope,
            back_aims,
            dgrad,
            middle_weight,
            summit_weight,
        ],
        subs=subs,
        summit_factor=summit_factor,
        middle_factor=middle_factor,
        encode_factor=encode_factor,
    )
    received = lax.ppermute(send, "core", swap)
    lift_slope = call(
        lift_kernel,
        shape(full, BF16),
        [dev, level_back, middle_slope, top_back, tops],
        summit_factor=summit_factor,
    )
    share = call(add_kernel, shape((features, features), BF16), [dev, keep, received])
    share = share.reshape(peers, features // peers, features)
    parts = lax.all_to_all(share, NEAR, 0, 0)
    inside = call(gather_kernel, shape(parts.shape[1:], BF16), [dev, parts])
    away = lax.ppermute(inside, "half", swap)
    copies = call(copies_kernel, shape(parts.shape, BF16), [dev, inside, away])
    mine = lax.all_to_all(copies, NEAR, 0, 0).reshape(features, features)
    other = lax.ppermute(mine, "core", swap)
    summit_grad = call(
        top_kernel, shape((features, features), F32), [dev, summit_in, top]
    )
    middle_grad = call(
        late_kernel, shape((features, features), F32), [dev, level, lift_slope]
    )
    encode_grad = jnp.where(core == 0, mine, other).astype(F32)
    decode_grad = jnp.where(core == 0, other, mine).astype(F32)
    return (grid_update, encode_grad, decode_grad, middle_grad, summit_grad)


def solution(mesh):
    tiles, subs = mesh.devices.shape
    fine = Mesh(mesh.devices.reshape(2, tiles // 2, subs // 2, 2), ALL)
    placed = (
        P(ALL, None),
        P(ALL, None),
        P(ALL, None),
        P(ALL, None),
        P(ALL),
        P(ALL),
        P(ALL),
        P(ALL),
        P(ALL),
        P(TILE),
        P(),
        P(),
        P(),
        P(),
        P(ALL, None),
    )
    return jax.shard_map(
        shards,
        mesh=fine,
        in_specs=placed,
        out_specs=(P(ALL, None), P(), P(), P(), P()),
        check_vma=False,
    )
```

```python
import functools

import jax
import jax.numpy as jnp
from jax import lax
from jax.experimental import pallas as pl
from jax.experimental.pallas import tpu as pltpu
from jax.sharding import Mesh, PartitionSpec as P


TOP_NODES = 512
LANES = 128
WORKING_BYTES = 10 * 2**20
TILE = ("half", "near")
ALL = TILE + ("row", "core")
NEAR = ("near", "row")
BF16 = jnp.bfloat16
F32 = jnp.float32
I32 = jnp.int32


def mm(left, right):
    return jnp.dot(left, right, preferred_element_type=F32)


def mm_tn(left, right):
    return lax.dot_general(left, right, (((0,), (0,)), ((), ())), preferred_element_type=F32)


def mm_nt(left, right):
    return lax.dot_general(left, right, (((1,), (1,)), ((), ())), preferred_element_type=F32)


def sigmoid(values):
    return 0.5 + 0.5 * jnp.tanh(0.5 * values)


def rows_onehot(ids, rows):
    n = ids.shape[1]
    hit = lax.broadcasted_iota(I32, (rows, n), 0) == ids
    return jnp.where(hit, 1.0, 0.0).astype(BF16)


def column(ids):
    n = ids.shape[1]
    wide = jnp.broadcast_to(ids.astype(F32), (8, n))
    return wide.T[:, :1].astype(I32)


def cols_onehot(ids, cols):
    n = ids.shape[1]
    hit = lax.broadcasted_iota(I32, (n, cols), 1) == column(ids)
    return jnp.where(hit, 1.0, 0.0).astype(BF16)


def coarse_split(ids):
    at = lax.broadcasted_iota(I32, (16, ids.shape[1]), 0)
    parts = jnp.where(at == 0, ids >> 4, jnp.where(at == 1, ids & 15, 0))
    return parts.astype(F32).astype(BF16)


def node_ids(block):
    codes = block.astype(F32)
    return (codes[2:3].astype(I32), (codes[0:1] * 16.0 + codes[1:2]).astype(I32))


def slots(source, device, core, rows):
    rel = source - device * rows
    before = rel < 0
    after = rel >= rows
    shift_before = jnp.where(core == 0, 3 * rows, 2 * rows)
    shift_after = jnp.where(core == 0, 0, rows)
    return rel + jnp.where(before, shift_before, 0) + jnp.where(after, shift_after, 0)


def ready_kernel(
    dev_ref,
    grid_ref,
    edges_ref,
    weight_ref,
    source_ref,
    target_ref,
    fine_ref,
    coarse_ref,
    edges_out_ref,
    weight_out_ref,
    own_ref,
    picks_ref,
    aims_ref,
    members_ref,
    nodes_ref,
    *,
    subs,
):
    device = dev_ref[0]
    rows, features = grid_ref.shape
    mesh_rows = fine_ref.shape[1]
    level_rows = coarse_ref.shape[1]
    picks = cols_onehot(slots(source_ref[...], device, device % 2, rows), 3 * rows)
    picks_ref[...] = picks[:, rows:]
    raw = target_ref[...]
    aimed = jnp.where(raw >= 0, raw - device * mesh_rows, -1)
    aims_ref[...] = rows_onehot(aimed, mesh_rows)
    local = fine_ref[...] - (device // subs) * level_rows
    members = rows_onehot(local, level_rows)
    members_ref[...] = members
    spot = (
        lax.broadcasted_iota(I32, (mesh_rows, features), 0)
        == lax.broadcasted_iota(I32, (mesh_rows, features), 1)
    )
    spread = jnp.where(spot, 1.0, 0.0).astype(BF16)
    at = lax.broadcasted_iota(I32, (16, mesh_rows), 0)
    codes = mm(coarse_split(coarse_ref[...]), members)
    codes = jnp.where(at == 2, local.astype(F32), codes)
    nodes_ref[...] = mm(codes.astype(BF16), spread).astype(BF16)[:8]
    own_ref[...] = mm(picks[:, :rows], grid_ref[...]).astype(BF16)
    edges_out_ref[...] = edges_ref[...]
    weight_out_ref[...] = weight_ref[...]


def encode_kernel(
    dev_ref,
    partner_ref,
    far_ref,
    mesh_ref,
    edges_ref,
    weight_ref,
    own_ref,
    picks_ref,
    aims_ref,
    members_ref,
    nodes_ref,
    fetched_ref,
    core_ref,
    farpkt_ref,
    keep_ref,
    *,
    factor,
):
    core = dev_ref[0] % 2
    mesh_rows = mesh_ref.shape[0]
    half = keep_ref.shape[0]
    others = jnp.concatenate([partner_ref[...], far_ref[...]], axis=0)
    fetched = (own_ref[...].astype(F32) + mm(picks_ref[...], others)).astype(BF16)
    fetched_ref[...] = fetched
    pre = mm(fetched, weight_ref[...]) + edges_ref[...].astype(F32)
    sig = sigmoid(pre)
    act = (pre * sig).astype(BF16)
    summed = mm(aims_ref[...], act)
    mid = (mesh_ref[...].astype(F32) + factor * summed).astype(BF16)
    part = mm(members_ref[...], mid)
    first = part[:half]
    second = part[half:]
    keep_ref[...] = jnp.where(core == 0, first, second)
    core_ref[:half] = jnp.where(core == 0, second, first).astype(BF16)
    core_ref[half : half + mesh_rows] = mid
    core_ref[half + mesh_rows :] = nodes_ref[...]
    farpkt_ref[:mesh_rows] = mid
    farpkt_ref[mesh_rows:] = nodes_ref[...]


def pack_kernel(dev_ref, keep_ref, core_ref, coarse_ref, out_ref, *, subs):
    device = dev_ref[0]
    core = device % 2
    tile = device // subs
    half, features = keep_ref.shape
    group = features // half
    level_rows = coarse_ref.shape[1]
    out_ref[:half] = (keep_ref[...] + core_ref[:half].astype(F32)).astype(BF16)
    j = lax.broadcasted_iota(I32, (level_rows, features), 0) - core * half
    lane = lax.broadcasted_iota(I32, (level_rows, features), 1) - (tile % group) * half
    sel = (j == lane) & (j >= 0) & (j < half)
    codes = mm(coarse_split(coarse_ref[...]), jnp.where(sel, 1.0, 0.0).astype(BF16))
    out_ref[half:] = codes.astype(BF16)[:8]


def row_total(dev_ref, mine_ref, first_ref, second_ref, half, subs):
    row = (dev_ref[0] % subs) // 2
    mine = mine_ref[:half].astype(F32)
    second = second_ref[:half].astype(F32)
    return row, first_ref[:half].astype(F32) + jnp.where(row == 0, mine, second)


def spread_kernel(dev_ref, mine_ref, first_ref, second_ref, out_ref, *, subs, half, factor):
    row, total = row_total(dev_ref, mine_ref, first_ref, second_ref, half, subs)
    mid = (factor * total).astype(BF16)
    codes = jnp.where(row == 0, mine_ref[half:].astype(F32), second_ref[half:].astype(F32))
    lanes = out_ref.shape[2]
    strips = mine_ref.shape[1] // lanes
    tail = jnp.concatenate(
        [codes[r : r + 1, i * lanes : (i + 1) * lanes] for r in range(2) for i in range(strips)],
        axis=0,
    ).astype(BF16)
    for peer in range(out_ref.shape[0]):
        for i in range(strips):
            out_ref[peer, i * half : (i + 1) * half] = mid[:, i * lanes : (i + 1) * lanes]
        out_ref[peer, strips * half :] = tail


def respread_kernel(dev_ref, mine_ref, first_ref, second_ref, out_ref, *, subs):
    half = mine_ref.shape[0]
    _, total = row_total(dev_ref, mine_ref, first_ref, second_ref, half, subs)
    total = total.astype(BF16)
    for peer in range(out_ref.shape[0]):
        out_ref[peer] = total


def placed_blocks(tile, near, group, half):
    count = min(group, near)
    mine = tile // near
    for part in range(2):
        side = mine if part == 0 else 1 - mine
        for first in range(0, near, count):
            at = side * near + first
            yield part, first, count, at // group, pl.multiple_of((at % group) * half, half)


def unpack_half(src_ref, tile, level_ref, ids_ref, half):
    near, span, lanes = src_ref.shape
    _, chunk, features = level_ref.shape
    strips = features // lanes
    unit = span // 2
    ids_ref[...] = jnp.zeros(ids_ref.shape, I32)
    for part, first, count, g, row in placed_blocks(tile, near, chunk // half, half):
        block = src_ref[first : first + count, part * unit : (part + 1) * unit]
        for i in range(strips):
            level_ref[g, pl.ds(row, count * half), i * lanes : (i + 1) * lanes] = block[
                :, i * half : (i + 1) * half
            ].reshape(count * half, lanes)
        codes = jnp.sum(block[:, strips * half :].astype(F32), axis=0)
        ids = codes[:strips] * 16.0 + codes[strips : 2 * strips]
        ids = jnp.concatenate([ids[i : i + 1] for i in range(strips)], axis=1)
        ids_ref[g] += jnp.broadcast_to(ids.astype(I32)[:, :chunk], (8, chunk))


def pooled(mid, ids, weight_ref):
    act = mm(mid, weight_ref[...])
    out = (mid.astype(F32) + act * sigmoid(act)).astype(BF16)
    return out, mm(rows_onehot(ids[:1], TOP_NODES), out)


def first_kernel(
    dev_ref, mine_ref, weight_ref, level_ref, ids_ref, out_ref, part_ref, *, subs, half
):
    unpack_half(mine_ref, dev_ref[0] // subs, level_ref, ids_ref, half)
    part = jnp.zeros(part_ref.shape, F32)
    for g in range(level_ref.shape[0]):
        out, add = pooled(level_ref[g], ids_ref[g], weight_ref)
        out_ref[g] = out
        part = part + add
    part_ref[...] = part


def middle_kernel(
    dev_ref,
    first_level_ref,
    first_ids_ref,
    first_out_ref,
    first_part_ref,
    other_ref,
    core_ref,
    farpkt_ref,
    farin_ref,
    picks_ref,
    returns_ref,
    incoming_ref,
    edges_ref,
    decode_weight_ref,
    middle_weight_ref,
    summit_weight_ref,
    fetched_ref,
    slope_ref,
    act_ref,
    own_ref,
    partner_ref,
    far_ref,
    level_ref,
    summit_in_ref,
    ids_ref,
    out_scr,
    *,
    subs,
    level_rows,
    summit_factor,
):
    device = dev_ref[0]
    core = device % 2
    tile = device // subs
    near = other_ref.shape[0]
    tiles = 2 * near
    half = level_rows // 2
    _, groups, chunk, _ = level_ref.shape
    level_ref[core] = first_level_ref[...]
    ids_ref[core] = first_ids_ref[...]
    for g in range(groups):
        out_scr[core, pl.ds(g * chunk, chunk)] = first_out_ref[g]
    away = 1 - core
    unpack_half(other_ref, tile, level_ref.at[away], ids_ref.at[away], half)
    part = jnp.zeros(first_part_ref.shape, F32)
    for g in range(groups):
        out, add = pooled(level_ref[away, g], ids_ref[away, g], middle_weight_ref)
        out_scr[away, pl.ds(g * chunk, chunk)] = out
        part = part + add
    summed = first_part_ref[...] + part
    summit_in = (summit_factor * summed).astype(BF16)
    summit_in_ref[...] = summit_in
    act = mm(summit_in, summit_weight_ref[...])
    sig = sigmoid(act)
    summit_out = (act * sig).astype(BF16)

    mesh_rows = farpkt_ref.shape[0] - 8
    rows = mesh_rows
    sub = device % subs
    far_tile = jnp.where(sub == 0, tile - 1, jnp.where(sub == subs - 1, tile + 1, tile))
    far_tile = jnp.clip(far_tile, 0, tiles - 1)

    def table(ref):
        pieces = []
        for at in (tile, far_tile):
            for h in range(2):
                pieces.append(ref[h, pl.ds(pl.multiple_of(at * half, half), half)])
        return jnp.concatenate(pieces, axis=0)

    own_fine, own_top = node_ids(farpkt_ref[rows:, :rows])
    partner_fine, partner_top = node_ids(core_ref[half + rows :, :rows])
    far_fine, far_top = node_ids(farin_ref[rows:, :rows])
    fine = jnp.concatenate([own_fine, partner_fine, far_fine + level_rows], axis=1)
    top = jnp.concatenate([own_top, partner_top, far_top], axis=1)
    lifted = mm(cols_onehot(fine, 2 * level_rows), table(out_scr)) + mm(
        cols_onehot(top, TOP_NODES), summit_out
    )
    mids = jnp.concatenate(
        [farpkt_ref[:rows], core_ref[half : half + rows], farin_ref[:rows]], axis=0
    )
    wide = (mids.astype(F32) + lifted).astype(BF16)

    fetched = mm(picks_ref[...], wide).astype(BF16)
    pre = mm(fetched, decode_weight_ref[...]) + edges_ref[...].astype(F32)
    sig = sigmoid(pre)
    fetched_ref[...] = fetched
    act_ref[...] = (pre * sig).astype(BF16)
    slope = (incoming_ref[...] * (sig * (1.0 + pre * (1.0 - sig)))).astype(BF16)
    slope_ref[...] = slope
    gathered = mm(returns_ref[...], slope).astype(BF16)
    returned = mm_nt(gathered, decode_weight_ref[...])
    own_ref[...] = returned[:rows]
    partner_ref[...] = returned[rows : 2 * rows]
    far_ref[...] = returned[2 * rows :].astype(BF16)


def silu_slope(values):
    sig = sigmoid(values)
    return sig * (1.0 + values * (1.0 - sig))


def slope_kernel(
    dev_ref,
    fetched_ref,
    edges_ref,
    weight_ref,
    source_ref,
    target_ref,
    encode_target_ref,
    cot_ref,
    slope_ref,
    picks_ref,
    returns_ref,
    aims_ref,
    incoming_ref,
    back_aims_ref,
    *,
    factor,
):
    device = dev_ref[0]
    rows = cot_ref.shape[0]
    place = slots(source_ref[...], device, device % 2, rows)
    picks_ref[...] = cols_onehot(place, 3 * rows)
    returns_ref[...] = rows_onehot(place, 3 * rows)
    raw = target_ref[...]
    aimed = jnp.where(raw >= 0, raw - device * rows, -1)
    aims_ref[...] = rows_onehot(aimed, rows)
    incoming_ref[...] = mm(cols_onehot(aimed, rows), cot_ref[...]) * factor
    raw = encode_target_ref[...]
    mesh_rows = back_aims_ref.shape[1]
    aimed = jnp.where(raw >= 0, raw - device * mesh_rows, -1)
    back_aims_ref[...] = cols_onehot(aimed, mesh_rows)
    pre = mm(fetched_ref[...], weight_ref[...]) + edges_ref[...].astype(F32)
    slope_ref[...] = silu_slope(pre).astype(BF16)


def update_kernel(
    dev_ref,
    grid_ref,
    aims_ref,
    act_ref,
    fetched_ref,
    slope_ref,
    level_ref,
    summit_in_ref,
    middle_weight_ref,
    summit_weight_ref,
    update_ref,
    dgrad_ref,
    middle_slope_ref,
    summit_slope_ref,
    *,
    factor,
):
    summed = mm(aims_ref[...], act_ref[...])
    update_ref[...] = (grid_ref[...].astype(F32) + factor * summed).astype(BF16)
    dgrad_ref[...] = mm_tn(fetched_ref[...], slope_ref[...])
    for h in range(2):
        for g in range(level_ref.shape[1]):
            act = mm(level_ref[h, g], middle_weight_ref[...])
            middle_slope_ref[h, g] = silu_slope(act).astype(BF16)
    summit_slope_ref[...] = silu_slope(mm(summit_in_ref[...], summit_weight_ref[...]))


def level_kernel(
    dev_ref, own_ref, farin_ref, partner_ref, farpkt_ref, core_ref,
    sum_ref, pkt_ref, keep_ref, *, level_rows
):
    core = dev_ref[0] % 2
    rows = own_ref.shape[0]
    half = level_rows // 2
    grad = own_ref[...] + farin_ref[...].astype(F32)
    sum_ref[...] = grad
    own_fine, _ = node_ids(farpkt_ref[rows:, :rows])
    partner_fine, _ = node_ids(core_ref[half + rows :, :rows])
    partner = partner_ref[...].astype(BF16)
    part = mm(rows_onehot(own_fine, level_rows), grad.astype(BF16)) + mm(
        rows_onehot(partner_fine, level_rows), partner
    )
    first = part[:half]
    second = part[half:]
    keep_ref[...] = jnp.where(core == 0, first, second)
    pkt_ref[:half] = jnp.where(core == 0, second, first).astype(BF16)
    pkt_ref[half:] = partner


def tops_kernel(dev_ref, ids_ref, coarse_ref, farpkt_ref, tops_ref, lifts_ref, fine_ref):
    for h in range(2):
        for g in range(ids_ref.shape[1]):
            tops_ref[h, g] = rows_onehot(ids_ref[h, g][:1], TOP_NODES)
    lifts_ref[...] = cols_onehot(coarse_ref[...], TOP_NODES)
    rows = fine_ref.shape[0]
    own_fine, _ = node_ids(farpkt_ref[rows:, :rows])
    fine_ref[...] = cols_onehot(own_fine, fine_ref.shape[1])


def back_kernel(
    dev_ref,
    mine_ref,
    other_ref,
    middle_slope_ref,
    summit_slope_ref,
    tops_ref,
    sum_ref,
    partnerin_ref,
    fine_ref,
    lifts_ref,
    fetched_ref,
    slope_ref,
    aims_ref,
    dgrad_ref,
    middle_weight_ref,
    summit_weight_ref,
    send_ref,
    keep_ref,
    grad_ref,
    top_ref,
    top_back_ref,
    *,
    subs,
    summit_factor,
    middle_factor,
    encode_factor,
):
    device = dev_ref[0]
    core = device % 2
    tile = device // subs
    near, pair, features = mine_ref.shape
    half = pair // 2
    _, groups, chunk, _ = grad_ref.shape
    group = chunk // half
    for part, first, count, g, row in placed_blocks(tile, near, group, half):
        for src, which in ((mine_ref, core), (other_ref, 1 - core)):
            grad_ref[which, g, pl.ds(row, count * half)] = src[
                first : first + count, part * half : (part + 1) * half
            ].reshape(count * half, features)
    total = jnp.zeros((TOP_NODES, features), F32)
    for g in range(groups):
        for h in range(2):
            total = total + mm(tops_ref[h, g], grad_ref[h, g])
    summit_slope = (total * summit_slope_ref[...]).astype(BF16)
    top_ref[...] = summit_slope
    summit_back = mm_nt(summit_slope, summit_weight_ref[...]).astype(BF16)
    top_back_ref[...] = summit_back
    spot = pl.multiple_of((tile % group) * half, half)

    def own(ref):
        pieces = [ref[h, tile // group, pl.ds(spot, half)] for h in range(2)]
        return jnp.concatenate(pieces, axis=0).astype(F32)

    level_total = own(grad_ref) + summit_factor * mm(lifts_ref[...], summit_back)
    slope = (level_total * own(middle_slope_ref)).astype(BF16)
    back = (level_total + mm_nt(slope, middle_weight_ref[...])).astype(BF16)
    mesh_total = (
        sum_ref[...]
        + partnerin_ref[half:].astype(F32)
        + middle_factor * mm(fine_ref[...], back)
    )
    upstream = mm(aims_ref[...], mesh_total.astype(BF16)) * encode_factor
    slope = (upstream * slope_ref[...].astype(F32)).astype(BF16)
    egrad = mm_tn(fetched_ref[...], slope)
    dgrad = dgrad_ref[...]
    send_ref[...] = jnp.where(core == 0, dgrad, egrad).astype(BF16)
    keep_ref[...] = jnp.where(core == 0, egrad, dgrad)


def lift_kernel(
    dev_ref, grad_ref, middle_slope_ref, top_back_ref, tops_ref, slope_ref, *, summit_factor
):
    for g in range(grad_ref.shape[1]):
        for h in range(2):
            lifted = mm_tn(tops_ref[h, g], top_back_ref[...])
            level_total = grad_ref[h, g].astype(F32) + summit_factor * lifted
            slope_ref[h, g] = (level_total * middle_slope_ref[h, g].astype(F32)).astype(BF16)


def late_kernel(dev_ref, level_ref, slope_ref, middle_grad_ref):
    middle_grad = jnp.zeros(middle_grad_ref.shape, F32)
    for g in range(level_ref.shape[1]):
        for h in range(2):
            middle_grad = middle_grad + mm_tn(level_ref[h, g], slope_ref[h, g])
    middle_grad_ref[...] = middle_grad


def add_kernel(dev_ref, mine_ref, other_ref, out_ref):
    rows = out_ref.shape[0]
    total = mine_ref[...].astype(F32) + other_ref[:rows].astype(F32)
    out_ref[...] = total.astype(BF16)


def gather_kernel(dev_ref, parts_ref, out_ref):
    total = parts_ref[0].astype(F32)
    for peer in range(1, parts_ref.shape[0]):
        total = total + parts_ref[peer].astype(F32)
    out_ref[...] = total.astype(BF16)


def copies_kernel(dev_ref, mine_ref, other_ref, out_ref):
    total = (mine_ref[...].astype(F32) + other_ref[...].astype(F32)).astype(BF16)
    for peer in range(out_ref.shape[0]):
        out_ref[peer] = total


def top_kernel(dev_ref, summit_in_ref, top_ref, summit_grad_ref):
    summit_grad_ref[...] = mm_tn(summit_in_ref[...], top_ref[...])


def call(body, outs, args, scratch=(), **static):
    vmem = pl.BlockSpec(memory_space=pltpu.VMEM)
    smem = pl.BlockSpec(memory_space=pltpu.SMEM)
    specs = [smem if a.ndim == 1 else vmem for a in args]
    single = not isinstance(outs, (list, tuple))
    held = [a for a in args if a.ndim > 1] + ([outs] if single else list(outs)) + list(scratch)
    limit = sum(a.size * a.dtype.itemsize for a in held) + WORKING_BYTES
    limit = min(limit, 60 * 2**20)
    return pl.pallas_call(
        functools.partial(body, **static),
        out_shape=outs,
        in_specs=specs,
        out_specs=vmem if single else [vmem] * len(outs),
        scratch_shapes=[pltpu.VMEM(s.shape, s.dtype) for s in scratch],
        compiler_params=pltpu.CompilerParams(vmem_limit_bytes=limit),
    )(*args)


def shape(dims, dtype):
    return jax.ShapeDtypeStruct(dims, dtype)


def shards(
    grid_feats,
    mesh_feats,
    encode_edges,
    decode_edges,
    encode_source,
    encode_target,
    decode_source,
    decode_target,
    owner_fine,
    owner_coarse,
    encode_weight,
    decode_weight,
    middle_weight,
    summit_weight,
    cotangent,
):
    rows, features = grid_feats.shape
    mesh_rows = mesh_feats.shape[0]
    level_rows = owner_coarse.shape[0]
    half = level_rows // 2
    tiles = lax.axis_size(TILE)
    subs = lax.axis_size("row") * lax.axis_size("core")
    devices = tiles * subs
    peers = devices // 4
    near = tiles // 2
    edges = encode_source.shape[0]
    swap = [(0, 1), (1, 0)]
    turn = [(1, 0), (3, 2), (0, 3), (2, 1)]
    over = [(1, 3), (3, 1)]
    beside = []
    for left in range(1, devices - 1, 2):
        beside += [(left, left + 1), (left + 1, left)]
    device = lax.axis_index(ALL).astype(I32)
    dev = device.reshape(1)
    core = device % 2
    encode_factor = mesh_rows / edges
    decode_factor = rows / decode_source.shape[0]
    middle_factor = level_rows / (mesh_rows * subs)
    summit_factor = TOP_NODES / (level_rows * tiles)
    group = min(features // half, tiles)
    groups = tiles // group
    chunk = group * half

    grid_far = lax.ppermute(grid_feats, ALL, beside)
    grid_partner = lax.ppermute(grid_feats, "core", swap)
    edges_in, weight_in, own_rows, picks, aims, members, nodes = call(
        ready_kernel,
        [
            shape((edges, features), BF16),
            shape((features, features), BF16),
            shape((edges, features), BF16),
            shape((edges, 2 * rows), BF16),
            shape((mesh_rows, edges), BF16),
            shape((level_rows, mesh_rows), BF16),
            shape((8, features), BF16),
        ],
        [
            dev,
            grid_feats,
            encode_edges,
            encode_weight,
            encode_source[None],
            encode_target[None],
            owner_fine[None],
            owner_coarse[None],
        ],
        subs=subs,
    )
    fetched, core_pkt, far_pkt, keep = call(
        encode_kernel,
        [
            shape((edges, features), BF16),
            shape((half + mesh_rows + 8, features), BF16),
            shape((mesh_rows + 8, features), BF16),
            shape((half, features), F32),
        ],
        [
            dev,
            grid_partner,
            grid_far,
            mesh_feats,
            edges_in,
            weight_in,
            own_rows,
            picks,
            aims,
            members,
            nodes,
        ],
        factor=encode_factor,
    )
    core_in = lax.ppermute(core_pkt, "core", swap)
    far_in = lax.ppermute(far_pkt, ALL, beside)
    mine = call(
        pack_kernel,
        shape((half + 8, features), BF16),
        [dev, keep, core_in, owner_coarse[None]],
        subs=subs,
    )
    first_in = lax.ppermute(mine, ("half", "row"), turn)
    second_in = lax.ppermute(mine, ("half", "row"), over)
    slope, picks, returns, aims, incoming, back_aims = call(
        slope_kernel,
        [
            shape((edges, features), BF16),
            shape((decode_source.shape[0], 3 * mesh_rows), BF16),
            shape((3 * mesh_rows, decode_source.shape[0]), BF16),
            shape((rows, decode_source.shape[0]), BF16),
            shape(decode_edges.shape, F32),
            shape((edges, mesh_rows), BF16),
        ],
        [
            dev,
            fetched,
            edges_in,
            weight_in,
            decode_source[None],
            decode_target[None],
            encode_target[None],
            cotangent,
        ],
        factor=decode_factor,
    )
    span = (features // LANES) * half + 8
    packed = call(
        spread_kernel,
        shape((2 * near, span, LANES), BF16),
        [dev, mine, first_in, second_in],
        subs=subs,
        half=half,
        factor=middle_factor,
    )
    mids = lax.all_to_all(packed, NEAR, 0, 0).reshape(near, 2 * span, LANES)
    mids_other = lax.ppermute(mids, "core", swap)
    firsts = call(
        first_kernel,
        [
            shape((groups, chunk, features), BF16),
            shape((groups, 8, chunk), I32),
            shape((groups, chunk, features), BF16),
            shape((TOP_NODES, features), F32),
        ],
        [dev, mids, middle_weight],
        subs=subs,
        half=half,
    )
    full = (2, groups, chunk, features)
    (
        decode_fetched,
        decode_slope,
        decode_act,
        own,
        partner,
        far,
        level,
        summit_in,
        ids,
    ) = call(
        middle_kernel,
        [
            shape(decode_edges.shape, BF16),
            shape(decode_edges.shape, BF16),
            shape(decode_edges.shape, BF16),
            shape((mesh_rows, features), F32),
            shape((mesh_rows, features), F32),
            shape((mesh_rows, features), BF16),
            shape(full, BF16),
            shape((TOP_NODES, features), BF16),
            shape((2, groups, 8, chunk), I32),
        ],
        [
            dev,
            *firsts,
            mids_other,
            core_in,
            far_pkt,
            far_in,
            picks,
            returns,
            incoming,
            decode_edges,
            decode_weight,
            middle_weight,
            summit_weight,
        ],
        scratch=[
            shape((2, tiles * half, features), BF16),
        ],
        subs=subs,
        level_rows=level_rows,
        summit_factor=summit_factor,
    )
    far_back = lax.ppermute(far, ALL, beside)
    grid_update, dgrad, middle_slope, summit_slope = call(
        update_kernel,
        [
            shape((rows, features), BF16),
            shape((features, features), F32),
            shape(full, BF16),
            shape((TOP_NODES, features), F32),
        ],
        [
            dev,
            grid_feats,
            aims,
            decode_act,
            decode_fetched,
            decode_slope,
            level,
            summit_in,
            middle_weight,
            summit_weight,
        ],
        factor=decode_factor,
    )
    grad_sum, core_pkt, keep = call(
        level_kernel,
        [
            shape((mesh_rows, features), F32),
            shape((half + mesh_rows, features), BF16),
            shape((half, features), F32),
        ],
        [dev, own, far_back, partner, far_pkt, core_in],
        level_rows=level_rows,
    )
    back_in = lax.ppermute(core_pkt, "core", swap)
    mine = call(add_kernel, shape((half, features), BF16), [dev, keep, back_in])
    first_in = lax.ppermute(mine, ("half", "row"), turn)
    second_in = lax.ppermute(mine, ("half", "row"), over)
    tops, lifts, fines = call(
        tops_kernel,
        [
            shape((2, groups, TOP_NODES, chunk), BF16),
            shape((level_rows, TOP_NODES), BF16),
            shape((mesh_rows, level_rows), BF16),
        ],
        [dev, ids, owner_coarse[None], far_pkt],
    )
    packed = call(
        respread_kernel,
        shape((2 * near, half, features), BF16),
        [dev, mine, first_in, second_in],
        subs=subs,
    )
    grads = lax.all_to_all(packed, NEAR, 0, 0).reshape(near, 2 * half, features)
    grads_other = lax.ppermute(grads, "core", swap)
    send, keep, level_back, top, top_back = call(
        back_kernel,
        [
            shape((features, features), BF16),
            shape((features, features), F32),
            shape(full, BF16),
            shape((TOP_NODES, features), BF16),
            shape((TOP_NODES, features), BF16),
        ],
        [
            dev,
            grads,
            grads_other,
            middle_slope,
            summit_slope,
            tops,
            grad_sum,
            back_in,
            fines,
            lifts,
            fetched,
            slope,
            back_aims,
            dgrad,
            middle_weight,
            summit_weight,
        ],
        subs=subs,
        summit_factor=summit_factor,
        middle_factor=middle_factor,
        encode_factor=encode_factor,
    )
    received = lax.ppermute(send, "core", swap)
    lift_slope = call(
        lift_kernel,
        shape(full, BF16),
        [dev, level_back, middle_slope, top_back, tops],
        summit_factor=summit_factor,
    )
    share = call(add_kernel, shape((features, features), BF16), [dev, keep, received])
    share = share.reshape(peers, features // peers, features)
    parts = lax.all_to_all(share, NEAR, 0, 0)
    inside = call(gather_kernel, shape(parts.shape[1:], BF16), [dev, parts])
    away = lax.ppermute(inside, "half", swap)
    copies = call(copies_kernel, shape(parts.shape, BF16), [dev, inside, away])
    mine = lax.all_to_all(copies, NEAR, 0, 0).reshape(features, features)
    other = lax.ppermute(mine, "core", swap)
    summit_grad = call(
        top_kernel, shape((features, features), F32), [dev, summit_in, top]
    )
    middle_grad = call(
        late_kernel, shape((features, features), F32), [dev, level, lift_slope]
    )
    encode_grad = jnp.where(core == 0, mine, other).astype(F32)
    decode_grad = jnp.where(core == 0, other, mine).astype(F32)
    return (grid_update, encode_grad, decode_grad, middle_grad, summit_grad)


def solution(mesh):
    tiles, subs = mesh.devices.shape
    fine = Mesh(mesh.devices.reshape(2, tiles // 2, subs // 2, 2), ALL)
    placed = (
        P(ALL, None),
        P(ALL, None),
        P(ALL, None),
        P(ALL, None),
        P(ALL),
        P(ALL),
        P(ALL),
        P(ALL),
        P(ALL),
        P(TILE),
        P(),
        P(),
        P(),
        P(),
        P(ALL, None),
    )
    return jax.shard_map(
        shards,
        mesh=fine,
        in_specs=placed,
        out_specs=(P(ALL, None), P(), P(), P(), P()),
        check_vma=False,
    )
```
